8 devices in a mesh: ep: 4 (over z, y, x), dp: 2 (over core).
Axes of the slice: x: 2, y: 2, z: 1, core: 2. Of those that a mesh axis runs over, the one named last changes fastest.
Arguments:
- act_in: bfloat16 [6144, 448], P(('ep', 'dp'))
- grad_out: bfloat16 [6144, 448], P(('ep', 'dp'))
- slot_ids: int32 [2, 6144, 8], P(None, ('ep', 'dp'))
- gate_vals: float32 [2, 6144, 8], P(None, ('ep', 'dp'))
- w_dense: bfloat16 [2, 448, 448], replicated
- w_gate: bfloat16 [2, 384, 448, 128], P(None, 'ep')
- w_up: bfloat16 [2, 384, 448, 128], P(None, 'ep')
- w_down: bfloat16 [2, 384, 128, 448], P(None, 'ep')
- ws_gate: bfloat16 [2, 448, 128], replicated
- ws_up: bfloat16 [2, 448, 128], replicated
- ws_down: bfloat16 [2, 128, 448], replicated
Outputs:
- output 1: bfloat16 [6144, 448], P(('ep', 'dp'))
- output 2: bfloat16 [2, 448, 448], replicated
- output 3: bfloat16 [2, 384, 448, 128], P(None, 'ep')
- output 4: bfloat16 [2, 384, 448, 128], P(None, 'ep')
- output 5: bfloat16 [2, 384, 128, 448], P(None, 'ep')
- output 6: bfloat16 [2, 448, 128], replicated
- output 7: bfloat16 [2, 448, 128], replicated
- output 8: bfloat16 [2, 128, 448], replicated
All inputs are finite; a program needn't handle non-finite values.
Results may differ from the reference program's by a relative error of at most 0.02.
Values are sent between devices in bfloat16 or wider.
A program may use at most 1 GiB of HBM per device.

```python
import functools
import jax
import jax.numpy as jnp
from jax import lax

D = 448
FF = 128
FS = 128
EXPERTS = 384
TOP = 8
TOKENS = 768
EP = 4
DP = 2
LAYERS = 2

NUM_DEV = EP * DP
CAP = 2 * TOKENS * TOP // EXPERTS
ROWS = NUM_DEV * TOKENS


def draw_slots(key):
    key_tok, key_exp = jax.random.split(key)
    mean_load = TOKENS * TOP // EXPERTS
    order = jax.random.permutation(key_tok, TOKENS)
    position = jnp.arange(TOP, dtype=jnp.int32)[None, :] * TOKENS + order[:, None]
    group = position // (4 * mean_load)
    rest = position % (4 * mean_load)
    first = 2 * mean_load
    second = first + mean_load // 2
    third = second + mean_load // 2
    within = (rest >= first).astype(jnp.int32) + (rest >= second).astype(jnp.int32) + (rest >= third).astype(jnp.int32)
    start = jnp.where(rest >= third, third, jnp.where(rest >= second, second, jnp.where(rest >= first, first, 0)))
    expert_perm = jax.random.permutation(key_exp, EXPERTS)
    expert = expert_perm[group * 4 + within]
    return (expert * CAP + rest - start).astype(jnp.int32)


def setup_inputs(seed: int = 0) -> dict:
    keys = jax.random.split(jax.random.key(seed), 12)
    slot_keys = jax.random.split(keys[0], LAYERS * NUM_DEV)
    slot_ids = jax.vmap(draw_slots)(slot_keys).reshape(LAYERS, ROWS, TOP)
    gate_vals = jax.random.uniform(keys[1], (LAYERS, ROWS, TOP), jnp.float32, 0.5, 1.5) / TOP
    act_in = jax.random.normal(keys[2], (ROWS, D), jnp.float32).astype(jnp.bfloat16)
    grad_out = jax.random.normal(keys[3], (ROWS, D), jnp.float32).astype(jnp.bfloat16)
    w_dense = (jax.random.normal(keys[4], (LAYERS, D, D), jnp.float32) * D ** -0.5).astype(jnp.bfloat16)
    w_gate = (jax.random.normal(keys[5], (LAYERS, EXPERTS, D, FF), jnp.float32) * D ** -0.5).astype(jnp.bfloat16)
    w_up = (jax.random.normal(keys[6], (LAYERS, EXPERTS, D, FF), jnp.float32) * D ** -0.5).astype(jnp.bfloat16)
    w_down = (jax.random.normal(keys[7], (LAYERS, EXPERTS, FF, D), jnp.float32) * FF ** -0.5).astype(jnp.bfloat16)
    ws_gate = (jax.random.normal(keys[8], (LAYERS, D, FS), jnp.float32) * D ** -0.5).astype(jnp.bfloat16)
    ws_up = (jax.random.normal(keys[9], (LAYERS, D, FS), jnp.float32) * D ** -0.5).astype(jnp.bfloat16)
    ws_down = (jax.random.normal(keys[10], (LAYERS, FS, D), jnp.float32) * FS ** -0.5).astype(jnp.bfloat16)
    return {"act_in": act_in, "grad_out": grad_out, "slot_ids": slot_ids, "gate_vals": gate_vals, "w_dense": w_dense, "w_gate": w_gate, "w_up": w_up, "w_down": w_down, "ws_gate": ws_gate, "ws_up": ws_up, "ws_down": ws_down}


def expert_block(args, w_gate32, w_up32, w_down32):
    mixed_loc, slot_loc, gate_loc = args
    slot_flat = slot_loc.reshape(TOKENS * TOP)
    copies = jnp.broadcast_to(mixed_loc[:, None, :], (TOKENS, TOP, D)).reshape(TOKENS * TOP, D)
    dispatched = jnp.zeros((EXPERTS * CAP, D), mixed_loc.dtype).at[slot_flat].set(copies)
    dispatched = dispatched.reshape(EXPERTS, CAP, D).astype(jnp.float32)
    a_one = jnp.einsum("ecd,edf->ecf", dispatched, w_gate32)
    a_three = jnp.einsum("ecd,edf->ecf", dispatched, w_up32)
    hidden = (jax.nn.silu(a_one) * a_three).astype(jnp.bfloat16)
    exp_out = jnp.einsum("ecf,efd->ecd", hidden.astype(jnp.float32), w_down32).astype(jnp.bfloat16)
    picked = exp_out.reshape(EXPERTS * CAP, D)[slot_flat].reshape(TOKENS, TOP, D)
    return jnp.sum(gate_loc[:, :, None] * picked.astype(jnp.float32), axis=1)


def moe_layer(act, layer_in):
    w_dense, w_gate, w_up, w_down, ws_gate, ws_up, ws_down, slot_ids, gate_vals = layer_in
    dense_pre = jnp.dot(act, w_dense, preferred_element_type=jnp.float32)
    mixed = (act.astype(jnp.float32) + dense_pre).astype(jnp.bfloat16)
    s_one = jnp.dot(mixed, ws_gate, preferred_element_type=jnp.float32)
    s_three = jnp.dot(mixed, ws_up, preferred_element_type=jnp.float32)
    shared_hidden = (jax.nn.silu(s_one) * s_three).astype(jnp.bfloat16)
    shared_out = jnp.dot(shared_hidden, ws_down, preferred_element_type=jnp.float32)
    block = jax.checkpoint(functools.partial(expert_block, w_gate32=w_gate.astype(jnp.float32), w_up32=w_up.astype(jnp.float32), w_down32=w_down.astype(jnp.float32)))
    routed = lax.map(block, (mixed.reshape(NUM_DEV, TOKENS, D), slot_ids.reshape(NUM_DEV, TOKENS, TOP), gate_vals.reshape(NUM_DEV, TOKENS, TOP)))
    routed = routed.reshape(ROWS, D)
    new_act = (mixed.astype(jnp.float32) + routed + shared_out).astype(jnp.bfloat16)
    return new_act, None


def reference(act_in, grad_out, slot_ids, gate_vals, w_dense, w_gate, w_up, w_down, ws_gate, ws_up, ws_down):
    def forward(act, dense_all, gate_all, up_all, down_all, sgate_all, sup_all, sdown_all):
        final, _ = lax.scan(moe_layer, act, (dense_all, gate_all, up_all, down_all, sgate_all, sup_all, sdown_all, slot_ids, gate_vals))
        return final
    _, pullback = jax.vjp(forward, act_in, w_dense, w_gate, w_up, w_down, ws_gate, ws_up, ws_down)
    grads = pullback(grad_out)
    return (grads[0], grads[1], grads[2], grads[3], grads[4], grads[5], grads[6], grads[7])
```

```python
import functools
import jax
import jax.numpy as jnp
from jax import lax
from jax.experimental import pallas as pl
from jax.experimental.pallas import tpu as pltpu
from jax.sharding import PartitionSpec as P

ALL_AXES = ("ep", "dp")
GROUP = 8
VMEM_LIMIT = 62 * 1024 * 1024
F32 = jnp.float32
BF16 = jnp.bfloat16


def dot(left, right, left_dim, right_dim):
    return lax.dot_general(left, right, (((left_dim,), (right_dim,)), ((), ())), preferred_element_type=F32)


def silu_parts(pre_act):
    sigma = jax.nn.sigmoid(pre_act)
    return pre_act * sigma, sigma * (1.0 + pre_act * (1.0 - sigma))


def route(meta_ref, src, first_expert, capacity, pick_ref, gate_ref):
    top = meta_ref.shape[1] // 2
    tokens = meta_ref.shape[2]
    slots = meta_ref[src, 0:top, :].astype(jnp.int32)
    gates = meta_ref[src, top : 2 * top, :]
    expert = slots // capacity - first_expert
    row = slots % capacity
    which = lax.broadcasted_iota(jnp.int32, (GROUP, tokens), 0)
    row_of = jnp.full((GROUP, tokens), -1, jnp.int32)
    gate_of = jnp.zeros((GROUP, tokens), F32)
    for j in range(top):
        hit = expert[j : j + 1, :] == which
        row_of = jnp.where(hit, row[j : j + 1, :], row_of)
        gate_of = jnp.where(hit, gates[j : j + 1, :], gate_of)
    rows = lax.broadcasted_iota(jnp.int32, (capacity, tokens), 0)
    for k in range(GROUP):
        hit = row_of[k : k + 1, :] == rows
        pick_ref[src, k * capacity : (k + 1) * capacity, :] = jnp.where(hit, 1.0, 0.0).astype(BF16)
        gate_ref[src, k * capacity : (k + 1) * capacity, :] = jnp.sum(jnp.where(hit, gate_of[k : k + 1, :], 0.0), axis=1, keepdims=True)


def fwd_kernel(capacity, base_ref, tok_ref, meta_ref, w1_ref, w3_ref, w2_ref, out_ref, pick_ref, gate_ref, x_ref, o_ref):
    group = pl.program_id(0)
    sources = tok_ref.shape[0]
    width = tok_ref.shape[1]
    rows = GROUP * capacity

    @pl.when(group == 0)
    def _():
        def clear(src, carry):
            out_ref[src] = jnp.zeros(out_ref.shape[1:], F32)
            return carry

        lax.fori_loop(0, sources, clear, 0)

    def dispatch(src, carry):
        route(meta_ref, src, base_ref[0] + group * GROUP, capacity, pick_ref, gate_ref)
        x_ref[src] = dot(pick_ref[src], tok_ref[src], 1, 1).astype(BF16)
        return carry

    lax.fori_loop(0, sources, dispatch, 0)

    def expert(k, carry):
        here = pl.ds(pl.multiple_of(k * capacity, capacity), capacity)
        x = x_ref[:, here, :].reshape(sources * capacity, width)
        a_one = dot(x, w1_ref[k], 1, 0)
        a_three = dot(x, w3_ref[k], 1, 0)
        hidden = (jax.nn.silu(a_one) * a_three).astype(BF16)
        out = dot(hidden, w2_ref[k], 1, 1).astype(BF16).astype(F32)
        gate = gate_ref[:, here, :].reshape(sources * capacity, 1)
        o_ref[:, here, :] = (gate * out).reshape(sources, capacity, width)
        return carry

    lax.fori_loop(0, GROUP, expert, 0)

    def combine(src, carry):
        rest = o_ref[src].T
        pick = pick_ref[src]
        total = out_ref[src]
        for _ in range(3):
            part = rest.astype(BF16)
            total = total + dot(part, pick, 1, 0)
            rest = rest - part.astype(F32)
        out_ref[src] = total
        return carry

    lax.fori_loop(0, sources, combine, 0)


def bwd_kernel(capacity, base_ref, tok_ref, grad_ref, meta_ref, w1_ref, w3_ref, w2_ref, out_ref, d1_ref, d3_ref, d2_ref, sum_ref, pick_ref, gate_ref, x_ref, g_ref):
    group = pl.program_id(0)
    sources = tok_ref.shape[0]
    width = tok_ref.shape[1]

    @pl.when(group == 0)
    def _():
        def clear(src, carry):
            sum_ref[src] = jnp.zeros(sum_ref.shape[1:], F32)
            return carry

        lax.fori_loop(0, sources, clear, 0)

    def dispatch(src, carry):
        route(meta_ref, src, base_ref[0] + group * GROUP, capacity, pick_ref, gate_ref)
        x_ref[src] = dot(pick_ref[src], tok_ref[src], 1, 1).astype(BF16)
        g_ref[src] = (gate_ref[src] * dot(pick_ref[src], grad_ref[src], 1, 1)).astype(BF16)
        return carry

    lax.fori_loop(0, sources, dispatch, 0)

    def expert(k, carry):
        here = pl.ds(pl.multiple_of(k * capacity, capacity), capacity)
        x = x_ref[:, here, :].reshape(sources * capacity, width)
        g = g_ref[:, here, :].reshape(sources * capacity, width)
        a_one = dot(x, w1_ref[k], 1, 0)
        a_three = dot(x, w3_ref[k], 1, 0)
        act, slope = silu_parts(a_one)
        hidden = (act * a_three).astype(BF16)
        grad_hidden = dot(g, w2_ref[k], 1, 0)
        grad_one = (grad_hidden * a_three * slope).astype(BF16)
        grad_three = (grad_hidden * act).astype(BF16)
        d2_ref[k] = dot(g, hidden, 0, 0).astype(BF16)
        d1_ref[k] = dot(x, grad_one, 0, 0).astype(BF16)
        d3_ref[k] = dot(x, grad_three, 0, 0).astype(BF16)
        back = dot(grad_one, w1_ref[k], 1, 1) + dot(grad_three, w3_ref[k], 1, 1)
        x_ref[:, here, :] = back.astype(BF16).reshape(sources, capacity, width)
        return carry

    lax.fori_loop(0, GROUP, expert, 0)

    def combine(src, carry):
        sum_ref[src] += dot(x_ref[src], pick_ref[src], 0, 0)
        return carry

    lax.fori_loop(0, sources, combine, 0)

    @pl.when(group == pl.num_programs(0) - 1)
    def _():
        def finish(src, carry):
            out_ref[src] = sum_ref[src].astype(BF16)
            return carry

        lax.fori_loop(0, sources, finish, 0)


def weight_specs(layer, width, ff):
    spec = pl.BlockSpec((None, GROUP, width, ff), lambda g, base: (layer, base[1] + g, 0, 0))
    return [spec, spec, spec]


def whole():
    return pl.BlockSpec(memory_space=pltpu.VMEM)


def expert_forward(layer, capacity, groups, base, tok, meta, w1, w3, w2):
    sources, width, tokens = tok.shape
    ff = w1.shape[3]
    rows = GROUP * capacity
    return pl.pallas_call(
        functools.partial(fwd_kernel, capacity),
        name=f"expert_fwd_{layer}",
        out_shape=jax.ShapeDtypeStruct((sources, width, tokens), F32),
        grid_spec=pltpu.PrefetchScalarGridSpec(
            num_scalar_prefetch=1,
            grid=(groups,),
            in_specs=[whole(), whole()] + weight_specs(layer, width, ff),
            out_specs=whole(),
            scratch_shapes=[
                pltpu.VMEM((sources, rows, tokens), BF16),
                pltpu.VMEM((sources, rows, 1), F32),
                pltpu.VMEM((sources, rows, width), BF16),
                pltpu.VMEM((sources, rows, width), F32),
            ],
        ),
        compiler_params=pltpu.CompilerParams(vmem_limit_bytes=VMEM_LIMIT),
        cost_estimate=pl.CostEstimate(flops=30_000_000_000, bytes_accessed=30_000_000, transcendentals=0),
    )(base, tok, meta, w1, w3, w2)


def expert_backward(layer, capacity, groups, base, tok, grad, meta, w1, w3, w2):
    sources, width, tokens = tok.shape
    ff = w1.shape[3]
    rows = GROUP * capacity
    grad_shape = jax.ShapeDtypeStruct((groups * GROUP, width, ff), BF16)
    grad_spec = pl.BlockSpec((GROUP, width, ff), lambda g, base: (g, 0, 0))
    return pl.pallas_call(
        functools.partial(bwd_kernel, capacity),
        name=f"expert_bwd_{layer}",
        out_shape=(jax.ShapeDtypeStruct((sources, width, tokens), BF16), grad_shape, grad_shape, grad_shape),
        grid_spec=pltpu.PrefetchScalarGridSpec(
            num_scalar_prefetch=1,
            grid=(groups,),
            in_specs=[whole(), whole(), whole()] + weight_specs(layer, width, ff),
            out_specs=(whole(), grad_spec, grad_spec, grad_spec),
            scratch_shapes=[
                pltpu.VMEM((sources, width, tokens), F32),
                pltpu.VMEM((sources, rows, tokens), BF16),
                pltpu.VMEM((sources, rows, 1), F32),
                pltpu.VMEM((sources, rows, width), BF16),
                pltpu.VMEM((sources, rows, width), BF16),
            ],
        ),
        compiler_params=pltpu.CompilerParams(vmem_limit_bytes=VMEM_LIMIT),
        cost_estimate=pl.CostEstimate(flops=40_000_000_000, bytes_accessed=50_000_000, transcendentals=0),
    )(base, tok, grad, meta, w1, w3, w2)


def dense_forward(act, w_dense, ws_gate, ws_up):
    mixed = (act.astype(F32) + dot(w_dense, act, 0, 0)).astype(BF16)
    s_one = dot(ws_gate, mixed, 0, 0)
    s_three = dot(ws_up, mixed, 0, 0)
    shared_hidden = (jax.nn.silu(s_one) * s_three).astype(BF16)
    return mixed, s_one, s_three, shared_hidden


def dense_backward(grad_y, routed, saved, act, w_dense, ws_gate, ws_up, ws_down):
    mixed, s_one, s_three, shared_hidden = saved
    act_one, slope = silu_parts(s_one)
    g_ws_down = dot(shared_hidden, grad_y, 1, 1).astype(BF16)
    grad_shared = dot(ws_down, grad_y, 1, 0)
    grad_s_one = (grad_shared * s_three * slope).astype(BF16)
    grad_s_three = (grad_shared * act_one).astype(BF16)
    g_ws_gate = dot(mixed, grad_s_one, 1, 1).astype(BF16)
    g_ws_up = dot(mixed, grad_s_three, 1, 1).astype(BF16)
    grad_mixed = (grad_y.astype(F32) + routed.astype(F32) + dot(ws_gate, grad_s_one, 1, 0) + dot(ws_up, grad_s_three, 1, 0)).astype(BF16)
    g_w_dense = dot(act, grad_mixed, 1, 1).astype(BF16)
    grad_act = (grad_mixed.astype(F32) + dot(w_dense, grad_mixed, 1, 0)).astype(BF16)
    return grad_act, (g_w_dense, g_ws_gate, g_ws_up, g_ws_down)


def solution(mesh):
    ep_size = mesh.shape["ep"]
    dp_size = mesh.shape["dp"]
    tok_spec = P(ALL_AXES, None)
    route_spec = P(None, ALL_AXES, None)
    exp_spec = P(None, "ep", None, None)
    repl_spec = P(None, None, None)

    def body(act_in, grad_out, slot_ids, gate_vals, w_dense, w_gate, w_up, w_down, ws_gate, ws_up, ws_down):
        layers, local_exp = w_gate.shape[:2]
        tokens = act_in.shape[0]
        top = slot_ids.shape[2]
        own = local_exp // dp_size
        groups = own // GROUP
        capacity = 2 * tokens * top // (local_exp * ep_size)
        dp = lax.axis_index("dp")
        base = jnp.stack([lax.axis_index("ep") * local_exp + dp * own, dp * groups]).astype(jnp.int32)
        w_down_t = jnp.swapaxes(w_down, 2, 3)
        meta = jnp.concatenate([jnp.swapaxes(slot_ids, 1, 2).astype(F32), jnp.swapaxes(gate_vals, 1, 2)], axis=1)
        meta = lax.all_gather(meta, ALL_AXES)

        def gather(x):
            return lax.all_gather(x, ALL_AXES)

        def scatter(x):
            return lax.psum_scatter(x, ALL_AXES, scatter_dimension=0, tiled=False)

        x1 = act_in.T
        grad_y2 = grad_out.T
        saved1 = dense_forward(x1, w_dense[0], ws_gate[0], ws_up[0])
        tok1 = gather(saved1[0])
        grad2_all = gather(grad_y2)
        part = expert_forward(0, capacity, groups, base, tok1, meta[:, 0], w_gate, w_up, w_down_t)
        routed = scatter(part)
        x2 = (saved1[0].astype(F32) + routed + dot(ws_down[0], saved1[3], 0, 0)).astype(BF16)
        saved2 = dense_forward(x2, w_dense[1], ws_gate[1], ws_up[1])
        tok2 = gather(saved2[0])
        back2, d1_2, d3_2, d2_2 = expert_backward(1, capacity, groups, base, tok2, grad2_all, meta[:, 1], w_gate, w_up, w_down_t)
        routed2 = scatter(back2)
        grad_y1, dense2 = dense_backward(grad_y2, routed2, saved2, x2, w_dense[1], ws_gate[1], ws_up[1], ws_down[1])
        grad1_all = gather(grad_y1)
        back1, d1_1, d3_1, d2_1 = expert_backward(0, capacity, groups, base, tok1, grad1_all, meta[:, 0], w_gate, w_up, w_down_t)
        routed1 = scatter(back1)
        grad_x, dense1 = dense_backward(grad_y1, routed1, saved1, x1, w_dense[0], ws_gate[0], ws_up[0], ws_down[0])

        def join(first, second):
            return jnp.stack([lax.all_gather(first, "dp", tiled=True), lax.all_gather(second, "dp", tiled=True)])

        dense_out = [jnp.stack([lax.psum(a, ALL_AXES), lax.psum(b, ALL_AXES)]) for a, b in zip(dense1, dense2)]
        g_gate = join(d1_1, d1_2)
        g_up = join(d3_1, d3_2)
        g_down = jnp.swapaxes(join(d2_1, d2_2), 2, 3)
        return (grad_x.T, dense_out[0], g_gate, g_up, g_down, dense_out[1], dense_out[2], dense_out[3])

    return jax.shard_map(body, mesh=mesh, in_specs=(tok_spec, tok_spec, route_spec, route_spec, repl_spec, exp_spec, exp_spec, exp_spec, repl_spec, repl_spec, repl_spec), out_specs=(tok_spec, repl_spec, exp_spec, exp_spec, exp_spec, repl_spec, repl_spec, repl_spec), check_vma=False)
```

```python
import functools
import jax
import jax.numpy as jnp
from jax import lax
from jax.experimental import pallas as pl
from jax.experimental.pallas import tpu as pltpu
from jax.sharding import PartitionSpec as P

ALL_AXES = ("ep", "dp")
GROUP = 8
VMEM_LIMIT = 62 * 1024 * 1024
F32 = jnp.float32
BF16 = jnp.bfloat16


def dot(left, right, left_dim, right_dim):
    return lax.dot_general(left, right, (((left_dim,), (right_dim,)), ((), ())), preferred_element_type=F32)


def silu_parts(pre_act):
    sigma = jax.nn.sigmoid(pre_act)
    return pre_act * sigma, sigma * (1.0 + pre_act * (1.0 - sigma))


def route(meta_ref, src, first_expert, capacity, pick_ref, gate_ref):
    top = meta_ref.shape[1] // 2
    tokens = meta_ref.shape[2]
    slots = meta_ref[src, 0:top, :].astype(jnp.int32)
    gates = meta_ref[src, top : 2 * top, :]
    expert = slots // capacity - first_expert
    row = slots % capacity
    which = lax.broadcasted_iota(jnp.int32, (GROUP, tokens), 0)
    row_of = jnp.full((GROUP, tokens), -1, jnp.int32)
    gate_of = jnp.zeros((GROUP, tokens), F32)
    for j in range(top):
        hit = expert[j : j + 1, :] == which
        row_of = jnp.where(hit, row[j : j + 1, :], row_of)
        gate_of = jnp.where(hit, gates[j : j + 1, :], gate_of)
    rows = lax.broadcasted_iota(jnp.int32, (capacity, tokens), 0)
    for k in range(GROUP):
        hit = row_of[k : k + 1, :] == rows
        pick_ref[src, k * capacity : (k + 1) * capacity, :] = jnp.where(hit, 1.0, 0.0).astype(BF16)
        gate_ref[src, k * capacity : (k + 1) * capacity, :] = jnp.sum(jnp.where(hit, gate_of[k : k + 1, :], 0.0), axis=1, keepdims=True)


def fwd_kernel(capacity, base_ref, tok_ref, meta_ref, w1_ref, w3_ref, w2_ref, out_ref, pick_ref, gate_ref, x_ref, o_ref):
    group = pl.program_id(0)
    sources = tok_ref.shape[0]
    width = tok_ref.shape[1]
    rows = GROUP * capacity

    @pl.when(group == 0)
    def _():
        def clear(src, carry):
            out_ref[src] = jnp.zeros(out_ref.shape[1:], F32)
            return carry

        lax.fori_loop(0, sources, clear, 0)

    def dispatch(src, carry):
        route(meta_ref, src, base_ref[0] + group * GROUP, capacity, pick_ref, gate_ref)
        x_ref[src] = dot(pick_ref[src], tok_ref[src], 1, 1).astype(BF16)
        return carry

    lax.fori_loop(0, sources, dispatch, 0)

    def expert(k, carry):
        here = pl.ds(pl.multiple_of(k * capacity, capacity), capacity)
        x = x_ref[:, here, :].reshape(sources * capacity, width)
        a_one = dot(x, w1_ref[k], 1, 0)
        a_three = dot(x, w3_ref[k], 1, 0)
        hidden = (jax.nn.silu(a_one) * a_three).astype(BF16)
        out = dot(hidden, w2_ref[k], 1, 1).astype(BF16).astype(F32)
        gate = gate_ref[:, here, :].reshape(sources * capacity, 1)
        o_ref[:, here, :] = (gate * out).reshape(sources, capacity, width)
        return carry

    lax.fori_loop(0, GROUP, expert, 0)

    def combine(src, carry):
        rest = o_ref[src].T
        pick = pick_ref[src]
        total = out_ref[src]
        for _ in range(3):
            part = rest.astype(BF16)
            total = total + dot(part, pick, 1, 0)
            rest = rest - part.astype(F32)
        out_ref[src] = total
        return carry

    lax.fori_loop(0, sources, combine, 0)


def bwd_kernel(capacity, held, pieces, base_ref, tok_ref, meta_ref, w1_ref, w3_ref, w2_ref, *refs):
    piece_refs, refs = refs[:pieces], refs[pieces + held :]
    out_ref, d1_ref, d3_ref, d2_ref, send_ref, sum_ref, grad_ref, pick_ref, gate_ref, x_ref, g_ref, sem = refs
    group = pl.program_id(0)
    sources = tok_ref.shape[0]
    width = tok_ref.shape[1]

    @pl.when(group == 0)
    def _():
        copies = [pltpu.make_async_copy(piece, grad_ref if pieces == 1 else grad_ref.at[n], sem.at[n]) for n, piece in enumerate(piece_refs)]
        for copy in copies:
            copy.start()

        def clear(src, carry):
            sum_ref[src] = jnp.zeros(sum_ref.shape[1:], F32)
            return carry

        lax.fori_loop(0, sources, clear, 0)
        for copy in copies:
            copy.wait()

    def dispatch(src, carry):
        route(meta_ref, src, base_ref[0] + group * GROUP, capacity, pick_ref, gate_ref)
        x_ref[src] = dot(pick_ref[src], tok_ref[src], 1, 1).astype(BF16)
        g_ref[src] = (gate_ref[src] * dot(pick_ref[src], grad_ref[src], 1, 1)).astype(BF16)
        return carry

    lax.fori_loop(0, sources, dispatch, 0)

    def expert(k, carry):
        here = pl.ds(pl.multiple_of(k * capacity, capacity), capacity)
        x = x_ref[:, here, :].reshape(sources * capacity, width)
        g = g_ref[:, here, :].reshape(sources * capacity, width)
        a_one = dot(x, w1_ref[k], 1, 0)
        a_three = dot(x, w3_ref[k], 1, 0)
        act, slope = silu_parts(a_one)
        hidden = (act * a_three).astype(BF16)
        grad_hidden = dot(g, w2_ref[k], 1, 0)
        grad_one = (grad_hidden * a_three * slope).astype(BF16)
        grad_three = (grad_hidden * act).astype(BF16)
        found = (dot(x, grad_one, 0, 0), dot(x, grad_three, 0, 0), dot(g, hidden, 0, 0))
        for i, (ref, value) in enumerate(zip((d1_ref, d3_ref, d2_ref), found)):
            ref[k] = value.astype(BF16)
            send_ref[i, k] = value.astype(BF16)
        back = dot(grad_one, w1_ref[k], 1, 1) + dot(grad_three, w3_ref[k], 1, 1)
        x_ref[:, here, :] = back.astype(BF16).reshape(sources, capacity, width)
        return carry

    lax.fori_loop(0, GROUP, expert, 0)

    def combine(src, carry):
        sum_ref[src] += dot(x_ref[src], pick_ref[src], 0, 0)
        return carry

    lax.fori_loop(0, sources, combine, 0)

    @pl.when(group == pl.num_programs(0) - 1)
    def _():
        def finish(src, carry):
            out_ref[src] = sum_ref[src].astype(BF16)
            return carry

        lax.fori_loop(0, sources, finish, 0)


def weight_specs(layer, width, ff):
    spec = pl.BlockSpec((None, GROUP, width, ff), lambda g, base: (layer, base[1] + g, 0, 0))
    return [spec, spec, spec]


def whole():
    return pl.BlockSpec(memory_space=pltpu.VMEM)


def expert_forward(layer, capacity, groups, base, tok, meta, w1, w3, w2):
    sources, width, tokens = tok.shape
    ff = w1.shape[3]
    rows = GROUP * capacity
    return pl.pallas_call(
        functools.partial(fwd_kernel, capacity),
        name=f"expert_fwd_{layer}",
        out_shape=jax.ShapeDtypeStruct((sources, width, tokens), F32),
        grid_spec=pltpu.PrefetchScalarGridSpec(
            num_scalar_prefetch=1,
            grid=(groups,),
            in_specs=[whole(), whole()] + weight_specs(layer, width, ff),
            out_specs=whole(),
            scratch_shapes=[
                pltpu.VMEM((sources, rows, tokens), BF16),
                pltpu.VMEM((sources, rows, 1), F32),
                pltpu.VMEM((sources, rows, width), BF16),
                pltpu.VMEM((sources, rows, width), F32),
            ],
        ),
        compiler_params=pltpu.CompilerParams(vmem_limit_bytes=VMEM_LIMIT),
        cost_estimate=pl.CostEstimate(flops=30_000_000_000, bytes_accessed=30_000_000, transcendentals=0),
    )(base, tok, meta, w1, w3, w2)


def expert_backward(layer, capacity, groups, base, tok, grads, meta, w1, w3, w2, held):
    sources, width, tokens = tok.shape
    ff = w1.shape[3]
    rows = GROUP * capacity
    own = groups * GROUP
    pieces = len(grads)
    grad_shape = jax.ShapeDtypeStruct(w1.shape, BF16)
    grad_spec = pl.BlockSpec((None, GROUP, width, ff), lambda g, base: (layer, base[1] + g, 0, 0))
    return pl.pallas_call(
        functools.partial(bwd_kernel, capacity, len(held), pieces),
        name=f"expert_bwd_{layer}",
        out_shape=(jax.ShapeDtypeStruct((sources, width, tokens), BF16), grad_shape, grad_shape, grad_shape, jax.ShapeDtypeStruct((3, own, width, ff), BF16)),
        grid_spec=pltpu.PrefetchScalarGridSpec(
            num_scalar_prefetch=1,
            grid=(groups,),
            in_specs=[whole(), whole()] + weight_specs(layer, width, ff) + [pl.BlockSpec(memory_space=pl.ANY)] * (pieces + len(held)),
            out_specs=(whole(), grad_spec, grad_spec, grad_spec, pl.BlockSpec((3, GROUP, width, ff), lambda g, base: (0, g, 0, 0))),
            scratch_shapes=[
                pltpu.VMEM((sources, width, tokens), F32),
                pltpu.VMEM((sources, width, tokens), BF16),
                pltpu.VMEM((sources, rows, tokens), BF16),
                pltpu.VMEM((sources, rows, 1), F32),
                pltpu.VMEM((sources, rows, width), BF16),
                pltpu.VMEM((sources, rows, width), BF16),
                pltpu.SemaphoreType.DMA((pieces,)),
            ],
        ),
        input_output_aliases={6 + pieces + i: 1 + i for i in range(len(held))},
        compiler_params=pltpu.CompilerParams(vmem_limit_bytes=VMEM_LIMIT),
        cost_estimate=pl.CostEstimate(flops=40_000_000_000, bytes_accessed=50_000_000, transcendentals=0),
    )(base, tok, meta, w1, w3, w2, *grads, *held)


def neighbours():
    ep = lax.axis_index("ep")
    dp = lax.axis_index("dp")
    return ({"ep": ep + 1 - 2 * (ep % 2), "dp": dp}, {"ep": (ep + 2) % 4, "dp": dp}, {"ep": ep, "dp": 1 - dp})


def greet(devices):
    barrier = pltpu.get_barrier_semaphore()
    for device in devices:
        pl.semaphore_signal(barrier, inc=1, device_id=device, device_id_type=pl.DeviceIdType.MESH)
    pl.semaphore_wait(barrier, len(devices))


def gather_kernel(count, *refs):
    own_refs, out_refs = refs[:count], refs[count : 2 * count]
    send_sem, recv_sem = refs[2 * count :]
    devices = neighbours()
    by_x, by_y, partner = devices
    greet(devices)

    def copy(which, n, source, target, half, device):
        rows = own_refs[which].shape[0]
        span = pl.ds(0, rows) if half is None else pl.ds(half * (rows // 2), rows // 2)
        block = own_refs[which].at[span] if source == 0 else out_refs[which].at[source, span]
        made = pltpu.make_async_remote_copy(
            src_ref=block,
            dst_ref=out_refs[which].at[target, span],
            send_sem=send_sem.at[which, n],
            recv_sem=recv_sem.at[which, n],
            device_id=device,
            device_id_type=pl.DeviceIdType.MESH,
        )
        made.start()
        return made

    made = []
    for which in range(count):
        made.append([
            copy(which, 0, 0, 1, 0, by_x),
            copy(which, 1, 0, 2, 1, by_y),
            copy(which, 2, 0, 1, 1, by_x),
            copy(which, 3, 0, 2, 0, by_y),
            copy(which, 4, 0, 4, None, partner),
        ])
    for which in range(count):
        out_refs[which][0] = own_refs[which][...]
    for which in range(count):
        steps = made[which]
        steps[0].wait_recv()
        steps.append(copy(which, 5, 1, 3, 0, by_y))
        steps[1].wait_recv()
        steps.append(copy(which, 6, 2, 3, 1, by_x))
        steps[2].wait_recv()
        steps.append(copy(which, 7, 1, 5, None, partner))
        steps[3].wait_recv()
        steps.append(copy(which, 8, 2, 6, None, partner))
    for which in range(count):
        steps = made[which]
        steps[5].wait_recv()
        steps.append(copy(which, 9, 3, 7, 0, partner))
        steps[6].wait_recv()
        steps.append(copy(which, 10, 3, 7, 1, partner))
    for which in range(count):
        for n in (4, 7, 8, 9, 10):
            made[which][n].wait_recv()
        for n in range(11):
            made[which][n].wait_send()


def gather_tokens(name, cid, arrays):
    count = len(arrays)
    out = pl.pallas_call(
        functools.partial(gather_kernel, count),
        name=name,
        out_shape=tuple(jax.ShapeDtypeStruct((8,) + x.shape, x.dtype) for x in arrays),
        in_specs=[whole()] * count,
        out_specs=(whole(),) * count,
        scratch_shapes=[pltpu.SemaphoreType.DMA((count, 11)), pltpu.SemaphoreType.DMA((count, 11))],
        compiler_params=pltpu.CompilerParams(collective_id=cid, has_side_effects=True, vmem_limit_bytes=32 * 1024 * 1024),
        cost_estimate=pl.CostEstimate(flops=10_000_000_000, bytes_accessed=10_000_000, transcendentals=0),
    )(*arrays)
    return out


def reduce_kernel(part_ref, out_ref, pair_ref, stage_ref, relay_ref, last_ref, send_sem, recv_sem):
    devices = neighbours()
    by_x, by_y, partner = devices
    greet(devices)
    rows = part_ref.shape[1]
    half = rows // 2
    low, high, full = pl.ds(0, half), pl.ds(half, half), pl.ds(0, rows)
    wire = part_ref.dtype

    def copy(n, source, target, device):
        made = pltpu.make_async_remote_copy(
            src_ref=source,
            dst_ref=target,
            send_sem=send_sem.at[n],
            recv_sem=recv_sem.at[n],
            device_id=device,
            device_id_type=pl.DeviceIdType.MESH,
        )
        made.start()
        return made

    def chip_sum(i, span):
        return part_ref[i, span, :].astype(F32) + pair_ref[i, span, :].astype(F32)

    steps = {i: copy(i, part_ref.at[4 + i], pair_ref.at[i], partner) for i in (3, 1, 2, 0)}
    steps[3].wait_recv()
    stage_ref[0, low, :] = chip_sum(3, low).astype(wire)
    steps[4] = copy(4, stage_ref.at[0, low], relay_ref.at[0], by_x)
    stage_ref[0, high, :] = chip_sum(3, high).astype(wire)
    steps[5] = copy(5, stage_ref.at[0, high], relay_ref.at[1], by_y)
    steps[1].wait_recv()
    stage_ref[1, low, :] = chip_sum(1, low).astype(wire)
    steps[6] = copy(6, stage_ref.at[1, low], last_ref.at[0, low], by_x)
    steps[2].wait_recv()
    stage_ref[2, high, :] = chip_sum(2, high).astype(wire)
    steps[7] = copy(7, stage_ref.at[2, high], last_ref.at[1, high], by_y)
    steps[5].wait_recv()
    stage_ref[1, high, :] = (chip_sum(1, high) + relay_ref[1].astype(F32)).astype(wire)
    steps[8] = copy(8, stage_ref.at[1, high], last_ref.at[0, high], by_x)
    steps[4].wait_recv()
    stage_ref[2, low, :] = (chip_sum(2, low) + relay_ref[0].astype(F32)).astype(wire)
    steps[9] = copy(9, stage_ref.at[2, low], last_ref.at[1, low], by_y)
    steps[0].wait_recv()
    out_ref[...] = chip_sum(0, full)
    steps[6].wait_recv()
    steps[7].wait_recv()
    steps[8].wait_recv()
    steps[9].wait_recv()
    out_ref[...] += last_ref[0].astype(F32) + last_ref[1].astype(F32)
    for n in range(10):
        steps[n].wait_send()


def reduce_tokens(name, cid, part):
    rows, tokens = part.shape[1:]
    return pl.pallas_call(
        reduce_kernel,
        name=name,
        out_shape=jax.ShapeDtypeStruct((rows, tokens), F32),
        in_specs=[whole()],
        out_specs=whole(),
        scratch_shapes=[
            pltpu.VMEM((4, rows, tokens), part.dtype),
            pltpu.VMEM((3, rows, tokens), part.dtype),
            pltpu.VMEM((2, rows // 2, tokens), part.dtype),
            pltpu.VMEM((2, rows, tokens), part.dtype),
            pltpu.SemaphoreType.DMA((10,)),
            pltpu.SemaphoreType.DMA((10,)),
        ],
        compiler_params=pltpu.CompilerParams(collective_id=cid, has_side_effects=True, vmem_limit_bytes=40 * 1024 * 1024),
        cost_estimate=pl.CostEstimate(flops=10_000_000_000, bytes_accessed=10_000_000, transcendentals=0),
    )(part)


def send_over(x, flip):
    return lax.ppermute(x, "ep", [(i, i ^ flip) for i in range(4)])


def swap_cores(x):
    return lax.ppermute(x, "dp", [(0, 1), (1, 0)])


def sum_start(x):
    half = x.shape[0] // 2
    dp = lax.axis_index("dp")
    mine = lax.dynamic_slice_in_dim(x, dp * half, half, 0)
    other = lax.dynamic_slice_in_dim(x, (1 - dp) * half, half, 0)
    chip = (mine.astype(F32) + swap_cores(other).astype(F32)).astype(BF16)
    return [chip, send_over(chip, 1), send_over(chip, 2), send_over(chip, 3)]


def sum_finish(parts):
    total = sum(part.astype(F32) for part in parts).astype(BF16)
    other = swap_cores(total)
    first = lax.axis_index("dp") == 0
    return jnp.concatenate([jnp.where(first, total, other), jnp.where(first, other, total)], axis=0)


def place_kernel(base_ref, recv_ref, *refs):
    for i in range(3):
        refs[3 + i][...] = recv_ref[i]


def place(layer, groups, base, recv, held):
    width, ff = recv.shape[2:]
    spec = pl.BlockSpec((None, GROUP, width, ff), lambda g, base: (layer, base[2] + g, 0, 0))
    shape = jax.ShapeDtypeStruct(held[0].shape, BF16)
    return pl.pallas_call(
        place_kernel,
        name=f"place_{layer}",
        out_shape=(shape, shape, shape),
        grid_spec=pltpu.PrefetchScalarGridSpec(
            num_scalar_prefetch=1,
            grid=(groups,),
            in_specs=[pl.BlockSpec((3, GROUP, width, ff), lambda g, base: (0, g, 0, 0))] + [pl.BlockSpec(memory_space=pl.ANY)] * 3,
            out_specs=(spec, spec, spec),
        ),
        input_output_aliases={2: 0, 3: 1, 4: 2},
        compiler_params=pltpu.CompilerParams(vmem_limit_bytes=VMEM_LIMIT),
        cost_estimate=pl.CostEstimate(flops=5_000_000_000, bytes_accessed=2 * recv.size * 2, transcendentals=0),
    )(base, recv, *held)


def dense_forward(act, w_dense, ws_gate, ws_up):
    mixed = (act.astype(F32) + dot(w_dense, act, 0, 0)).astype(BF16)
    s_one = dot(ws_gate, mixed, 0, 0)
    s_three = dot(ws_up, mixed, 0, 0)
    shared_hidden = (jax.nn.silu(s_one) * s_three).astype(BF16)
    return mixed, s_one, s_three, shared_hidden


def shared_backward(grad_y, saved, ws_gate, ws_up, ws_down):
    mixed, s_one, s_three, shared_hidden = saved
    act_one, slope = silu_parts(s_one)
    grad_shared = dot(ws_down, grad_y, 1, 0)
    grad_s_one = (grad_shared * s_three * slope).astype(BF16)
    grad_s_three = (grad_shared * act_one).astype(BF16)
    g_ws_down = dot(grad_y, shared_hidden, 1, 1).astype(BF16)
    g_ws_gate = dot(mixed, grad_s_one, 1, 1).astype(BF16)
    g_ws_up = dot(mixed, grad_s_three, 1, 1).astype(BF16)
    back = dot(ws_gate, grad_s_one, 1, 0) + dot(ws_up, grad_s_three, 1, 0)
    return back, [g_ws_gate, g_ws_up, g_ws_down]


def dense_finish(grad_y, routed, shared, act, w_dense):
    grad_mixed = (grad_y.astype(F32) + routed + shared).astype(BF16)
    grad_act = (grad_mixed.astype(F32) + dot(w_dense, grad_mixed, 1, 0)).astype(BF16)
    return grad_act, dot(act, grad_mixed, 1, 1).astype(BF16)


def dense_backward(grad_y, routed, saved, act, w_dense, ws_gate, ws_up, ws_down):
    back, parts = shared_backward(grad_y, saved, ws_gate, ws_up, ws_down)
    grad_act, g_w_dense = dense_finish(grad_y, routed, back, act, w_dense)
    return grad_act, [g_w_dense] + parts


def solution(mesh):
    ep_size = mesh.shape["ep"]
    dp_size = mesh.shape["dp"]
    tok_spec = P(ALL_AXES, None)
    route_spec = P(None, ALL_AXES, None)
    exp_spec = P(None, "ep", None, None)
    repl_spec = P(None, None, None)

    def body(act_in, grad_out, slot_ids, gate_vals, w_dense, w_gate, w_up, w_down, ws_gate, ws_up, ws_down):
        layers, local_exp = w_gate.shape[:2]
        tokens = act_in.shape[0]
        top = slot_ids.shape[2]
        own = local_exp // dp_size
        groups = own // GROUP
        capacity = 2 * tokens * top // (local_exp * ep_size)
        dp = lax.axis_index("dp")
        base = jnp.stack([lax.axis_index("ep") * local_exp + dp * own, dp * groups, (dp_size - 1 - dp) * groups]).astype(jnp.int32)
        w_down_t = jnp.swapaxes(w_down, 2, 3)
        meta = jnp.concatenate([jnp.swapaxes(slot_ids, 1, 2).astype(F32), jnp.swapaxes(gate_vals, 1, 2)], axis=1)
        meta = meta.reshape(layers * 2 * top, tokens)

        x1 = act_in.T
        grad_y2 = grad_out.T
        saved1 = dense_forward(x1, w_dense[0], ws_gate[0], ws_up[0])
        tok1, metas = gather_tokens("gather_first", 0, [saved1[0], meta])
        tok1, grad_y2 = lax.optimization_barrier((tok1, grad_y2))
        grads2 = [grad_y2, send_over(grad_y2, 1), send_over(grad_y2, 2), send_over(grad_y2, 3)]
        grads2 = grads2 + [swap_cores(x) for x in grads2]
        meta1, meta2 = metas[:, : 2 * top], metas[:, 2 * top :]
        part = expert_forward(0, capacity, groups, base, tok1, meta1, w_gate, w_up, w_down_t)
        routed = reduce_tokens("reduce_fwd", 1, part)
        x2 = (saved1[0].astype(F32) + routed + dot(ws_down[0], saved1[3], 0, 0)).astype(BF16)
        saved2 = dense_forward(x2, w_dense[1], ws_gate[1], ws_up[1])
        (tok2,) = gather_tokens("gather_fwd", 2, [saved2[0]])
        back2, *held, send2 = expert_backward(1, capacity, groups, base, tok2, grads2, meta2, w_gate, w_up, w_down_t, [])
        recv2 = swap_cores(send2)
        routed2 = reduce_tokens("reduce_bwd_1", 3, back2)
        grad_y1, dense2 = dense_backward(grad_y2, routed2, saved2, x2, w_dense[1], ws_gate[1], ws_up[1], ws_down[1])
        (grad1_all,) = gather_tokens("gather_bwd", 4, [grad_y1])
        shared1, parts1 = shared_backward(grad_y1, saved1, ws_gate[0], ws_up[0], ws_down[0])
        ff = ws_gate.shape[2]
        width = w_dense.shape[1]
        early = jnp.concatenate(dense2 + parts1 + [jnp.zeros((width, -(width + 6 * ff) % 128), BF16)], axis=1)
        early = sum_start(early)
        held = place(1, groups, base, recv2, held)
        back1, *held, send1 = expert_backward(0, capacity, groups, base, tok1, [grad1_all], meta1, w_gate, w_up, w_down_t, held)
        recv1 = swap_cores(send1)
        routed1 = reduce_tokens("reduce_bwd_0", 5, back1)
        grad_x, g_w_dense1 = dense_finish(grad_y1, routed1, shared1, x1, w_dense[0])
        late = sum_start(g_w_dense1)
        g_gate, g_up, g_down = place(0, groups, base, recv1, held)
        g_down = jnp.swapaxes(g_down, 2, 3)
        early = sum_finish(early)
        late = sum_finish(late)
        g_dense = jnp.stack([late, early[:, :width]])
        shared = [jnp.stack([early[:, width + (3 + i) * ff : width + (4 + i) * ff], early[:, width + i * ff : width + (i + 1) * ff]]) for i in range(3)]
        return (grad_x.T, g_dense, g_gate, g_up, g_down, shared[0], shared[1], jnp.swapaxes(shared[2], 1, 2))

    return jax.shard_map(body, mesh=mesh, in_specs=(tok_spec, tok_spec, route_spec, route_spec, repl_spec, exp_spec, exp_spec, exp_spec, repl_spec, repl_spec, repl_spec), out_specs=(tok_spec, repl_spec, exp_spec, exp_spec, exp_spec, repl_spec, repl_spec, repl_spec), check_vma=False)
```

```python
import functools
import jax
import jax.numpy as jnp
from jax import lax
from jax.experimental import pallas as pl
from jax.experimental.pallas import tpu as pltpu
from jax.sharding import PartitionSpec as P

ALL_AXES = ("ep", "dp")
GROUP = 8
UNROLL = 8
VMEM_LIMIT = 62 * 1024 * 1024
F32 = jnp.float32
BF16 = jnp.bfloat16


def dot(left, right, left_dim, right_dim):
    return lax.dot_general(left, right, (((left_dim,), (right_dim,)), ((), ())), preferred_element_type=F32)


def silu_parts(pre_act):
    sigma = jax.nn.sigmoid(pre_act)
    return pre_act * sigma, sigma * (1.0 + pre_act * (1.0 - sigma))


def route(meta_ref, src, first_expert, capacity, pick_ref, slot, tok_ref):
    top = meta_ref.shape[1] // 2
    tokens = meta_ref.shape[2]
    width = tok_ref.shape[1] - 4 * GROUP
    slots = meta_ref[src, 0:top, :].astype(jnp.int32)
    gates = meta_ref[src, top : 2 * top, :]
    expert = slots // capacity - first_expert
    row = (slots % capacity).astype(F32)
    which = lax.broadcasted_iota(jnp.int32, (GROUP, tokens), 0)
    row_of = jnp.full((GROUP, tokens), -1.0, F32)
    gate_of = jnp.zeros((GROUP, tokens), F32)
    for j in range(top):
        hit = expert[j : j + 1, :] == which
        row_of = jnp.where(hit, row[j : j + 1, :], row_of)
        gate_of = jnp.where(hit, gates[j : j + 1, :], gate_of)
    high = gate_of.astype(BF16)
    rest = gate_of - high.astype(F32)
    middle = rest.astype(BF16)
    low = (rest - middle.astype(F32)).astype(BF16)
    tok_ref[src, width : width + 4 * GROUP, :] = jnp.concatenate([high, middle, low, jnp.zeros_like(low)], axis=0)
    step = 16
    rows = lax.broadcasted_iota(jnp.int32, (step, tokens), 0).astype(F32).astype(BF16)
    for k in range(GROUP):
        wanted = jnp.broadcast_to(row_of[k : k + 1, :], (step, tokens)).astype(BF16)
        for h in range(capacity // step):
            hit = wanted == rows + jnp.asarray(h * step, BF16)
            start = k * capacity + h * step
            pick_ref[slot, src, start : start + step, :] = jnp.where(hit, jnp.asarray(1, BF16), jnp.asarray(0, BF16))


def build_rows(capacity, src, slot, pick_ref, tok_ref, gate_ref, x_ref):
    width = x_ref.shape[2]
    found = dot(pick_ref[slot, src], tok_ref[src], 1, 1)
    x_ref[src] = found[:, :width].astype(BF16)
    gates = []
    for k in range(GROUP):
        rows = found[k * capacity : (k + 1) * capacity, :]
        gates.append(rows[:, width + k : width + k + 1] + rows[:, width + GROUP + k : width + GROUP + k + 1] + rows[:, width + 2 * GROUP + k : width + 2 * GROUP + k + 1])
    gate = jnp.concatenate(gates, axis=0)
    gate_ref[src] = gate
    return gate


def schedule(groups, sources, begin, wait, dispatch, expert, combine, finish):
    group = pl.program_id(0)

    @pl.when(group == 0)
    def _():
        begin()

        def first(src, carry):
            wait(src)
            dispatch(src)
            return carry

        lax.fori_loop(0, sources, first, 0)

    @pl.when((group > 0) & (group < groups))
    def _():
        def middle(src, carry):
            combine(src)
            dispatch(src)
            return carry

        lax.fori_loop(0, sources, middle, 0)

    @pl.when(group < groups)
    def _():
        def one(k, carry):
            expert(k)
            return carry

        lax.fori_loop(0, GROUP, one, 0, unroll=UNROLL)

    @pl.when(group == groups)
    def _():
        def last(src, carry):
            finish(src)
            return carry

        lax.fori_loop(0, sources, last, 0)


def fwd_kernel(capacity, groups, base_ref, meta_ref, w1_ref, w3_ref, w2_ref, tokens_ref, out_ref, sum_ref, tok_ref, pick_ref, gate_ref, x_ref, o_ref, sem, out_sem):
    group = pl.program_id(0)
    sources = tok_ref.shape[0]
    width = x_ref.shape[2]
    now = group % 2
    before = 1 - now

    def load(src):
        return pltpu.make_async_copy(tokens_ref.at[src], tok_ref.at[src, pl.ds(0, width)], sem.at[src])

    def begin():
        for src in range(sources):
            load(src).start()

    def dispatch(src):
        route(meta_ref, src, base_ref[0] + group * GROUP, capacity, pick_ref, now, tok_ref)
        build_rows(capacity, src, now, pick_ref, tok_ref, gate_ref, x_ref)

    def expert(k):
        here = pl.ds(pl.multiple_of(k * capacity, capacity), capacity)
        x = x_ref[:, here, :].reshape(sources * capacity, width)
        ff = w1_ref.shape[2]
        a = dot(x, jnp.concatenate([w1_ref[k], w3_ref[k]], axis=1), 1, 0)
        hidden = (jax.nn.silu(a[:, :ff]) * a[:, ff:]).astype(BF16)
        out = dot(hidden, w2_ref[k], 1, 1).astype(BF16).astype(F32)
        gate = gate_ref[:, here, :].reshape(sources * capacity, 1)
        o_ref[:, here, :] = (gate * out).reshape(sources, capacity, width)

    def added(src):
        rest = o_ref[src].T
        pick = pick_ref[before, src]
        parts = []
        for _ in range(3):
            parts.append(rest.astype(BF16))
            rest = rest - parts[-1].astype(F32)
        return dot(parts[0], pick, 1, 0) + dot(parts[1], pick, 1, 0) + dot(parts[2], pick, 1, 0)

    def combine(src):
        @pl.when(group == 1)
        def _():
            sum_ref[src] = jnp.zeros(sum_ref.shape[1:], F32)

        sum_ref[src] += added(src)

    def store(src):
        return pltpu.make_async_copy(sum_ref.at[src], out_ref.at[src], out_sem.at[src])

    def finish(src):
        sum_ref[src] += added(src)
        store(src).start()

    schedule(groups, sources, begin, lambda src: load(src).wait(), dispatch, expert, combine, finish)

    @pl.when(group == groups)
    def _():
        for src in range(sources):
            store(src).wait()


def bwd_kernel(layer, capacity, groups, held, pieces, base_ref, meta_ref, w1_ref, w3_ref, w2_ref, tokens_ref, *refs):
    piece_refs, other_refs, refs = refs[:pieces], refs[pieces : pieces + held], refs[pieces + held :]
    out_ref, d1_ref, d3_ref, d2_ref, send_ref, sum_ref, tok_ref, grad_ref, pick_ref, gate_ref, x_ref, g_ref, r_ref, d_ref, sem, grad_sem, out_sem, d_sem = refs[:18]
    d_refs = (d1_ref, d3_ref, d2_ref)
    group = pl.program_id(0)
    sources = tok_ref.shape[0]
    width = x_ref.shape[2]
    now = group % 2
    before = 1 - now

    def load(src):
        return pltpu.make_async_copy(tokens_ref.at[src], tok_ref.at[src, pl.ds(0, width)], sem.at[src])

    def load_grad(src):
        piece = piece_refs[0].at[src] if pieces == 1 else piece_refs[src]
        return pltpu.make_async_copy(piece, grad_ref.at[src], grad_sem.at[src])

    def begin():
        for src in range(sources):
            load(src).start()
            load_grad(src).start()

    def wait(src):
        load(src).wait()
        pltpu.make_async_copy(grad_ref.at[src], grad_ref.at[src], grad_sem.at[src]).wait()

    def dispatch(src):
        route(meta_ref, src, base_ref[0] + group * GROUP, capacity, pick_ref, now, tok_ref)
        gate = build_rows(capacity, src, now, pick_ref, tok_ref, gate_ref, x_ref)
        g_ref[src] = (gate * dot(pick_ref[now, src], grad_ref[src], 1, 1)).astype(BF16)

    def expert(k):
        here = pl.ds(pl.multiple_of(k * capacity, capacity), capacity)
        x = x_ref[:, here, :].reshape(sources * capacity, width)
        g = g_ref[:, here, :].reshape(sources * capacity, width)
        ff = w1_ref.shape[2]
        both = jnp.concatenate([w1_ref[k], w3_ref[k]], axis=1)
        a = dot(x, both, 1, 0)
        a_three = a[:, ff:]
        act, slope = silu_parts(a[:, :ff])
        hidden = (act * a_three).astype(BF16)
        grad_hidden = dot(g, w2_ref[k], 1, 0)
        grad_one = (grad_hidden * a_three * slope).astype(BF16)
        grad_three = (grad_hidden * act).astype(BF16)
        grads = jnp.concatenate([grad_one, grad_three], axis=1)
        r_ref[:, here, :] = dot(grads, both, 1, 1).astype(BF16).reshape(sources, capacity, width)
        d13 = dot(x, grads, 0, 0).astype(BF16)
        d2 = dot(g, hidden, 0, 0).astype(BF16)
        for i, value in enumerate((d13[:, :ff], d13[:, ff:], d2)):
            d_ref[now, i, k] = value

    def added(src):
        return dot(r_ref[src], pick_ref[before, src], 0, 0)

    def combine(src):
        @pl.when(group == 1)
        def _():
            sum_ref[src] = jnp.zeros(sum_ref.shape[1:], F32)

        sum_ref[src] += added(src)

    def store(src):
        return pltpu.make_async_copy(grad_ref.at[src], out_ref.at[src], out_sem.at[src])

    def finish(src):
        grad_ref[src] = (sum_ref[src] + added(src)).astype(BF16)
        store(src).start()

    def experts_at(start, step):
        return pl.ds(pl.multiple_of((start + step) * GROUP, GROUP), GROUP)

    def d_stores(step):
        slot = step % 2
        made = [pltpu.make_async_copy(d_ref.at[slot, i], d_refs[i].at[layer, experts_at(base_ref[1], step)], d_sem.at[slot, i]) for i in range(3)]
        return made + [pltpu.make_async_copy(d_ref.at[slot], send_ref.at[:, experts_at(0, step)], d_sem.at[slot, 3])]

    def other_load(step):
        return pltpu.make_async_copy(other_refs[0].at[:, experts_at(0, step)], refs[18].at[step % 2], refs[19].at[step % 2, 3])

    def other_stores(step):
        slot = step % 2
        return [pltpu.make_async_copy(refs[18].at[slot, i], d_refs[i].at[1 - layer, experts_at(base_ref[2], step)], refs[19].at[slot, i]) for i in range(3)]

    def start_all(copies):
        for copy in copies:
            copy.start()

    def wait_all(copies):
        for copy in copies:
            copy.wait()

    @pl.when(group >= 2)
    def _():
        wait_all(d_stores(group - 2))
        if held:
            wait_all(other_stores(group - 2))

    if held:
        @pl.when(group >= 1)
        def _():
            other_load(group - 1).wait()
            start_all(other_stores(group - 1))

        @pl.when(group < groups)
        def _():
            other_load(group).start()

    schedule(groups, sources, begin, wait, dispatch, expert, combine, finish)

    @pl.when(group < groups)
    def _():
        start_all(d_stores(group))

    @pl.when(group == groups)
    def _():
        wait_all(d_stores(group - 1))
        if held:
            wait_all(other_stores(group - 1))
        for src in range(sources):
            store(src).wait()


def weight_specs(layer, groups, width, ff):
    spec = pl.BlockSpec((None, GROUP, width, ff), lambda g, base: (layer, base[1] + jnp.minimum(g, groups - 1), 0, 0))
    return [spec, spec, spec]


def whole():
    return pl.BlockSpec(memory_space=pltpu.VMEM)


def anywhere():
    return pl.BlockSpec(memory_space=pl.ANY)


def expert_forward(layer, capacity, groups, base, tok, meta, w1, w3, w2):
    sources, width, tokens = tok.shape
    ff = w1.shape[3]
    rows = GROUP * capacity
    return pl.pallas_call(
        functools.partial(fwd_kernel, capacity, groups),
        out_shape=jax.ShapeDtypeStruct((sources, width, tokens), F32),
        grid_spec=pltpu.PrefetchScalarGridSpec(
            num_scalar_prefetch=1,
            grid=(groups + 1,),
            in_specs=[whole()] + weight_specs(layer, groups, width, ff) + [anywhere()],
            out_specs=anywhere(),
            scratch_shapes=[
                pltpu.VMEM((sources, width, tokens), F32),
                pltpu.VMEM((sources, width + 4 * GROUP, tokens), BF16),
                pltpu.VMEM((2, sources, rows, tokens), BF16),
                pltpu.VMEM((sources, rows, 1), F32),
                pltpu.VMEM((sources, rows, width), BF16),
                pltpu.VMEM((sources, rows, width), F32),
                pltpu.SemaphoreType.DMA((sources,)),
                pltpu.SemaphoreType.DMA((sources,)),
            ],
        ),
        compiler_params=pltpu.CompilerParams(vmem_limit_bytes=VMEM_LIMIT),
        cost_estimate=pl.CostEstimate(flops=30_000_000_000, bytes_accessed=30_000_000, transcendentals=0),
    )(base, meta, w1, w3, w2, tok)


def expert_backward(layer, capacity, groups, base, tok, grads, meta, w1, w3, w2, held):
    sources, width, tokens = tok.shape
    ff = w1.shape[3]
    rows = GROUP * capacity
    own = groups * GROUP
    pieces = len(grads)
    grad_shape = jax.ShapeDtypeStruct(w1.shape, BF16)
    block = pltpu.VMEM((2, 3, GROUP, width, ff), BF16)
    more = [block, pltpu.SemaphoreType.DMA((2, 4))] if held else []
    return pl.pallas_call(
        functools.partial(bwd_kernel, layer, capacity, groups, len(held), pieces),
        out_shape=(jax.ShapeDtypeStruct((sources, width, tokens), BF16), grad_shape, grad_shape, grad_shape, jax.ShapeDtypeStruct((3, own, width, ff), BF16)),
        grid_spec=pltpu.PrefetchScalarGridSpec(
            num_scalar_prefetch=1,
            grid=(groups + 1,),
            in_specs=[whole()] + weight_specs(layer, groups, width, ff) + [anywhere()] * (1 + pieces + len(held)),
            out_specs=(anywhere(),) * 5,
            scratch_shapes=[
                pltpu.VMEM((sources, width, tokens), F32),
                pltpu.VMEM((sources, width + 4 * GROUP, tokens), BF16),
                pltpu.VMEM((sources, width, tokens), BF16),
                pltpu.VMEM((2, sources, rows, tokens), BF16),
                pltpu.VMEM((sources, rows, 1), F32),
                pltpu.VMEM((sources, rows, width), BF16),
                pltpu.VMEM((sources, rows, width), BF16),
                pltpu.VMEM((sources, rows, width), BF16),
                block,
                pltpu.SemaphoreType.DMA((sources,)),
                pltpu.SemaphoreType.DMA((sources,)),
                pltpu.SemaphoreType.DMA((sources,)),
                pltpu.SemaphoreType.DMA((2, 4)),
            ]
            + more,
        ),
        input_output_aliases={7 + pieces + i: 1 + i for i in range(len(held) - 1)},
        compiler_params=pltpu.CompilerParams(vmem_limit_bytes=VMEM_LIMIT),
        cost_estimate=pl.CostEstimate(flops=40_000_000_000, bytes_accessed=50_000_000, transcendentals=0),
    )(base, meta, w1, w3, w2, tok, *grads, *held)


def place_kernel(base_ref, recv_ref, *refs):
    for i in range(3):
        refs[3 + i][...] = recv_ref[i]


def place(layer, groups, base, recv, held):
    width, ff = recv.shape[2:]
    few = 8
    spec = pl.BlockSpec((None, few, width, ff), lambda g, base: (layer, base[2] * (GROUP // few) + g, 0, 0))
    shape = jax.ShapeDtypeStruct(held[0].shape, BF16)
    return pl.pallas_call(
        place_kernel,
        out_shape=(shape, shape, shape),
        grid_spec=pltpu.PrefetchScalarGridSpec(
            num_scalar_prefetch=1,
            grid=(groups * GROUP // few,),
            in_specs=[pl.BlockSpec((3, few, width, ff), lambda g, base: (0, g, 0, 0))] + [anywhere()] * 3,
            out_specs=(spec, spec, spec),
        ),
        input_output_aliases={2: 0, 3: 1, 4: 2},
        compiler_params=pltpu.CompilerParams(vmem_limit_bytes=VMEM_LIMIT),
        cost_estimate=pl.CostEstimate(flops=5_000_000_000, bytes_accessed=2 * recv.size * 2, transcendentals=0),
    )(base, recv, *held)


def neighbours():
    ep = lax.axis_index("ep")
    dp = lax.axis_index("dp")
    return ({"ep": ep + 1 - 2 * (ep % 2), "dp": dp}, {"ep": (ep + 2) % 4, "dp": dp}, {"ep": ep, "dp": 1 - dp})


def greet(devices):
    barrier = pltpu.get_barrier_semaphore()
    for device in devices:
        pl.semaphore_signal(barrier, inc=1, device_id=device, device_id_type=pl.DeviceIdType.MESH)
    pl.semaphore_wait(barrier, len(devices))


def gather_kernel(count, *refs):
    own_refs, out_refs, land_refs = refs[:count], refs[count : 2 * count], refs[2 * count : 3 * count]
    send_sem, recv_sem, store_sem = refs[3 * count :]
    by_x, by_y, partner = devices = neighbours()
    greet(devices)
    stores = []

    def copy(which, n, source, target, half, device):
        rows = own_refs[which].shape[0]
        span = pl.ds(0, rows) if half is None else pl.ds(half * (rows // 2), rows // 2)
        block = own_refs[which].at[span] if source == 0 else land_refs[which].at[source, span]
        made = pltpu.make_async_remote_copy(
            src_ref=block,
            dst_ref=land_refs[which].at[target, span],
            send_sem=send_sem.at[which, n],
            recv_sem=recv_sem.at[which, n],
            device_id=device,
            device_id_type=pl.DeviceIdType.MESH,
        )
        made.start()
        return made

    def store(which, slot):
        block = own_refs[which] if slot == 0 else land_refs[which].at[slot]
        made = pltpu.make_async_copy(block, out_refs[which].at[slot], store_sem.at[which, slot])
        made.start()
        stores.append(made)

    made = []
    for which in range(count):
        made.append([
            copy(which, 0, 0, 1, 0, by_x),
            copy(which, 1, 0, 2, 1, by_y),
            copy(which, 2, 0, 1, 1, by_x),
            copy(which, 3, 0, 2, 0, by_y),
            copy(which, 4, 0, 4, None, partner),
        ])
        store(which, 0)
    for which in range(count):
        steps = made[which]
        steps[0].wait_recv()
        steps.append(copy(which, 5, 1, 3, 0, by_y))
        steps[1].wait_recv()
        steps.append(copy(which, 6, 2, 3, 1, by_x))
        steps[2].wait_recv()
        steps.append(copy(which, 7, 1, 5, None, partner))
        store(which, 1)
        steps[3].wait_recv()
        steps.append(copy(which, 8, 2, 6, None, partner))
        store(which, 2)
        steps[4].wait_recv()
        store(which, 4)
    for which in range(count):
        steps = made[which]
        steps[5].wait_recv()
        steps.append(copy(which, 9, 3, 7, 0, partner))
        steps[6].wait_recv()
        steps.append(copy(which, 10, 3, 7, 1, partner))
        store(which, 3)
    for which in range(count):
        steps = made[which]
        steps[7].wait_recv()
        store(which, 5)
        steps[8].wait_recv()
        store(which, 6)
        steps[9].wait_recv()
        steps[10].wait_recv()
        store(which, 7)
        for n in range(11):
            steps[n].wait_send()
    for made_store in stores:
        made_store.wait()


def gather_tokens(cid, arrays):
    count = len(arrays)
    out = pl.pallas_call(
        functools.partial(gather_kernel, count),
        out_shape=tuple(jax.ShapeDtypeStruct((8,) + x.shape, x.dtype) for x in arrays),
        in_specs=[whole()] * count,
        out_specs=(anywhere(),) * count,
        scratch_shapes=[pltpu.VMEM((8,) + x.shape, x.dtype) for x in arrays] + [pltpu.SemaphoreType.DMA((count, n)) for n in (11, 11, 8)],
        compiler_params=pltpu.CompilerParams(collective_id=cid, has_side_effects=True, vmem_limit_bytes=VMEM_LIMIT),
        cost_estimate=pl.CostEstimate(flops=10_000_000_000, bytes_accessed=10_000_000, transcendentals=0),
    )(*arrays)
    return out


def reduce_kernel(extra, part_ref, *refs):
    extra_ref, refs = refs[:extra], refs[extra:]
    (out_ref, *other_ref), refs = refs[: 1 + extra], refs[1 + extra :]
    mine_ref, pair_ref, stage_ref, relay_ref, last_ref, send_sem, recv_sem, load_sem = refs
    devices = neighbours()
    by_x, by_y, partner = devices
    greet(devices)
    rows = part_ref.shape[1]
    half = rows // 2
    low, high, full = pl.ds(0, half), pl.ds(half, half), pl.ds(0, rows)
    wire = part_ref.dtype

    def copy(n, source, target, device):
        made = pltpu.make_async_remote_copy(
            src_ref=source,
            dst_ref=target,
            send_sem=send_sem.at[n],
            recv_sem=recv_sem.at[n],
            device_id=device,
            device_id_type=pl.DeviceIdType.MESH,
        )
        made.start()
        return made

    def chip_sum(i, span):
        return mine_ref[i, span, :].astype(F32) + pair_ref[i, span, :].astype(F32)

    loads = {}
    for i in (3, 1, 2, 0):
        loads[i] = pltpu.make_async_copy(part_ref.at[i], mine_ref.at[i], load_sem.at[i])
        loads[i].start()
    steps = {i: copy(i, part_ref.at[4 + i], pair_ref.at[i], partner) for i in (3, 1, 2, 0)}
    loads[3].wait()
    steps[3].wait_recv()
    stage_ref[0, low, :] = chip_sum(3, low).astype(wire)
    steps[4] = copy(4, stage_ref.at[0, low], relay_ref.at[0], by_x)
    stage_ref[0, high, :] = chip_sum(3, high).astype(wire)
    steps[5] = copy(5, stage_ref.at[0, high], relay_ref.at[1], by_y)
    loads[1].wait()
    steps[1].wait_recv()
    stage_ref[1, low, :] = chip_sum(1, low).astype(wire)
    steps[6] = copy(6, stage_ref.at[1, low], last_ref.at[0, low], by_x)
    loads[2].wait()
    steps[2].wait_recv()
    stage_ref[2, high, :] = chip_sum(2, high).astype(wire)
    steps[7] = copy(7, stage_ref.at[2, high], last_ref.at[1, high], by_y)
    if extra:
        for i in range(3):
            steps[10 + i] = copy(10 + i, extra_ref[0].at[i], other_ref[0].at[i], partner)
    steps[5].wait_recv()
    stage_ref[1, high, :] = (chip_sum(1, high) + relay_ref[1].astype(F32)).astype(wire)
    steps[8] = copy(8, stage_ref.at[1, high], last_ref.at[0, high], by_x)
    steps[4].wait_recv()
    stage_ref[2, low, :] = (chip_sum(2, low) + relay_ref[0].astype(F32)).astype(wire)
    steps[9] = copy(9, stage_ref.at[2, low], last_ref.at[1, low], by_y)
    loads[0].wait()
    steps[0].wait_recv()
    out_ref[...] = chip_sum(0, full)
    steps[6].wait_recv()
    steps[7].wait_recv()
    steps[8].wait_recv()
    steps[9].wait_recv()
    out_ref[...] += last_ref[0].astype(F32) + last_ref[1].astype(F32)
    for n in range(10, 10 + 3 * extra):
        steps[n].wait_recv()
    for n in range(10 + 3 * extra):
        steps[n].wait_send()


def reduce_tokens(cid, part, *extra):
    rows, tokens = part.shape[1:]
    out = pl.pallas_call(
        functools.partial(reduce_kernel, len(extra)),
        out_shape=(jax.ShapeDtypeStruct((rows, tokens), F32),) + tuple(jax.ShapeDtypeStruct(x.shape, x.dtype) for x in extra),
        in_specs=[anywhere()] * (1 + len(extra)),
        out_specs=(whole(),) + (anywhere(),) * len(extra),
        scratch_shapes=[
            pltpu.VMEM((4, rows, tokens), part.dtype),
            pltpu.VMEM((4, rows, tokens), part.dtype),
            pltpu.VMEM((3, rows, tokens), part.dtype),
            pltpu.VMEM((2, rows // 2, tokens), part.dtype),
            pltpu.VMEM((2, rows, tokens), part.dtype),
            pltpu.SemaphoreType.DMA((13,)),
            pltpu.SemaphoreType.DMA((13,)),
            pltpu.SemaphoreType.DMA((4,)),
        ],
        compiler_params=pltpu.CompilerParams(collective_id=cid, has_side_effects=True, vmem_limit_bytes=VMEM_LIMIT),
        cost_estimate=pl.CostEstimate(flops=10_000_000_000, bytes_accessed=10_000_000, transcendentals=0),
    )(part, *extra)
    return out if extra else out[0]


def send_over(x, flip):
    return lax.ppermute(x, "ep", [(i, i ^ flip) for i in range(4)])


def swap_cores(x):
    return lax.ppermute(x, "dp", [(0, 1), (1, 0)])


def sum_start(x):
    half = x.shape[0] // 2
    dp = lax.axis_index("dp")
    mine = lax.dynamic_slice_in_dim(x, dp * half, half, 0)
    other = lax.dynamic_slice_in_dim(x, (1 - dp) * half, half, 0)
    chip = (mine.astype(F32) + swap_cores(other).astype(F32)).astype(BF16)
    sent = [chip]
    for flip in (1, 2, 3):
        sent.append(send_over(chip, flip))
    return sent


def sum_finish(parts):
    total = sum(part.astype(F32) for part in parts).astype(BF16)
    other = swap_cores(total)
    first = lax.axis_index("dp") == 0
    return jnp.concatenate([jnp.where(first, total, other), jnp.where(first, other, total)], axis=0)


def dense_forward(act, w_dense, ws_gate, ws_up):
    mixed = (act.astype(F32) + dot(w_dense, act, 0, 0)).astype(BF16)
    s_one = dot(ws_gate, mixed, 0, 0)
    s_three = dot(ws_up, mixed, 0, 0)
    shared_hidden = (jax.nn.silu(s_one) * s_three).astype(BF16)
    return mixed, s_one, s_three, shared_hidden


def shared_backward(grad_y, saved, ws_gate, ws_up, ws_down):
    mixed, s_one, s_three, shared_hidden = saved
    act_one, slope = silu_parts(s_one)
    grad_shared = dot(ws_down, grad_y, 1, 0)
    grad_s_one = (grad_shared * s_three * slope).astype(BF16)
    grad_s_three = (grad_shared * act_one).astype(BF16)
    g_ws_down = dot(grad_y, shared_hidden, 1, 1).astype(BF16)
    g_ws_gate = dot(mixed, grad_s_one, 1, 1).astype(BF16)
    g_ws_up = dot(mixed, grad_s_three, 1, 1).astype(BF16)
    back = dot(ws_gate, grad_s_one, 1, 0) + dot(ws_up, grad_s_three, 1, 0)
    return back, [g_ws_gate, g_ws_up, g_ws_down]


def dense_finish(grad_y, routed, shared, act, w_dense):
    grad_mixed = (grad_y.astype(F32) + routed + shared).astype(BF16)
    grad_act = (grad_mixed.astype(F32) + dot(w_dense, grad_mixed, 1, 0)).astype(BF16)
    return grad_act, dot(act, grad_mixed, 1, 1).astype(BF16)


def dense_backward(grad_y, routed, saved, act, w_dense, ws_gate, ws_up, ws_down):
    back, parts = shared_backward(grad_y, saved, ws_gate, ws_up, ws_down)
    grad_act, g_w_dense = dense_finish(grad_y, routed, back, act, w_dense)
    return grad_act, [g_w_dense] + parts


def solution(mesh):
    ep_size = mesh.shape["ep"]
    dp_size = mesh.shape["dp"]
    tok_spec = P(ALL_AXES, None)
    route_spec = P(None, ALL_AXES, None)
    exp_spec = P(None, "ep", None, None)
    repl_spec = P(None, None, None)

    def body(act_in, grad_out, slot_ids, gate_vals, w_dense, w_gate, w_up, w_down, ws_gate, ws_up, ws_down):
        layers, local_exp = w_gate.shape[:2]
        tokens = act_in.shape[0]
        top = slot_ids.shape[2]
        own = local_exp // dp_size
        groups = own // GROUP
        capacity = 2 * tokens * top // (local_exp * ep_size)
        dp = lax.axis_index("dp")
        base = jnp.stack([lax.axis_index("ep") * local_exp + dp * own, dp * groups, (dp_size - 1 - dp) * groups]).astype(jnp.int32)
        w_down_t = jnp.swapaxes(w_down, 2, 3)
        meta = jnp.concatenate([jnp.swapaxes(slot_ids, 1, 2).astype(F32), jnp.swapaxes(gate_vals, 1, 2)], axis=1)
        meta = meta.reshape(layers * 2 * top, tokens)

        x1 = act_in.T
        grad_y2 = grad_out.T
        saved1 = dense_forward(x1, w_dense[0], ws_gate[0], ws_up[0])
        tok1, metas = gather_tokens(0, [saved1[0], meta])
        tok1, grad_y2 = lax.optimization_barrier((tok1, grad_y2))
        grads2 = [grad_y2, send_over(grad_y2, 1), send_over(grad_y2, 2), send_over(grad_y2, 3)]
        grads2 = grads2 + [swap_cores(x) for x in grads2]
        meta1, meta2 = metas[:, : 2 * top], metas[:, 2 * top :]
        part = expert_forward(0, capacity, groups, base, tok1, meta1, w_gate, w_up, w_down_t)
        routed = reduce_tokens(1, part)
        x2 = (saved1[0].astype(F32) + routed + dot(ws_down[0], saved1[3], 0, 0)).astype(BF16)
        saved2 = dense_forward(x2, w_dense[1], ws_gate[1], ws_up[1])
        (tok2,) = gather_tokens(2, [saved2[0]])
        back2, *held, send2 = expert_backward(1, capacity, groups, base, tok2, grads2, meta2, w_gate, w_up, w_down_t, [])
        routed2, recv2 = reduce_tokens(3, back2, send2)
        grad_y1, dense2 = dense_backward(grad_y2, routed2, saved2, x2, w_dense[1], ws_gate[1], ws_up[1], ws_down[1])
        (grad1_all,) = gather_tokens(4, [grad_y1])
        shared1, parts1 = shared_backward(grad_y1, saved1, ws_gate[0], ws_up[0], ws_down[0])
        ff = ws_gate.shape[2]
        width = w_dense.shape[1]
        early = jnp.concatenate(dense2 + parts1 + [jnp.zeros((width, -(width + 6 * ff) % 128), BF16)], axis=1)
        early = sum_start(early)
        tok1, early[0] = lax.optimization_barrier((tok1, early[0]))
        back1, *held, send1 = expert_backward(0, capacity, groups, base, tok1, [grad1_all], meta1, w_gate, w_up, w_down_t, [recv2] + held)
        routed1, recv1 = reduce_tokens(5, back1, send1)
        grad_x, g_w_dense1 = dense_finish(grad_y1, routed1, shared1, x1, w_dense[0])
        late = sum_start(g_w_dense1)
        g_gate, g_up, g_down = place(0, groups, base, recv1, held)
        g_gate, late = lax.optimization_barrier((g_gate, late))
        g_down = jnp.swapaxes(g_down, 2, 3)
        early = sum_finish(early)
        late = sum_finish(late)
        g_dense = jnp.stack([late, early[:, :width]])
        shared = [jnp.stack([early[:, width + (3 + i) * ff : width + (4 + i) * ff], early[:, width + i * ff : width + (i + 1) * ff]]) for i in range(3)]
        return (grad_x.T, g_dense, g_gate, g_up, g_down, shared[0], shared[1], jnp.swapaxes(shared[2], 1, 2))

    return jax.shard_map(body, mesh=mesh, in_specs=(tok_spec, tok_spec, route_spec, route_spec, repl_spec, exp_spec, exp_spec, exp_spec, repl_spec, repl_spec, repl_spec), out_specs=(tok_spec, repl_spec, exp_spec, exp_spec, exp_spec, repl_spec, repl_spec, repl_spec), check_vma=False)
```

```python
import functools
import jax
import jax.numpy as jnp
from jax import lax
from jax.experimental import pallas as pl
from jax.experimental.pallas import tpu as pltpu
from jax.sharding import PartitionSpec as P

ALL_AXES = ("ep", "dp")
GROUP = 8
UNROLL = 8
VMEM_LIMIT = 62 << 20
LOW, HIGH = range(2)
OWN, X, Y, FAR = range(4)
COST = pl.CostEstimate(flops=20_000_000_000, bytes_accessed=20_000_000, transcendentals=0)
F32 = jnp.float32
BF16 = jnp.bfloat16


def dot(left, right, left_dim, right_dim):
    return lax.dot_general(left, right, (((left_dim,), (right_dim,)), ((), ())), preferred_element_type=F32)


def dot_nn(left, right):
    return dot(left, right, 1, 0)


def dot_nt(left, right):
    return dot(left, right, 1, 1)


def dot_tn(left, right):
    return dot(left, right, 0, 0)


def silu_parts(pre_act):
    sigma = jax.nn.sigmoid(pre_act)
    return pre_act * sigma, sigma * (1.0 + pre_act * (1.0 - sigma))


def route(meta_ref, src, first_expert, capacity, pick_ref, slot, tok_ref=None):
    top = meta_ref.shape[1] // 2
    tokens = meta_ref.shape[2]
    slots = meta_ref[src, 0:top, :].astype(jnp.int32)
    gates = meta_ref[src, top : 2 * top, :]
    expert = slots // capacity - first_expert
    row = (slots % capacity).astype(F32)
    which = lax.broadcasted_iota(jnp.int32, (GROUP, tokens), 0)
    row_of = jnp.full((GROUP, tokens), -1.0, F32)
    gate_of = jnp.zeros((GROUP, tokens), F32)
    for j in range(top):
        hit = expert[j : j + 1, :] == which
        row_of = jnp.where(hit, row[j : j + 1, :], row_of)
        gate_of = jnp.where(hit, gates[j : j + 1, :], gate_of)
    if tok_ref is not None:
        width = tok_ref.shape[1] - 4 * GROUP
        high = gate_of.astype(BF16)
        rest = gate_of - high.astype(F32)
        middle = rest.astype(BF16)
        low = (rest - middle.astype(F32)).astype(BF16)
        tok_ref[src, width : width + 4 * GROUP, :] = jnp.concatenate([high, middle, low, jnp.zeros_like(low)], axis=0)
    step = 16
    rows = lax.broadcasted_iota(jnp.int32, (step, tokens), 0).astype(F32).astype(BF16)
    for k in range(GROUP):
        wanted = jnp.broadcast_to(row_of[k : k + 1, :], (step, tokens)).astype(BF16)
        for h in range(capacity // step):
            hit = wanted == rows + jnp.asarray(h * step, BF16)
            start = k * capacity + h * step
            pick_ref[slot, src, start : start + step, :] = jnp.where(hit, jnp.asarray(1, BF16), jnp.asarray(0, BF16))


def gate_column(found, capacity):
    width = found.shape[1] - 4 * GROUP
    gates = []
    for k in range(GROUP):
        rows = found[k * capacity : (k + 1) * capacity, :]
        gates.append(rows[:, width + k : width + k + 1] + rows[:, width + GROUP + k : width + GROUP + k + 1] + rows[:, width + 2 * GROUP + k : width + 2 * GROUP + k + 1])
    return jnp.concatenate(gates, axis=0)


def schedule(groups, sources, begin, wait, dispatch, expert, combine, finish):
    group = pl.program_id(0)

    @pl.when(group == 0)
    def _():
        begin()

        def first(src, carry):
            wait(src)
            dispatch(src)
            return carry

        lax.fori_loop(0, sources, first, 0)

    @pl.when((group > 0) & (group < groups))
    def _():
        def middle(src, carry):
            combine(src)
            dispatch(src)
            return carry

        lax.fori_loop(0, sources, middle, 0)

    @pl.when(group < groups)
    def _():
        def one(k, carry):
            expert(k)
            return carry

        lax.fori_loop(0, GROUP, one, 0, unroll=UNROLL)

    @pl.when(group == groups)
    def _():
        def last(src, carry):
            finish(src)
            return carry

        lax.fori_loop(0, sources, last, 0)


def start_all(copies):
    for copy in copies:
        copy.start()


def wait_all(copies):
    for copy in copies:
        copy.wait()


def fwd_kernel(capacity, groups, base_ref, meta_ref, w1_ref, w3_ref, w2_ref, tokens_ref, out_ref, xs_ref, sum_ref, tok_ref, pick_ref, gate_ref, x_ref, o_ref, sem, out_sem, save_sem):
    group = pl.program_id(0)
    sources = tok_ref.shape[0]
    width = w1_ref.shape[1]
    now = group % 2
    before = 1 - now

    def load(src):
        return pltpu.make_async_copy(tokens_ref.at[src], tok_ref.at[src, pl.ds(0, width)], sem.at[src])

    def begin():
        for src in range(sources):
            load(src).start()

    def dispatch(src):
        route(meta_ref, src, base_ref[0] + group * GROUP, capacity, pick_ref, now, tok_ref)
        found = dot_nt(pick_ref[now, src], tok_ref[src])
        x_ref[now, src] = found.astype(BF16)
        gate_ref[src] = gate_column(found, capacity)

    def expert(k):
        here = pl.ds(pl.multiple_of(k * capacity, capacity), capacity)
        x = x_ref[now, :, here, :width].reshape(sources * capacity, width)
        ff = w1_ref.shape[2]
        a = dot_nn(x, jnp.concatenate([w1_ref[k], w3_ref[k]], axis=1))
        hidden = (jax.nn.silu(a[:, :ff]) * a[:, ff:]).astype(BF16)
        out = dot_nt(hidden, w2_ref[k]).astype(BF16).astype(F32)
        gate = gate_ref[:, here, :].reshape(sources * capacity, 1)
        o_ref[:, here, :] = (gate * out).reshape(sources, capacity, width)

    def added(src):
        rest = o_ref[src].T
        pick = pick_ref[before, src]
        parts = []
        for _ in range(3):
            parts.append(rest.astype(BF16))
            rest = rest - parts[-1].astype(F32)
        return dot_nn(parts[0], pick) + dot_nn(parts[1], pick) + dot_nn(parts[2], pick)

    def combine(src):
        @pl.when(group == 1)
        def _():
            sum_ref[src] = jnp.zeros(sum_ref.shape[1:], F32)

        sum_ref[src] += added(src)

    def store(src):
        return pltpu.make_async_copy(sum_ref.at[src], out_ref.at[src], out_sem.at[src])

    def finish(src):
        sum_ref[src] += added(src)
        store(src).start()

    def saves(step):
        slot = step % 2
        return [pltpu.make_async_copy(kept.at[slot], to.at[step], save_sem.at[slot, n]) for n, (kept, to) in enumerate(((x_ref, xs_ref),))]

    @pl.when(group >= 2)
    def _():
        wait_all(saves(group - 2))

    schedule(groups, sources, begin, lambda src: load(src).wait(), dispatch, expert, combine, finish)

    @pl.when(group < groups)
    def _():
        start_all(saves(group))

    @pl.when(group == groups)
    def _():
        wait_all(saves(group - 1))
        for src in range(sources):
            store(src).wait()


def bwd_kernel(layer, capacity, groups, held, pieces, keeps, base_ref, meta_ref, w1_ref, w3_ref, w2_ref, *refs):
    given_ref, piece_refs, other_refs, refs = refs[0], refs[1 : 1 + pieces], refs[1 + pieces : 1 + pieces + held], refs[1 + pieces + held :]
    out_ref, d1_ref, d3_ref, d2_ref, sum_ref, grad_ref, pick_ref, x_ref, g_ref, r_ref, d_ref, sem, grad_sem, out_sem, d_sem, from_ref = refs[:16]
    d_refs = (d1_ref, d3_ref, d2_ref)
    group = pl.program_id(0)
    sources = sum_ref.shape[0]
    width = w1_ref.shape[1]
    now = group % 2
    before = 1 - now
    x_slot = now if keeps else 0

    def load(src):
        return pltpu.make_async_copy(given_ref.at[src], from_ref.at[src, pl.ds(0, width)], sem.at[src])

    def loads_saved(step):
        return [pltpu.make_async_copy(given_ref.at[step], x_ref.at[step % 2], sem.at[step % 2])]

    def load_grad(src):
        piece = piece_refs[0].at[src] if pieces == 1 else piece_refs[src]
        return pltpu.make_async_copy(piece, grad_ref.at[src], grad_sem.at[src])

    def begin():
        if keeps:
            start_all(loads_saved(0))
        for src in range(sources):
            if not keeps:
                load(src).start()
            load_grad(src).start()
        if keeps:
            wait_all(loads_saved(0))

    def wait(src):
        if not keeps:
            load(src).wait()
        pltpu.make_async_copy(grad_ref.at[src], grad_ref.at[src], grad_sem.at[src]).wait()

    def dispatch(src):
        if keeps:
            route(meta_ref, src, base_ref[0] + group * GROUP, capacity, pick_ref, now)
            gate = gate_column(x_ref[now, src].astype(F32), capacity)
        else:
            route(meta_ref, src, base_ref[0] + group * GROUP, capacity, pick_ref, now, from_ref)
            found = dot_nt(pick_ref[now, src], from_ref[src])
            gate = gate_column(found, capacity)
            x_ref[0, src] = found.astype(BF16)
        g_ref[src] = (gate * dot_nt(pick_ref[now, src], grad_ref[src])).astype(BF16)

    def next_saved():
        @pl.when((group > 0) & (group < groups))
        def _():
            wait_all(loads_saved(group))

        @pl.when(group < groups - 1)
        def _():
            start_all(loads_saved(group + 1))

    def expert(k):
        here = pl.ds(pl.multiple_of(k * capacity, capacity), capacity)
        x = x_ref[x_slot, :, here, :width].reshape(sources * capacity, width)
        g = g_ref[:, here, :].reshape(sources * capacity, width)
        ff = w1_ref.shape[2]
        both = jnp.concatenate([w1_ref[k], w3_ref[k]], axis=1)
        a = dot_nn(x, both)
        a_three = a[:, ff:]
        act, slope = silu_parts(a[:, :ff])
        hidden = (act * a_three).astype(BF16)
        grad_hidden = dot_nn(g, w2_ref[k])
        grad_one = (grad_hidden * a_three * slope).astype(BF16)
        grad_three = (grad_hidden * act).astype(BF16)
        grads = jnp.concatenate([grad_one, grad_three], axis=1)
        r_ref[:, here, :] = dot_nt(grads, both).astype(BF16).reshape(sources, capacity, width)
        d13 = dot_tn(x, grads).astype(BF16)
        d2 = dot_tn(g, hidden).astype(BF16)
        for i, value in enumerate((d13[:, :ff], d13[:, ff:], d2)):
            d_ref[now, i, k] = value

    def added(src):
        return dot_tn(r_ref[src], pick_ref[before, src])

    def combine(src):
        @pl.when(group == 1)
        def _():
            sum_ref[src] = jnp.zeros(sum_ref.shape[1:], F32)

        sum_ref[src] += added(src)

    def store(src):
        return pltpu.make_async_copy(grad_ref.at[src], out_ref.at[src], out_sem.at[src])

    def finish(src):
        grad_ref[src] = (sum_ref[src] + added(src)).astype(BF16)
        store(src).start()

    def experts_at(start, step):
        return pl.ds(pl.multiple_of((start + step) * GROUP, GROUP), GROUP)

    def d_stores(step):
        slot = step % 2
        return [pltpu.make_async_copy(d_ref.at[slot, i], d_refs[i].at[layer, experts_at(base_ref[1], step)], d_sem.at[slot, i]) for i in range(3)]

    def other_load(step):
        return pltpu.make_async_copy(other_refs[0].at[:, experts_at(0, step)], refs[16].at[step % 2], refs[17].at[step % 2, 3])

    def other_stores(step):
        slot = step % 2
        return [pltpu.make_async_copy(refs[16].at[slot, i], d_refs[i].at[1 - layer, experts_at(base_ref[2], step)], refs[17].at[slot, i]) for i in range(3)]

    @pl.when(group >= 2)
    def _():
        wait_all(d_stores(group - 2))
        if held:
            wait_all(other_stores(group - 2))

    if held:
        @pl.when(group >= 1)
        def _():
            other_load(group - 1).wait()
            start_all(other_stores(group - 1))

        @pl.when(group < groups)
        def _():
            other_load(group).start()

    if keeps:
        next_saved()

    schedule(groups, sources, begin, wait, dispatch, expert, combine, finish)

    @pl.when(group < groups)
    def _():
        start_all(d_stores(group))

    @pl.when(group == groups)
    def _():
        wait_all(d_stores(group - 1))
        if held:
            wait_all(other_stores(group - 1))
        for src in range(sources):
            store(src).wait()


def weight_specs(layer, groups, width, ff):
    spec = pl.BlockSpec((None, GROUP, width, ff), lambda g, base: (layer, base[1] + jnp.minimum(g, groups - 1), 0, 0))
    return [spec, spec, spec]


def whole():
    return pl.BlockSpec(memory_space=pltpu.VMEM)


def anywhere():
    return pl.BlockSpec(memory_space=pl.ANY)


def expert_forward(layer, capacity, groups, base, tok, meta, w1, w3, w2):
    sources, width, tokens = tok.shape
    ff = w1.shape[3]
    rows = GROUP * capacity
    return pl.pallas_call(
        functools.partial(fwd_kernel, capacity, groups),
        out_shape=(
            jax.ShapeDtypeStruct((sources, width, tokens), F32),
            jax.ShapeDtypeStruct((groups, sources, rows, width + 4 * GROUP), BF16),
        ),
        grid_spec=pltpu.PrefetchScalarGridSpec(
            num_scalar_prefetch=1,
            grid=(groups + 1,),
            in_specs=[whole()] + weight_specs(layer, groups, width, ff) + [anywhere()],
            out_specs=(anywhere(),) * 2,
            scratch_shapes=[
                pltpu.VMEM((sources, width, tokens), F32),
                pltpu.VMEM((sources, width + 4 * GROUP, tokens), BF16),
                pltpu.VMEM((2, sources, rows, tokens), BF16),
                pltpu.VMEM((sources, rows, 1), F32),
                pltpu.VMEM((2, sources, rows, width + 4 * GROUP), BF16),
                pltpu.VMEM((sources, rows, width), F32),
                pltpu.SemaphoreType.DMA((sources,)),
                pltpu.SemaphoreType.DMA((sources,)),
                pltpu.SemaphoreType.DMA((2, 1)),
            ],
        ),
        compiler_params=pltpu.CompilerParams(vmem_limit_bytes=VMEM_LIMIT),
        cost_estimate=COST,
    )(base, meta, w1, w3, w2, tok)


def expert_backward(layer, capacity, groups, base, given, keeps, grads, meta, w1, w3, w2, held):
    sources, tokens = meta.shape[0], meta.shape[2]
    width = w1.shape[2]
    ff = w1.shape[3]
    rows = GROUP * capacity
    pieces = len(grads)
    grad_shape = jax.ShapeDtypeStruct(w1.shape, BF16)
    block = pltpu.VMEM((2, 3, GROUP, width, ff), BF16)
    more = [block, pltpu.SemaphoreType.DMA((2, 4))] if held else []
    return pl.pallas_call(
        functools.partial(bwd_kernel, layer, capacity, groups, len(held), pieces, keeps),
        out_shape=(jax.ShapeDtypeStruct((sources, width, tokens), BF16), grad_shape, grad_shape, grad_shape),
        grid_spec=pltpu.PrefetchScalarGridSpec(
            num_scalar_prefetch=1,
            grid=(groups + 1,),
            in_specs=[whole()] + weight_specs(layer, groups, width, ff) + [anywhere()] * (1 + pieces + len(held)),
            out_specs=(anywhere(),) * 4,
            scratch_shapes=[
                pltpu.VMEM((sources, width, tokens), F32),
                pltpu.VMEM((sources, width, tokens), BF16),
                pltpu.VMEM((2, sources, rows, tokens), BF16),
                pltpu.VMEM((2 if keeps else 1, sources, rows, width + 4 * GROUP), BF16),
                pltpu.VMEM((sources, rows, width), BF16),
                pltpu.VMEM((sources, rows, width), BF16),
                block,
                pltpu.SemaphoreType.DMA((sources,)),
                pltpu.SemaphoreType.DMA((sources,)),
                pltpu.SemaphoreType.DMA((sources,)),
                pltpu.SemaphoreType.DMA((2, 4)),
                pltpu.VMEM((8, 128), BF16) if keeps else pltpu.VMEM((sources, width + 4 * GROUP, tokens), BF16),
            ]
            + more,
        ),
        input_output_aliases={7 + pieces + i: 1 + i for i in range(len(held) - 1)},
        compiler_params=pltpu.CompilerParams(vmem_limit_bytes=VMEM_LIMIT),
        cost_estimate=COST,
    )(base, meta, w1, w3, w2, given, *grads, *held)


def place_kernel(base_ref, recv_ref, *refs):
    for i in range(3):
        refs[3 + i][...] = recv_ref[i]


def place(layer, groups, base, recv, held):
    width, ff = recv.shape[2:]
    few = 8
    spec = pl.BlockSpec((None, few, width, ff), lambda g, base: (layer, base[2] * (GROUP // few) + g, 0, 0))
    shape = jax.ShapeDtypeStruct(held[0].shape, BF16)
    return pl.pallas_call(
        place_kernel,
        out_shape=(shape, shape, shape),
        grid_spec=pltpu.PrefetchScalarGridSpec(
            num_scalar_prefetch=1,
            grid=(groups * GROUP // few,),
            in_specs=[pl.BlockSpec((3, few, width, ff), lambda g, base: (0, g, 0, 0))] + [anywhere()] * 3,
            out_specs=(spec, spec, spec),
        ),
        input_output_aliases={2: 0, 3: 1, 4: 2},
        compiler_params=pltpu.CompilerParams(vmem_limit_bytes=VMEM_LIMIT),
        cost_estimate=COST,
    )(base, recv, *held)


def neighbours():
    ep = lax.axis_index("ep")
    dp = lax.axis_index("dp")
    return ({"ep": ep + 1 - 2 * (ep % 2), "dp": dp}, {"ep": (ep + 2) % 4, "dp": dp}, {"ep": ep, "dp": 1 - dp})


def greet(devices):
    barrier = pltpu.get_barrier_semaphore()
    for device in devices:
        pl.semaphore_signal(barrier, inc=1, device_id=device, device_id_type=pl.DeviceIdType.MESH)
    pl.semaphore_wait(barrier, len(devices))


def send_block(source, target, send, recv, device):
    made = pltpu.make_async_remote_copy(src_ref=source, dst_ref=target, send_sem=send, recv_sem=recv, device_id=device, device_id_type=pl.DeviceIdType.MESH)
    made.start()
    return made


def gather_phase(devices, own_refs, out_refs, land_refs, sems, shadows):
    by_x, by_y, partner = devices
    send_sem, recv_sem, store_sem = sems
    count = len(own_refs)
    stores = []

    made = [[] for _ in own_refs]

    def copy(which, source, target, half, device):
        rows = own_refs[which].shape[0]
        span = pl.ds(0, rows) if half is None else pl.ds(half * (rows // 2), rows // 2)
        block = land_refs[which].at[source, span] if source else own_refs[which].at[span]
        n = len(made[which])
        made[which].append(send_block(block, land_refs[which].at[target, span], send_sem.at[which, n], recv_sem.at[which, n], device))
        return made[which][n]

    def store(which, slot):
        block = land_refs[which].at[slot] if slot else own_refs[which]
        started = pltpu.make_async_copy(block, out_refs[which].at[slot], store_sem.at[which, slot])
        started.start()
        stores.append(started)

    near, far, pair = [], [], []
    for which in range(count):
        near.append([copy(which, OWN, X, LOW, by_x), copy(which, OWN, Y, HIGH, by_y), copy(which, OWN, X, HIGH, by_x), copy(which, OWN, Y, LOW, by_y)])
        pair.append(copy(which, OWN, 4, None, partner))
        store(which, OWN)
    shadows[0]()
    for which in range(count):
        x_low, y_high, x_high, y_low = near[which]
        x_low.wait_recv()
        relay_low = copy(which, X, FAR, LOW, by_y)
        y_high.wait_recv()
        relay_high = copy(which, Y, FAR, HIGH, by_x)
        if not far:
            shadows[1]()
        x_high.wait_recv()
        pair_x = copy(which, X, 4 + X, None, partner)
        store(which, X)
        y_low.wait_recv()
        pair_y = copy(which, Y, 4 + Y, None, partner)
        store(which, Y)
        pair[which].wait_recv()
        store(which, 4)
        far.append((relay_low, relay_high, pair_x, pair_y))
    for which in range(count):
        relay_low, relay_high, pair_x, pair_y = far[which]
        relay_low.wait_recv()
        pair_low = copy(which, FAR, 4 + FAR, LOW, partner)
        relay_high.wait_recv()
        pair_high = copy(which, FAR, 4 + FAR, HIGH, partner)
        store(which, FAR)
        pair_x.wait_recv()
        store(which, 4 + X)
        pair_y.wait_recv()
        store(which, 4 + Y)
        pair_low.wait_recv()
        pair_high.wait_recv()
        store(which, 4 + FAR)
        for step in made[which]:
            step.wait_send()
    wait_all(stores)


def gather_scratch(*arrays):
    count = len(arrays)
    return [pltpu.VMEM((8,) + x.shape, x.dtype) for x in arrays] + [pltpu.SemaphoreType.DMA((count, n)) for n in (11, 11, 8)]


def reduce_phase(devices, part_ref, out_ref, scratch, extras, shadow):
    mine_ref, pair_ref, stage_ref, relay_ref, last_ref, send_sem, recv_sem, load_sem = scratch
    by_x, by_y, partner = devices
    rows = part_ref.shape[1]
    half = rows // 2
    low, high, full = pl.ds(0, half), pl.ds(half, half), pl.ds(0, rows)
    wire = part_ref.dtype

    made = []

    def copy(source, target, device):
        n = len(made)
        made.append(send_block(source, target, send_sem.at[n], recv_sem.at[n], device))
        return made[n]

    def chip_sum(i, span):
        return mine_ref[i, span, :].astype(F32) + pair_ref[i, span, :].astype(F32)

    loads, pair = {}, {}
    for i in (FAR, X, Y, OWN):
        loads[i] = pltpu.make_async_copy(part_ref.at[i], mine_ref.at[i], load_sem.at[i])
        loads[i].start()
        pair[i] = copy(part_ref.at[4 + i], pair_ref.at[i], partner)

    def ready(i):
        loads[i].wait()
        pair[i].wait_recv()

    ready(FAR)
    stage_ref[OWN, low, :] = chip_sum(FAR, low).astype(wire)
    relay_x = copy(stage_ref.at[OWN, low], relay_ref.at[LOW], by_x)
    stage_ref[OWN, high, :] = chip_sum(FAR, high).astype(wire)
    relay_y = copy(stage_ref.at[OWN, high], relay_ref.at[HIGH], by_y)
    ready(X)
    stage_ref[X, low, :] = chip_sum(X, low).astype(wire)
    arrive = [copy(stage_ref.at[X, low], last_ref.at[LOW, low], by_x)]
    ready(Y)
    stage_ref[Y, high, :] = chip_sum(Y, high).astype(wire)
    arrive.append(copy(stage_ref.at[Y, high], last_ref.at[HIGH, high], by_y))
    others = [copy(source, target, partner) for source, target in extras]
    relay_y.wait_recv()
    stage_ref[X, high, :] = (chip_sum(X, high) + relay_ref[HIGH].astype(F32)).astype(wire)
    arrive.append(copy(stage_ref.at[X, high], last_ref.at[LOW, high], by_x))
    relay_x.wait_recv()
    stage_ref[Y, low, :] = (chip_sum(Y, low) + relay_ref[LOW].astype(F32)).astype(wire)
    arrive.append(copy(stage_ref.at[Y, low], last_ref.at[HIGH, low], by_y))
    ready(OWN)
    out_ref[...] = chip_sum(OWN, full)
    shadow()
    for step in arrive:
        step.wait_recv()
    out_ref[...] += last_ref[LOW].astype(F32) + last_ref[HIGH].astype(F32)

    def drain():
        for step in others:
            step.wait_recv()
        for step in made:
            step.wait_send()

    return drain


def reduce_scratch(part):
    rows, tokens = part.shape[1:]
    return [
        pltpu.VMEM((4, rows, tokens), part.dtype),
        pltpu.VMEM((4, rows, tokens), part.dtype),
        pltpu.VMEM((3, rows, tokens), part.dtype),
        pltpu.VMEM((2, rows // 2, tokens), part.dtype),
        pltpu.VMEM((2, rows, tokens), part.dtype),
        pltpu.SemaphoreType.DMA((13,)),
        pltpu.SemaphoreType.DMA((13,)),
        pltpu.SemaphoreType.DMA((4,)),
    ]


def nothing():
    pass


def mix(x_ref, w_dense_ref):
    x = x_ref[...]
    return (x.astype(F32) + dot_tn(w_dense_ref[...], x)).astype(BF16)


def shared_forward(mixed, ws_gate, ws_up):
    s_one = dot_tn(ws_gate, mixed)
    s_three = dot_tn(ws_up, mixed)
    return s_one, s_three, (jax.nn.silu(s_one) * s_three).astype(BF16)


def shared_backward(grad_y, mixed, ws_gate, ws_up, ws_down, pack_ref, start):
    s_one, s_three, shared_hidden = shared_forward(mixed, ws_gate, ws_up)
    act_one, slope = silu_parts(s_one)
    grad_shared = dot_tn(ws_down, grad_y)
    grad_s_one = (grad_shared * s_three * slope).astype(BF16)
    grad_s_three = (grad_shared * act_one).astype(BF16)
    ff = ws_gate.shape[1]
    for i, value in enumerate((dot_nt(mixed, grad_s_one), dot_nt(mixed, grad_s_three), dot_nt(grad_y, shared_hidden))):
        pack_ref[:, start + i * ff : start + (i + 1) * ff] = value.astype(BF16)
    return dot_nn(ws_gate, grad_s_one) + dot_nn(ws_up, grad_s_three)


def comm_call(kernel, cid, out_shape, in_specs, out_specs, scratch, operands):
    return pl.pallas_call(
        kernel,
        out_shape=out_shape,
        in_specs=in_specs,
        out_specs=out_specs,
        scratch_shapes=scratch,
        compiler_params=pltpu.CompilerParams(collective_id=cid, has_side_effects=True, vmem_limit_bytes=VMEM_LIMIT),
        cost_estimate=COST,
    )(*operands)


def first_kernel(x_ref, w_dense_ref, meta_ref, tok_ref, metas_ref, own_ref, land_ref, land_meta_ref, *sems):
    devices = neighbours()
    own_ref[...] = mix(x_ref, w_dense_ref)
    greet(devices)
    gather_phase(devices, [own_ref, meta_ref], [tok_ref, metas_ref], [land_ref, land_meta_ref], sems, (nothing, nothing))


def first_exchange(x, w_dense, meta):
    outs = (jax.ShapeDtypeStruct((8,) + x.shape, BF16), jax.ShapeDtypeStruct((8,) + meta.shape, F32), jax.ShapeDtypeStruct(x.shape, BF16))
    return comm_call(first_kernel, 0, outs, [whole()] * 3, (anywhere(), anywhere(), whole()), gather_scratch(x, meta), (x, w_dense, meta))


def forward_kernel(part_ref, u1_ref, ws_gate_ref, ws_up_ref, ws_down_ref, w_dense_ref, tok_ref, x2_ref, u2_ref, sum_ref, shared_ref, *scratch):
    devices = neighbours()
    greet(devices)

    def shadow():
        hidden = shared_forward(u1_ref[...], ws_gate_ref[...], ws_up_ref[...])[2]
        shared_ref[...] = dot_nn(ws_down_ref[...], hidden)

    drain = reduce_phase(devices, part_ref, sum_ref, scratch[:8], [], shadow)
    x2_ref[...] = (u1_ref[...].astype(F32) + sum_ref[...] + shared_ref[...]).astype(BF16)
    u2_ref[...] = mix(x2_ref, w_dense_ref)
    gather_phase(devices, [u2_ref], [tok_ref], [scratch[8]], scratch[9:], (nothing, nothing))
    drain()


def forward_exchange(part, u1, ws_gate, ws_up, ws_down_t, w_dense):
    outs = (jax.ShapeDtypeStruct((8,) + u1.shape, BF16), jax.ShapeDtypeStruct(u1.shape, BF16), jax.ShapeDtypeStruct(u1.shape, BF16))
    scratch = [pltpu.VMEM(u1.shape, F32), pltpu.VMEM(u1.shape, F32)] + reduce_scratch(part) + gather_scratch(u1)
    specs = [anywhere()] + [whole()] * 5
    return comm_call(forward_kernel, 1, outs, specs, (anywhere(), whole(), whole()), scratch, (part, u1, ws_gate, ws_up, ws_down_t, w_dense))


def expert_half(refs, layer, target_ref):
    own = target_ref.shape[1]
    start = lax.axis_index("dp") * own
    return [(ref.at[layer, pl.ds(start, own)], target_ref.at[i]) for i, ref in enumerate(refs)]


def backward_kernel(part_ref, d1_ref, d3_ref, d2_ref, grad_y_ref, x2_ref, u2_ref, u1_ref, w_dense_ref, *refs):
    shared2, shared1, refs = refs[:3], refs[3:6], refs[6:]
    grad_all_ref, recv_ref, grad_x_ref, back_ref, pack_ref, sum_ref, mixed_ref = refs[:7]
    scratch = refs[7:]
    devices = neighbours()
    greet(devices)
    ff = shared1[0].shape[1]
    width = x2_ref.shape[0]

    def shadow():
        back_ref[...] = shared_backward(grad_y_ref[...], u2_ref[...], *(ref[...] for ref in shared2), pack_ref, 0)

    drain = reduce_phase(devices, part_ref, sum_ref, scratch[:8], expert_half((d1_ref, d3_ref, d2_ref), 1, recv_ref), shadow)
    mixed_ref[...] = (grad_y_ref[...].astype(F32) + sum_ref[...] + back_ref[...]).astype(BF16)
    grad_x_ref[...] = (mixed_ref[...].astype(F32) + dot_nn(w_dense_ref[...], mixed_ref[...])).astype(BF16)

    def dense_part():
        pack_ref[:, 6 * ff : 6 * ff + width] = dot_nt(x2_ref[...], mixed_ref[...]).astype(BF16)
        pack_ref[:, 6 * ff + width :] = jnp.zeros((width, pack_ref.shape[1] - 6 * ff - width), BF16)

    def shared_part():
        back_ref[...] = shared_backward(grad_x_ref[...], u1_ref[...], *(ref[...] for ref in shared1), pack_ref, 3 * ff)

    gather_phase(devices, [grad_x_ref], [grad_all_ref], [scratch[8]], scratch[9:], (dense_part, shared_part))
    drain()


def backward_exchange(part, held, grad_y, x2, u2, u1, w_dense, shared2, shared1):
    ff = shared1[0].shape[1]
    width = x2.shape[0]
    packed = 6 * ff + width + -(6 * ff + width) % 128
    own = held[0].shape[1] // 2
    outs = (
        jax.ShapeDtypeStruct((8,) + x2.shape, BF16),
        jax.ShapeDtypeStruct((3, own) + held[0].shape[2:], BF16),
        jax.ShapeDtypeStruct(x2.shape, BF16),
        jax.ShapeDtypeStruct(x2.shape, F32),
        jax.ShapeDtypeStruct((width, packed), BF16),
    )
    scratch = [pltpu.VMEM(x2.shape, F32), pltpu.VMEM(x2.shape, BF16)] + reduce_scratch(part) + gather_scratch(x2)
    operands = (part, *held, grad_y, x2, u2, u1, w_dense, *shared2, *shared1)
    specs = [anywhere()] * 4 + [whole()] * 11
    return comm_call(backward_kernel, 2, outs, specs, (anywhere(), anywhere()) + (whole(),) * 3, scratch, operands)


def last_kernel(part_ref, d1_ref, d3_ref, d2_ref, out_ref, recv_ref, *scratch):
    devices = neighbours()
    greet(devices)
    reduce_phase(devices, part_ref, out_ref, scratch, expert_half((d1_ref, d3_ref, d2_ref), 0, recv_ref), nothing)()


def last_exchange(part, held):
    own = held[0].shape[1] // 2
    outs = (jax.ShapeDtypeStruct(part.shape[1:], F32), jax.ShapeDtypeStruct((3, own) + held[0].shape[2:], BF16))
    return comm_call(last_kernel, 3, outs, [anywhere()] * 4, (whole(), anywhere()), reduce_scratch(part), (part, *held))


def send_over(x, flip):
    return lax.ppermute(x, "ep", [(i, i ^ flip) for i in range(4)])


def swap_cores(x):
    return lax.ppermute(x, "dp", [(0, 1), (1, 0)])


def sum_start(x):
    half = x.shape[0] // 2
    dp = lax.axis_index("dp")
    mine = lax.dynamic_slice_in_dim(x, dp * half, half, 0)
    other = lax.dynamic_slice_in_dim(x, (1 - dp) * half, half, 0)
    chip = (mine.astype(F32) + swap_cores(other).astype(F32)).astype(BF16)
    sent = [chip]
    for flip in (1, 2, 3):
        sent.append(send_over(chip, flip))
    return sent


def sum_finish(parts):
    total = sum(part.astype(F32) for part in parts).astype(BF16)
    other = swap_cores(total)
    first = lax.axis_index("dp") == 0
    return jnp.concatenate([jnp.where(first, total, other), jnp.where(first, other, total)], axis=0)


def dense_finish(grad_y, routed, shared, act, w_dense):
    grad_mixed = (grad_y.astype(F32) + routed + shared).astype(BF16)
    grad_act = (grad_mixed.astype(F32) + dot_nn(w_dense, grad_mixed)).astype(BF16)
    return grad_act, dot_nt(act, grad_mixed).astype(BF16)


def solution(mesh):
    ep_size = mesh.shape["ep"]
    dp_size = mesh.shape["dp"]
    tok_spec = P(ALL_AXES)
    route_spec = P(None, ALL_AXES)
    exp_spec = P(None, "ep")
    repl_spec = P()

    def body(act_in, grad_out, slot_ids, gate_vals, w_dense, w_gate, w_up, w_down, ws_gate, ws_up, ws_down):
        layers, local_exp = w_gate.shape[:2]
        tokens = act_in.shape[0]
        top = slot_ids.shape[2]
        own = local_exp // dp_size
        groups = own // GROUP
        capacity = 2 * tokens * top // (local_exp * ep_size)
        dp = lax.axis_index("dp")
        base = jnp.stack([lax.axis_index("ep") * local_exp + dp * own, dp * groups, (dp_size - 1 - dp) * groups]).astype(jnp.int32)
        w_down_t = jnp.swapaxes(w_down, 2, 3)
        meta = jnp.concatenate([jnp.swapaxes(slot_ids, 1, 2).astype(F32), jnp.swapaxes(gate_vals, 1, 2)], axis=1)
        meta = meta.reshape(layers * 2 * top, tokens)

        x1 = act_in.T
        grad_y2 = grad_out.T
        shared_w = [(ws_gate[layer], ws_up[layer], jnp.swapaxes(ws_down[layer], 0, 1)) for layer in range(layers)]
        tok1, metas, u1 = first_exchange(x1, w_dense[0], meta)
        tok1, grad_y2 = lax.optimization_barrier((tok1, grad_y2))
        grads2 = [grad_y2, send_over(grad_y2, 1), send_over(grad_y2, 2), send_over(grad_y2, 3)]
        grads2 = grads2 + [swap_cores(x) for x in grads2]
        meta1, meta2 = metas[:, : 2 * top], metas[:, 2 * top :]
        part, rows1 = expert_forward(0, capacity, groups, base, tok1, meta1, w_gate, w_up, w_down_t)
        tok2, x2, u2 = forward_exchange(part, u1, *shared_w[0], w_dense[1])
        back2, *held = expert_backward(1, capacity, groups, base, tok2, False, grads2, meta2, w_gate, w_up, w_down_t, [])
        grad1_all, recv2, grad_y1, shared1, early = backward_exchange(back2, held, grad_y2, x2, u2, u1, w_dense[1], shared_w[1], shared_w[0])
        ff = ws_gate.shape[2]
        width = w_dense.shape[1]
        early = sum_start(early)
        grad1_all, early[0] = lax.optimization_barrier((grad1_all, early[0]))
        back1, *held = expert_backward(0, capacity, groups, base, rows1, True, [grad1_all], meta1, w_gate, w_up, w_down_t, [recv2] + held)
        routed1, recv1 = last_exchange(back1, held)
        grad_x, g_w_dense1 = dense_finish(grad_y1, routed1, shared1, x1, w_dense[0])
        late = sum_start(g_w_dense1)
        g_gate, g_up, g_down = place(0, groups, base, recv1, held)
        g_gate, late = lax.optimization_barrier((g_gate, late))
        g_down = jnp.swapaxes(g_down, 2, 3)
        early = sum_finish(early)
        late = sum_finish(late)
        g_dense = jnp.stack([late, early[:, 6 * ff : 6 * ff + width]])
        shared = [jnp.stack([early[:, (3 + i) * ff : (4 + i) * ff], early[:, i * ff : (i + 1) * ff]]) for i in range(3)]
        return (grad_x.T, g_dense, g_gate, g_up, g_down, shared[0], shared[1], jnp.swapaxes(shared[2], 1, 2))

    return jax.shard_map(body, mesh=mesh, in_specs=(tok_spec, tok_spec, route_spec, route_spec, repl_spec, exp_spec, exp_spec, exp_spec, repl_spec, repl_spec, repl_spec), out_specs=(tok_spec, repl_spec, exp_spec, exp_spec, exp_spec, repl_spec, repl_spec, repl_spec), check_vma=False)
```

```python
import functools
import jax
import jax.numpy as jnp
from jax import lax
from jax.experimental import pallas as pl
from jax.experimental.pallas import tpu as pltpu
from jax.sharding import PartitionSpec as P

ALL_AXES = ("ep", "dp")
GROUP = 8
UNROLL = 8
VMEM_LIMIT = 62 << 20
LOW, HIGH = range(2)
OWN, X, Y, FAR = range(4)
COST = pl.CostEstimate(flops=20_000_000_000, bytes_accessed=20_000_000, transcendentals=0)
F32 = jnp.float32
BF16 = jnp.bfloat16


def dot(left, right, left_dim, right_dim):
    return lax.dot_general(left, right, (((left_dim,), (right_dim,)), ((), ())), preferred_element_type=F32)


def dot_nn(left, right):
    return dot(left, right, 1, 0)


def dot_nt(left, right):
    return dot(left, right, 1, 1)


def dot_tn(left, right):
    return dot(left, right, 0, 0)


def silu_parts(pre_act):
    sigma = jax.nn.sigmoid(pre_act)
    return pre_act * sigma, sigma * (1.0 + pre_act * (1.0 - sigma))


def route(meta_ref, layer, src, first_expert, capacity, pick_ref, slot, tok_ref=None):
    top = meta_ref.shape[1] // 4
    tokens = meta_ref.shape[2]
    start = 2 * layer * top
    slots = meta_ref[src, start : start + top, :].astype(jnp.int32)
    gates = meta_ref[src, start + top : start + 2 * top, :]
    expert = slots // capacity - first_expert
    row = (slots % capacity).astype(F32)
    which = lax.broadcasted_iota(jnp.int32, (GROUP, tokens), 0)
    row_of = jnp.full((GROUP, tokens), -1.0, F32)
    gate_of = jnp.zeros((GROUP, tokens), F32)
    for j in range(top):
        hit = expert[j : j + 1, :] == which
        row_of = jnp.where(hit, row[j : j + 1, :], row_of)
        gate_of = jnp.where(hit, gates[j : j + 1, :], gate_of)
    if tok_ref is not None:
        width = tok_ref.shape[1] - 4 * GROUP
        high = gate_of.astype(BF16)
        rest = gate_of - high.astype(F32)
        middle = rest.astype(BF16)
        low = (rest - middle.astype(F32)).astype(BF16)
        tok_ref[src, width : width + 4 * GROUP, :] = jnp.concatenate([high, middle, low, jnp.zeros_like(low)], axis=0)
    step = 16
    rows = lax.broadcasted_iota(jnp.int32, (step, tokens), 0).astype(F32).astype(BF16)
    for k in range(GROUP):
        wanted = jnp.broadcast_to(row_of[k : k + 1, :], (step, tokens)).astype(BF16)
        for h in range(capacity // step):
            hit = wanted == rows + jnp.asarray(h * step, BF16)
            start = k * capacity + h * step
            pick_ref[slot, src, start : start + step, :] = jnp.where(hit, jnp.asarray(1, BF16), jnp.asarray(0, BF16))


def gate_column(found, capacity):
    width = found.shape[1] - 4 * GROUP
    gates = []
    for k in range(GROUP):
        rows = found[k * capacity : (k + 1) * capacity, :]
        gates.append(rows[:, width + k : width + k + 1] + rows[:, width + GROUP + k : width + GROUP + k + 1] + rows[:, width + 2 * GROUP + k : width + 2 * GROUP + k + 1])
    return jnp.concatenate(gates, axis=0)


def schedule(groups, sources, begin, wait, dispatch, expert, combine, finish):
    group = pl.program_id(0)

    @pl.when(group == 0)
    def _():
        begin()

        def first(src, carry):
            wait(src)
            dispatch(src)
            return carry

        lax.fori_loop(0, sources, first, 0)

    @pl.when((group > 0) & (group < groups))
    def _():
        def middle(src, carry):
            combine(src)
            dispatch(src)
            return carry

        lax.fori_loop(0, sources, middle, 0)

    @pl.when(group < groups)
    def _():
        def one(k, carry):
            expert(k)
            return carry

        lax.fori_loop(0, GROUP, one, 0, unroll=UNROLL)

    @pl.when(group == groups)
    def _():
        def last(src, carry):
            finish(src)
            return carry

        lax.fori_loop(0, sources, last, 0)


def start_all(copies):
    for copy in copies:
        copy.start()


def wait_all(copies):
    for copy in copies:
        copy.wait()


def fwd_kernel(layer, capacity, groups, base_ref, meta_ref, w1_ref, w3_ref, w2_ref, tokens_ref, out_ref, xs_ref, sum_ref, tok_ref, pick_ref, gate_ref, x_ref, o_ref, sem, out_sem, save_sem):
    group = pl.program_id(0)
    sources = tok_ref.shape[0]
    width = w1_ref.shape[1]
    now = group % 2
    before = 1 - now

    def load(src):
        return pltpu.make_async_copy(tokens_ref.at[src], tok_ref.at[src, pl.ds(0, width)], sem.at[src])

    def begin():
        for src in range(sources):
            load(src).start()

    def dispatch(src):
        route(meta_ref, layer, src, base_ref[0] + group * GROUP, capacity, pick_ref, now, tok_ref)
        found = dot_nt(pick_ref[now, src], tok_ref[src])
        x_ref[now, src] = found.astype(BF16)
        gate_ref[src] = gate_column(found, capacity)

    def expert(k):
        here = pl.ds(pl.multiple_of(k * capacity, capacity), capacity)
        x = x_ref[now, :, here, :width].reshape(sources * capacity, width)
        ff = w1_ref.shape[2]
        a = dot_nn(x, jnp.concatenate([w1_ref[k], w3_ref[k]], axis=1))
        hidden = (jax.nn.silu(a[:, :ff]) * a[:, ff:]).astype(BF16)
        out = dot_nt(hidden, w2_ref[k]).astype(BF16).astype(F32)
        gate = gate_ref[:, here, :].reshape(sources * capacity, 1)
        o_ref[:, here, :] = (gate * out).reshape(sources, capacity, width)

    def added(src):
        rest = o_ref[src].T
        pick = pick_ref[before, src]
        parts = []
        for _ in range(3):
            parts.append(rest.astype(BF16))
            rest = rest - parts[-1].astype(F32)
        return dot_nn(parts[0], pick) + dot_nn(parts[1], pick) + dot_nn(parts[2], pick)

    def combine(src):
        @pl.when(group == 1)
        def _():
            sum_ref[src] = jnp.zeros(sum_ref.shape[1:], F32)

        sum_ref[src] += added(src)

    def store(src):
        return pltpu.make_async_copy(sum_ref.at[src], out_ref.at[src], out_sem.at[src])

    def finish(src):
        sum_ref[src] += added(src)
        store(src).start()

    def saves(step):
        slot = step % 2
        return [pltpu.make_async_copy(kept.at[slot], to.at[step], save_sem.at[slot, n]) for n, (kept, to) in enumerate(((x_ref, xs_ref),))]

    @pl.when(group >= 2)
    def _():
        wait_all(saves(group - 2))

    schedule(groups, sources, begin, lambda src: load(src).wait(), dispatch, expert, combine, finish)

    @pl.when(group < groups)
    def _():
        start_all(saves(group))

    @pl.when(group == groups)
    def _():
        wait_all(saves(group - 1))
        for src in range(sources):
            store(src).wait()


def bwd_kernel(layer, capacity, groups, held, pieces, keeps, base_ref, meta_ref, w1_ref, w3_ref, w2_ref, *refs):
    given_ref, piece_refs, other_refs, refs = refs[0], refs[1 : 1 + pieces], refs[1 + pieces : 1 + pieces + held], refs[1 + pieces + held :]
    out_ref, d1_ref, d3_ref, d2_ref, sum_ref, grad_ref, pick_ref, x_ref, g_ref, r_ref, d_ref, sem, grad_sem, out_sem, d_sem, from_ref = refs[:16]
    d_refs = (d1_ref, d3_ref, d2_ref)
    group = pl.program_id(0)
    sources = sum_ref.shape[0]
    width = w1_ref.shape[1]
    now = group % 2
    before = 1 - now
    x_slot = now if keeps else 0

    def load(src):
        return pltpu.make_async_copy(given_ref.at[src], from_ref.at[src, pl.ds(0, width)], sem.at[src])

    def loads_saved(step):
        return [pltpu.make_async_copy(given_ref.at[step], x_ref.at[step % 2], sem.at[step % 2])]

    def load_grad(src):
        piece = piece_refs[0].at[src] if pieces == 1 else piece_refs[src]
        return pltpu.make_async_copy(piece, grad_ref.at[src], grad_sem.at[src])

    def begin():
        if keeps:
            start_all(loads_saved(0))
        for src in range(sources):
            if not keeps:
                load(src).start()
            load_grad(src).start()
        if keeps:
            wait_all(loads_saved(0))

    def wait(src):
        if not keeps:
            load(src).wait()
        pltpu.make_async_copy(grad_ref.at[src], grad_ref.at[src], grad_sem.at[src]).wait()

    def dispatch(src):
        if keeps:
            route(meta_ref, layer, src, base_ref[0] + group * GROUP, capacity, pick_ref, now)
            gate = gate_column(x_ref[now, src].astype(F32), capacity)
        else:
            route(meta_ref, layer, src, base_ref[0] + group * GROUP, capacity, pick_ref, now, from_ref)
            found = dot_nt(pick_ref[now, src], from_ref[src])
            gate = gate_column(found, capacity)
            x_ref[0, src] = found.astype(BF16)
        g_ref[src] = (gate * dot_nt(pick_ref[now, src], grad_ref[src])).astype(BF16)

    def next_saved():
        @pl.when((group > 0) & (group < groups))
        def _():
            wait_all(loads_saved(group))

        @pl.when(group < groups - 1)
        def _():
            start_all(loads_saved(group + 1))

    def expert(k):
        here = pl.ds(pl.multiple_of(k * capacity, capacity), capacity)
        x = x_ref[x_slot, :, here, :width].reshape(sources * capacity, width)
        g = g_ref[:, here, :].reshape(sources * capacity, width)
        ff = w1_ref.shape[2]
        both = jnp.concatenate([w1_ref[k], w3_ref[k]], axis=1)
        a = dot_nn(x, both)
        a_three = a[:, ff:]
        act, slope = silu_parts(a[:, :ff])
        hidden = (act * a_three).astype(BF16)
        grad_hidden = dot_nn(g, w2_ref[k])
        grad_one = (grad_hidden * a_three * slope).astype(BF16)
        grad_three = (grad_hidden * act).astype(BF16)
        grads = jnp.concatenate([grad_one, grad_three], axis=1)
        r_ref[:, here, :] = dot_nt(grads, both).astype(BF16).reshape(sources, capacity, width)
        d13 = dot_tn(x, grads).astype(BF16)
        d2 = dot_tn(g, hidden).astype(BF16)
        for i, value in enumerate((d13[:, :ff], d13[:, ff:], d2)):
            d_ref[now, i, k] = value

    def added(src):
        return dot_tn(r_ref[src], pick_ref[before, src])

    def combine(src):
        @pl.when(group == 1)
        def _():
            sum_ref[src] = jnp.zeros(sum_ref.shape[1:], F32)

        sum_ref[src] += added(src)

    def store(src):
        return pltpu.make_async_copy(grad_ref.at[src], out_ref.at[src], out_sem.at[src])

    def finish(src):
        grad_ref[src] = (sum_ref[src] + added(src)).astype(BF16)
        store(src).start()

    def experts_at(start, step):
        return pl.ds(pl.multiple_of((start + step) * GROUP, GROUP), GROUP)

    def d_stores(step):
        slot = step % 2
        return [pltpu.make_async_copy(d_ref.at[slot, i], d_refs[i].at[layer, experts_at(base_ref[1], step)], d_sem.at[slot, i]) for i in range(3)]

    def other_load(step):
        return pltpu.make_async_copy(other_refs[0].at[:, experts_at(0, step)], refs[16].at[step % 2], refs[17].at[step % 2, 3])

    def other_stores(step):
        slot = step % 2
        return [pltpu.make_async_copy(refs[16].at[slot, i], d_refs[i].at[1 - layer, experts_at(base_ref[2], step)], refs[17].at[slot, i]) for i in range(3)]

    @pl.when(group >= 2)
    def _():
        wait_all(d_stores(group - 2))
        if held:
            wait_all(other_stores(group - 2))

    if held:
        @pl.when(group >= 1)
        def _():
            other_load(group - 1).wait()
            start_all(other_stores(group - 1))

        @pl.when(group < groups)
        def _():
            other_load(group).start()

    if keeps:
        next_saved()

    schedule(groups, sources, begin, wait, dispatch, expert, combine, finish)

    @pl.when(group < groups)
    def _():
        start_all(d_stores(group))

    @pl.when(group == groups)
    def _():
        wait_all(d_stores(group - 1))
        if held:
            wait_all(other_stores(group - 1))
        for src in range(sources):
            store(src).wait()


def weight_specs(layer, groups, width, ff):
    spec = pl.BlockSpec((None, GROUP, width, ff), lambda g, base: (layer, base[1] + jnp.minimum(g, groups - 1), 0, 0))
    return [spec, spec, spec]


def whole():
    return pl.BlockSpec(memory_space=pltpu.VMEM)


def anywhere():
    return pl.BlockSpec(memory_space=pl.ANY)


def expert_forward(layer, capacity, groups, base, tok, meta, w1, w3, w2):
    sources, width, tokens = tok.shape
    ff = w1.shape[3]
    rows = GROUP * capacity
    return pl.pallas_call(
        functools.partial(fwd_kernel, layer, capacity, groups),
        out_shape=(
            jax.ShapeDtypeStruct((sources, width, tokens), F32),
            jax.ShapeDtypeStruct((groups, sources, rows, width + 4 * GROUP), BF16),
        ),
        grid_spec=pltpu.PrefetchScalarGridSpec(
            num_scalar_prefetch=1,
            grid=(groups + 1,),
            in_specs=[whole()] + weight_specs(layer, groups, width, ff) + [anywhere()],
            out_specs=(anywhere(),) * 2,
            scratch_shapes=[
                pltpu.VMEM((sources, width, tokens), F32),
                pltpu.VMEM((sources, width + 4 * GROUP, tokens), BF16),
                pltpu.VMEM((2, sources, rows, tokens), BF16),
                pltpu.VMEM((sources, rows, 1), F32),
                pltpu.VMEM((2, sources, rows, width + 4 * GROUP), BF16),
                pltpu.VMEM((sources, rows, width), F32),
                pltpu.SemaphoreType.DMA((sources,)),
                pltpu.SemaphoreType.DMA((sources,)),
                pltpu.SemaphoreType.DMA((2, 1)),
            ],
        ),
        compiler_params=pltpu.CompilerParams(vmem_limit_bytes=VMEM_LIMIT),
        cost_estimate=COST,
    )(base, meta, w1, w3, w2, tok)


def expert_backward(layer, capacity, groups, base, given, keeps, grads, meta, w1, w3, w2, held):
    sources, tokens = meta.shape[0], meta.shape[2]
    width = w1.shape[2]
    ff = w1.shape[3]
    rows = GROUP * capacity
    pieces = len(grads)
    grad_shape = jax.ShapeDtypeStruct(w1.shape, BF16)
    block = pltpu.VMEM((2, 3, GROUP, width, ff), BF16)
    more = [block, pltpu.SemaphoreType.DMA((2, 4))] if held else []
    return pl.pallas_call(
        functools.partial(bwd_kernel, layer, capacity, groups, len(held), pieces, keeps),
        out_shape=(jax.ShapeDtypeStruct((sources, width, tokens), BF16), grad_shape, grad_shape, grad_shape),
        grid_spec=pltpu.PrefetchScalarGridSpec(
            num_scalar_prefetch=1,
            grid=(groups + 1,),
            in_specs=[whole()] + weight_specs(layer, groups, width, ff) + [anywhere()] * (1 + pieces + len(held)),
            out_specs=(anywhere(),) * 4,
            scratch_shapes=[
                pltpu.VMEM((sources, width, tokens), F32),
                pltpu.VMEM((sources, width, tokens), BF16),
                pltpu.VMEM((2, sources, rows, tokens), BF16),
                pltpu.VMEM((2 if keeps else 1, sources, rows, width + 4 * GROUP), BF16),
                pltpu.VMEM((sources, rows, width), BF16),
                pltpu.VMEM((sources, rows, width), BF16),
                block,
                pltpu.SemaphoreType.DMA((sources,)),
                pltpu.SemaphoreType.DMA((sources,)),
                pltpu.SemaphoreType.DMA((sources,)),
                pltpu.SemaphoreType.DMA((2, 4)),
                pltpu.VMEM((8, 128), BF16) if keeps else pltpu.VMEM((sources, width + 4 * GROUP, tokens), BF16),
            ]
            + more,
        ),
        input_output_aliases={7 + pieces + i: 1 + i for i in range(len(held) - 1)},
        compiler_params=pltpu.CompilerParams(vmem_limit_bytes=VMEM_LIMIT),
        cost_estimate=COST,
    )(base, meta, w1, w3, w2, given, *grads, *held)


def place_kernel(base_ref, recv_ref, *refs):
    for i in range(3):
        refs[3 + i][...] = recv_ref[i]


def place(layer, groups, base, recv, held):
    width, ff = recv.shape[2:]
    few = 8
    spec = pl.BlockSpec((None, few, width, ff), lambda g, base: (layer, base[2] * (GROUP // few) + g, 0, 0))
    shape = jax.ShapeDtypeStruct(held[0].shape, BF16)
    return pl.pallas_call(
        place_kernel,
        out_shape=(shape, shape, shape),
        grid_spec=pltpu.PrefetchScalarGridSpec(
            num_scalar_prefetch=1,
            grid=(groups * GROUP // few,),
            in_specs=[pl.BlockSpec((3, few, width, ff), lambda g, base: (0, g, 0, 0))] + [anywhere()] * 3,
            out_specs=(spec, spec, spec),
        ),
        input_output_aliases={2: 0, 3: 1, 4: 2},
        compiler_params=pltpu.CompilerParams(vmem_limit_bytes=VMEM_LIMIT),
        cost_estimate=COST,
    )(base, recv, *held)


def neighbours():
    ep = lax.axis_index("ep")
    dp = lax.axis_index("dp")
    return ({"ep": ep + 1 - 2 * (ep % 2), "dp": dp}, {"ep": (ep + 2) % 4, "dp": dp}, {"ep": ep, "dp": 1 - dp})


def greet(devices):
    barrier = pltpu.get_barrier_semaphore()
    for device in devices:
        pl.semaphore_signal(barrier, inc=1, device_id=device, device_id_type=pl.DeviceIdType.MESH)
    pl.semaphore_wait(barrier, len(devices))


def send_block(source, target, send, recv, device):
    made = pltpu.make_async_remote_copy(src_ref=source, dst_ref=target, send_sem=send, recv_sem=recv, device_id=device, device_id_type=pl.DeviceIdType.MESH)
    made.start()
    return made


def gather_phase(devices, own_refs, out_refs, land_refs, sems, shadows):
    by_x, by_y, partner = devices
    send_sem, recv_sem, store_sem = sems
    count = len(own_refs)
    stores = []

    made = [[] for _ in own_refs]

    def copy(which, source, target, half, device):
        rows = own_refs[which].shape[0]
        span = pl.ds(0, rows) if half is None else pl.ds(half * (rows // 2), rows // 2)
        block = land_refs[which].at[source, span] if source else own_refs[which].at[span]
        n = len(made[which])
        made[which].append(send_block(block, land_refs[which].at[target, span], send_sem.at[which, n], recv_sem.at[which, n], device))
        return made[which][n]

    def store(which, slot):
        block = land_refs[which].at[slot] if slot else own_refs[which]
        started = pltpu.make_async_copy(block, out_refs[which].at[slot], store_sem.at[which, slot])
        started.start()
        stores.append(started)

    near, far, pair = [], [], []
    for which in range(count):
        near.append([copy(which, OWN, X, LOW, by_x), copy(which, OWN, Y, HIGH, by_y), copy(which, OWN, X, HIGH, by_x), copy(which, OWN, Y, LOW, by_y)])
        pair.append(copy(which, OWN, 4, None, partner))
        store(which, OWN)
    shadows[0]()
    for which in range(count):
        x_low, y_high, x_high, y_low = near[which]
        x_low.wait_recv()
        relay_low = copy(which, X, FAR, LOW, by_y)
        y_high.wait_recv()
        relay_high = copy(which, Y, FAR, HIGH, by_x)
        if not far:
            shadows[1]()
        x_high.wait_recv()
        pair_x = copy(which, X, 4 + X, None, partner)
        store(which, X)
        y_low.wait_recv()
        pair_y = copy(which, Y, 4 + Y, None, partner)
        store(which, Y)
        pair[which].wait_recv()
        store(which, 4)
        far.append((relay_low, relay_high, pair_x, pair_y))
    for which in range(count):
        relay_low, relay_high, pair_x, pair_y = far[which]
        relay_low.wait_recv()
        pair_low = copy(which, FAR, 4 + FAR, LOW, partner)
        if which == 0:
            shadows[2]()
        relay_high.wait_recv()
        pair_high = copy(which, FAR, 4 + FAR, HIGH, partner)
        store(which, FAR)
        pair_x.wait_recv()
        store(which, 4 + X)
        pair_y.wait_recv()
        store(which, 4 + Y)
        pair_low.wait_recv()
        pair_high.wait_recv()
        store(which, 4 + FAR)
        for step in made[which]:
            step.wait_send()
    wait_all(stores)


def gather_scratch(*arrays):
    count = len(arrays)
    return [pltpu.VMEM((8,) + x.shape, x.dtype) for x in arrays] + [pltpu.SemaphoreType.DMA((count, n)) for n in (11, 11, 8)]


def reduce_phase(devices, part_ref, out_ref, scratch, extras, shadow):
    mine_ref, pair_ref, stage_ref, relay_ref, last_ref, send_sem, recv_sem, load_sem = scratch
    by_x, by_y, partner = devices
    rows = part_ref.shape[1]
    half = rows // 2
    low, high, full = pl.ds(0, half), pl.ds(half, half), pl.ds(0, rows)
    wire = part_ref.dtype

    made = []

    def copy(source, target, device):
        n = len(made)
        made.append(send_block(source, target, send_sem.at[n], recv_sem.at[n], device))
        return made[n]

    def chip_sum(i, span):
        return mine_ref[i, span, :].astype(F32) + pair_ref[i, span, :].astype(F32)

    loads, pair = {}, {}
    for i in (FAR, X, Y, OWN):
        loads[i] = pltpu.make_async_copy(part_ref.at[i], mine_ref.at[i], load_sem.at[i])
        loads[i].start()
        pair[i] = copy(part_ref.at[4 + i], pair_ref.at[i], partner)

    def ready(i):
        loads[i].wait()
        pair[i].wait_recv()

    ready(FAR)
    stage_ref[OWN, low, :] = chip_sum(FAR, low).astype(wire)
    relay_x = copy(stage_ref.at[OWN, low], relay_ref.at[LOW], by_x)
    stage_ref[OWN, high, :] = chip_sum(FAR, high).astype(wire)
    relay_y = copy(stage_ref.at[OWN, high], relay_ref.at[HIGH], by_y)
    ready(X)
    stage_ref[X, low, :] = chip_sum(X, low).astype(wire)
    arrive = [copy(stage_ref.at[X, low], last_ref.at[LOW, low], by_x)]
    ready(Y)
    stage_ref[Y, high, :] = chip_sum(Y, high).astype(wire)
    arrive.append(copy(stage_ref.at[Y, high], last_ref.at[HIGH, high], by_y))
    others = [copy(source, target, partner) for source, target in extras]
    relay_y.wait_recv()
    stage_ref[X, high, :] = (chip_sum(X, high) + relay_ref[HIGH].astype(F32)).astype(wire)
    arrive.append(copy(stage_ref.at[X, high], last_ref.at[LOW, high], by_x))
    relay_x.wait_recv()
    stage_ref[Y, low, :] = (chip_sum(Y, low) + relay_ref[LOW].astype(F32)).astype(wire)
    arrive.append(copy(stage_ref.at[Y, low], last_ref.at[HIGH, low], by_y))
    ready(OWN)
    out_ref[...] = chip_sum(OWN, full)
    shadow()
    for step in arrive:
        step.wait_recv()
    out_ref[...] += last_ref[LOW].astype(F32) + last_ref[HIGH].astype(F32)

    def drain():
        for step in others:
            step.wait_recv()
        for step in made:
            step.wait_send()

    return drain


def reduce_scratch(part):
    rows, tokens = part.shape[1:]
    return [
        pltpu.VMEM((4, rows, tokens), part.dtype),
        pltpu.VMEM((4, rows, tokens), part.dtype),
        pltpu.VMEM((3, rows, tokens), part.dtype),
        pltpu.VMEM((2, rows // 2, tokens), part.dtype),
        pltpu.VMEM((2, rows, tokens), part.dtype),
        pltpu.SemaphoreType.DMA((13,)),
        pltpu.SemaphoreType.DMA((13,)),
        pltpu.SemaphoreType.DMA((4,)),
    ]


def nothing():
    pass


def mix(x_ref, w_dense):
    x = x_ref[...]
    return (x.astype(F32) + dot_tn(w_dense, x)).astype(BF16)


def shared_forward(mixed, ws_gate, ws_up):
    s_one = dot_tn(ws_gate, mixed)
    s_three = dot_tn(ws_up, mixed)
    return s_one, s_three, (jax.nn.silu(s_one) * s_three).astype(BF16)


def shared_backward(grad_y, mixed, ws_gate, ws_up, ws_down, pack_ref, start):
    s_one, s_three, shared_hidden = shared_forward(mixed, ws_gate, ws_up)
    act_one, slope = silu_parts(s_one)
    grad_shared = dot_tn(ws_down, grad_y)
    grad_s_one = (grad_shared * s_three * slope).astype(BF16)
    grad_s_three = (grad_shared * act_one).astype(BF16)
    ff = ws_gate.shape[1]
    for i, value in enumerate((dot_nt(mixed, grad_s_one), dot_nt(mixed, grad_s_three), dot_nt(grad_y, shared_hidden))):
        pack_ref[:, start + i * ff : start + (i + 1) * ff] = value.astype(BF16)
    return dot_nn(ws_gate, grad_s_one) + dot_nn(ws_up, grad_s_three)


def comm_call(kernel, cid, out_shape, in_specs, out_specs, scratch, operands):
    return pl.pallas_call(
        kernel,
        out_shape=out_shape,
        in_specs=in_specs,
        out_specs=out_specs,
        scratch_shapes=scratch,
        compiler_params=pltpu.CompilerParams(collective_id=cid, has_side_effects=True, vmem_limit_bytes=VMEM_LIMIT),
        cost_estimate=COST,
    )(*operands)


def first_kernel(x_ref, w_dense_ref, meta_ref, tok_ref, metas_ref, own_ref, land_ref, land_meta_ref, *sems):
    devices = neighbours()
    own_ref[...] = mix(x_ref, w_dense_ref[0])
    greet(devices)
    gather_phase(devices, [own_ref, meta_ref], [tok_ref, metas_ref], [land_ref, land_meta_ref], sems, (nothing,) * 3)


def first_exchange(x, w_dense, meta):
    outs = (jax.ShapeDtypeStruct((8,) + x.shape, BF16), jax.ShapeDtypeStruct((8,) + meta.shape, F32), jax.ShapeDtypeStruct(x.shape, BF16))
    return comm_call(first_kernel, 0, outs, [whole()] * 3, (anywhere(), anywhere(), whole()), gather_scratch(x, meta), (x, w_dense, meta))


def forward_kernel(part_ref, u1_ref, ws_gate_ref, ws_up_ref, ws_down_ref, w_dense_ref, tok_ref, x2_ref, u2_ref, sum_ref, shared_ref, *scratch):
    devices = neighbours()
    greet(devices)

    def shadow():
        hidden = shared_forward(u1_ref[...], ws_gate_ref[0], ws_up_ref[0])[2]
        shared_ref[...] = dot_nn(ws_down_ref[0], hidden)

    drain = reduce_phase(devices, part_ref, sum_ref, scratch[:8], [], shadow)
    x2_ref[...] = (u1_ref[...].astype(F32) + sum_ref[...] + shared_ref[...]).astype(BF16)
    u2_ref[...] = mix(x2_ref, w_dense_ref[1])
    gather_phase(devices, [u2_ref], [tok_ref], [scratch[8]], scratch[9:], (nothing,) * 3)
    drain()


def forward_exchange(part, u1, ws_gate, ws_up, ws_down_t, w_dense):
    outs = (jax.ShapeDtypeStruct((8,) + u1.shape, BF16), jax.ShapeDtypeStruct(u1.shape, BF16), jax.ShapeDtypeStruct(u1.shape, BF16))
    scratch = [pltpu.VMEM(u1.shape, F32), pltpu.VMEM(u1.shape, F32)] + reduce_scratch(part) + gather_scratch(u1)
    specs = [anywhere()] + [whole()] * 5
    return comm_call(forward_kernel, 1, outs, specs, (anywhere(), whole(), whole()), scratch, (part, u1, ws_gate, ws_up, ws_down_t, w_dense))


def expert_half(refs, layer, target_ref):
    own = target_ref.shape[1]
    start = lax.axis_index("dp") * own
    return [(ref.at[layer, pl.ds(start, own)], target_ref.at[i]) for i, ref in enumerate(refs)]


def pair_half(partner, pack_ref, land_ref, sems):
    half = land_ref.shape[0]
    dp = lax.axis_index("dp")
    sent = []

    def start():
        theirs = pack_ref.at[pl.ds(pl.multiple_of((1 - dp) * half, 16), half)]
        sent.append(send_block(theirs, land_ref, sems.at[0], sems.at[1], partner))

    def finish():
        sent[0].wait()
        mine = pack_ref[pl.ds(pl.multiple_of(dp * half, 16), half), :]
        return (mine.astype(F32) + land_ref[...].astype(F32)).astype(BF16)

    return start, finish


def pair_scratch(shape):
    return [pltpu.VMEM(shape, BF16), pltpu.VMEM((shape[0] // 2, shape[1]), BF16), pltpu.SemaphoreType.DMA((2,))]


def backward_kernel(part_ref, d1_ref, d3_ref, d2_ref, grad_y_ref, x2_ref, u2_ref, u1_ref, w_dense_ref, ws_gate_ref, ws_up_ref, ws_down_ref, *refs):
    grad_all_ref, recv_ref, grad_x_ref, back_ref, chip_ref, sum_ref, mixed_ref, pack_ref, land_ref, pair_sem = refs[:10]
    scratch = refs[10:]
    devices = neighbours()
    greet(devices)
    ff = ws_gate_ref.shape[2]
    width = x2_ref.shape[0]
    start_pair, finish_pair = pair_half(devices[2], pack_ref, land_ref, pair_sem)

    def shadow():
        back_ref[...] = shared_backward(grad_y_ref[...], u2_ref[...], ws_gate_ref[1], ws_up_ref[1], ws_down_ref[1], pack_ref, 0)

    drain = reduce_phase(devices, part_ref, sum_ref, scratch[:8], expert_half((d1_ref, d3_ref, d2_ref), 1, recv_ref), shadow)
    mixed_ref[...] = (grad_y_ref[...].astype(F32) + sum_ref[...] + back_ref[...]).astype(BF16)
    grad_x_ref[...] = (mixed_ref[...].astype(F32) + dot_nn(w_dense_ref[1], mixed_ref[...])).astype(BF16)

    def dense_part():
        pack_ref[:, 6 * ff : 6 * ff + width] = dot_nt(x2_ref[...], mixed_ref[...]).astype(BF16)
        pack_ref[:, 6 * ff + width :] = jnp.zeros((width, pack_ref.shape[1] - 6 * ff - width), BF16)

    def shared_part():
        back_ref[...] = shared_backward(grad_x_ref[...], u1_ref[...], ws_gate_ref[0], ws_up_ref[0], ws_down_ref[0], pack_ref, 3 * ff)

    gather_phase(devices, [grad_x_ref], [grad_all_ref], [scratch[8]], scratch[9:], (dense_part, shared_part, start_pair))
    chip_ref[...] = finish_pair()
    drain()


def backward_exchange(part, held, grad_y, x2, u2, u1, w_dense, ws_gate, ws_up, ws_down_t):
    ff = ws_gate.shape[2]
    width = x2.shape[0]
    packed = 6 * ff + width + -(6 * ff + width) % 128
    own = held[0].shape[1] // 2
    outs = (
        jax.ShapeDtypeStruct((8,) + x2.shape, BF16),
        jax.ShapeDtypeStruct((3, own) + held[0].shape[2:], BF16),
        jax.ShapeDtypeStruct(x2.shape, BF16),
        jax.ShapeDtypeStruct(x2.shape, F32),
        jax.ShapeDtypeStruct((width // 2, packed), BF16),
    )
    scratch = [pltpu.VMEM(x2.shape, F32), pltpu.VMEM(x2.shape, BF16)] + pair_scratch((width, packed)) + reduce_scratch(part) + gather_scratch(x2)
    operands = (part, *held, grad_y, x2, u2, u1, w_dense, ws_gate, ws_up, ws_down_t)
    specs = [anywhere()] * 4 + [whole()] * 8
    return comm_call(backward_kernel, 2, outs, specs, (anywhere(), anywhere()) + (whole(),) * 3, scratch, operands)


def last_kernel(part_ref, d1_ref, d3_ref, d2_ref, grad_y_ref, back_ref, x_ref, w_dense_ref, grad_x_ref, recv_ref, chip_ref, sum_ref, mixed_ref, pack_ref, land_ref, pair_sem, *scratch):
    devices = neighbours()
    greet(devices)
    start_pair, finish_pair = pair_half(devices[2], pack_ref, land_ref, pair_sem)
    drain = reduce_phase(devices, part_ref, sum_ref, scratch, expert_half((d1_ref, d3_ref, d2_ref), 0, recv_ref), nothing)
    mixed_ref[...] = (grad_y_ref[...].astype(F32) + sum_ref[...] + back_ref[...]).astype(BF16)
    pack_ref[...] = dot_nt(x_ref[...], mixed_ref[...]).astype(BF16)
    grad_x_ref[...] = (mixed_ref[...].astype(F32) + dot_nn(w_dense_ref[0], mixed_ref[...])).astype(BF16)
    start_pair()
    drain()
    chip_ref[...] = finish_pair()


def last_exchange(part, held, grad_y, back, x, w_dense):
    own = held[0].shape[1] // 2
    width = x.shape[0]
    outs = (jax.ShapeDtypeStruct(x.shape, BF16), jax.ShapeDtypeStruct((3, own) + held[0].shape[2:], BF16), jax.ShapeDtypeStruct((width // 2, width), BF16))
    scratch = [pltpu.VMEM(x.shape, F32), pltpu.VMEM(x.shape, BF16)] + pair_scratch((width, width)) + reduce_scratch(part)
    specs = [anywhere()] * 4 + [whole()] * 4
    return comm_call(last_kernel, 3, outs, specs, (whole(), anywhere(), whole()), scratch, (part, *held, grad_y, back, x, w_dense))


def send_over(x, flip):
    return lax.ppermute(x, "ep", [(i, i ^ flip) for i in range(4)])


def swap_cores(x):
    return lax.ppermute(x, "dp", [(0, 1), (1, 0)])


def sum_start(chip):
    sent = [chip]
    for flip in (1, 2, 3):
        sent.append(send_over(chip, flip))
    return sent


def sum_finish(parts):
    total = sum(part.astype(F32) for part in parts).astype(BF16)
    other = swap_cores(total)
    first = lax.axis_index("dp") == 0
    return jnp.concatenate([jnp.where(first, total, other), jnp.where(first, other, total)], axis=0)


def solution(mesh):
    ep_size = mesh.shape["ep"]
    dp_size = mesh.shape["dp"]
    tok_spec = P(ALL_AXES)
    route_spec = P(None, ALL_AXES)
    exp_spec = P(None, "ep")
    repl_spec = P()

    def body(act_in, grad_out, slot_ids, gate_vals, w_dense, w_gate, w_up, w_down, ws_gate, ws_up, ws_down):
        layers, local_exp = w_gate.shape[:2]
        tokens = act_in.shape[0]
        top = slot_ids.shape[2]
        own = local_exp // dp_size
        groups = own // GROUP
        capacity = 2 * tokens * top // (local_exp * ep_size)
        dp = lax.axis_index("dp")
        base = jnp.stack([lax.axis_index("ep") * local_exp + dp * own, dp * groups, (dp_size - 1 - dp) * groups]).astype(jnp.int32)
        w_down_t = jnp.swapaxes(w_down, 2, 3)
        meta = jnp.concatenate([jnp.swapaxes(slot_ids, 1, 2).astype(F32), jnp.swapaxes(gate_vals, 1, 2)], axis=1)
        meta = meta.reshape(layers * 2 * top, tokens)

        x1 = act_in.T
        grad_y2 = grad_out.T
        shared_w = (ws_gate, ws_up, jnp.swapaxes(ws_down, 1, 2))
        tok1, metas, u1 = first_exchange(x1, w_dense, meta)
        tok1, grad_y2 = lax.optimization_barrier((tok1, grad_y2))
        grads2 = [grad_y2, send_over(grad_y2, 1), send_over(grad_y2, 2), send_over(grad_y2, 3)]
        grads2 = grads2 + [swap_cores(x) for x in grads2]
        part, rows1 = expert_forward(0, capacity, groups, base, tok1, metas, w_gate, w_up, w_down_t)
        tok2, x2, u2 = forward_exchange(part, u1, *shared_w, w_dense)
        back2, *held = expert_backward(1, capacity, groups, base, tok2, False, grads2, metas, w_gate, w_up, w_down_t, [])
        grad1_all, recv2, grad_y1, shared1, early = backward_exchange(back2, held, grad_y2, x2, u2, u1, w_dense, *shared_w)
        ff = ws_gate.shape[2]
        width = w_dense.shape[1]
        early = sum_start(early)
        grad1_all, early[0] = lax.optimization_barrier((grad1_all, early[0]))
        back1, *held = expert_backward(0, capacity, groups, base, rows1, True, [grad1_all], metas, w_gate, w_up, w_down_t, [recv2] + held)
        grad_x, recv1, late = last_exchange(back1, held, grad_y1, shared1, x1, w_dense)
        late = sum_start(late)
        g_gate, g_up, g_down = place(0, groups, base, recv1, held)
        g_gate, late = lax.optimization_barrier((g_gate, late))
        g_down = jnp.swapaxes(g_down, 2, 3)
        early = sum_finish(early)
        late = sum_finish(late)
        g_dense = jnp.stack([late, early[:, 6 * ff : 6 * ff + width]])
        shared = [jnp.stack([early[:, (3 + i) * ff : (4 + i) * ff], early[:, i * ff : (i + 1) * ff]]) for i in range(3)]
        return (grad_x.T, g_dense, g_gate, g_up, g_down, shared[0], shared[1], jnp.swapaxes(shared[2], 1, 2))

    return jax.shard_map(body, mesh=mesh, in_specs=(tok_spec, tok_spec, route_spec, route_spec, repl_spec, exp_spec, exp_spec, exp_spec, repl_spec, repl_spec, repl_spec), out_specs=(tok_spec, repl_spec, exp_spec, exp_spec, exp_spec, repl_spec, repl_spec, repl_spec), check_vma=False)
```

```python
import functools
import jax
import jax.numpy as jnp
from jax import lax
from jax.experimental import pallas as pl
from jax.experimental.pallas import tpu as pltpu
from jax.sharding import PartitionSpec as P

ALL_AXES = ("ep", "dp")
GROUP = 8
UNROLL = 8
VMEM_LIMIT = 62 << 20
LOW, HIGH = range(2)
OWN, X, Y, FAR = range(4)
COST = pl.CostEstimate(flops=20_000_000_000, bytes_accessed=20_000_000, transcendentals=0)
F32 = jnp.float32
BF16 = jnp.bfloat16


def dot(left, right, left_dim, right_dim):
    return lax.dot_general(left, right, (((left_dim,), (right_dim,)), ((), ())), preferred_element_type=F32)


def dot_nn(left, right):
    return dot(left, right, 1, 0)


def dot_nt(left, right):
    return dot(left, right, 1, 1)


def dot_tn(left, right):
    return dot(left, right, 0, 0)


def silu_parts(pre_act):
    sigma = jax.nn.sigmoid(pre_act)
    return pre_act * sigma, sigma * (1.0 + pre_act * (1.0 - sigma))


def route(meta_ref, layer, src, first_expert, capacity, pick_ref, slot, tok_ref=None, weigh_ref=None):
    top = meta_ref.shape[1] // 4
    tokens = meta_ref.shape[2]
    start = 2 * layer * top
    slots = meta_ref[src, start : start + top, :].astype(jnp.int32)
    gates = meta_ref[src, start + top : start + 2 * top, :]
    expert = slots // capacity - first_expert
    row = (slots % capacity).astype(F32)
    which = lax.broadcasted_iota(jnp.int32, (GROUP, tokens), 0)
    row_of = jnp.full((GROUP, tokens), -1.0, F32)
    gate_of = jnp.zeros((GROUP, tokens), F32)
    for j in range(top):
        hit = expert[j : j + 1, :] == which
        row_of = jnp.where(hit, row[j : j + 1, :], row_of)
        gate_of = jnp.where(hit, gates[j : j + 1, :], gate_of)
    if tok_ref is not None:
        width = tok_ref.shape[1] - 4 * GROUP
        high = gate_of.astype(BF16)
        rest = gate_of - high.astype(F32)
        middle = rest.astype(BF16)
        low = (rest - middle.astype(F32)).astype(BF16)
        tok_ref[src, width : width + 4 * GROUP, :] = jnp.concatenate([high, middle, low, jnp.zeros_like(low)], axis=0)
    step = 16
    rows = lax.broadcasted_iota(jnp.int32, (step, tokens), 0).astype(F32).astype(BF16)
    for k in range(GROUP):
        wanted = jnp.broadcast_to(row_of[k : k + 1, :], (step, tokens)).astype(BF16)
        if weigh_ref is not None:
            parts = [jnp.broadcast_to(part[k : k + 1, :].astype(F32), (step, tokens)).astype(BF16) for part in (high, middle, low)]
        for h in range(capacity // step):
            hit = wanted == rows + jnp.asarray(h * step, BF16)
            start = k * capacity + h * step
            pick_ref[slot, src, start : start + step, :] = jnp.where(hit, jnp.asarray(1, BF16), jnp.asarray(0, BF16))
            if weigh_ref is not None:
                for i, part in enumerate(parts):
                    weigh_ref[slot, i, src, start : start + step, :] = jnp.where(hit, part, jnp.asarray(0, BF16))


def gate_column(found, capacity):
    width = found.shape[1] - 4 * GROUP
    gates = []
    for k in range(GROUP):
        rows = found[k * capacity : (k + 1) * capacity, :]
        gates.append(rows[:, width + k : width + k + 1] + rows[:, width + GROUP + k : width + GROUP + k + 1] + rows[:, width + 2 * GROUP + k : width + 2 * GROUP + k + 1])
    return jnp.concatenate(gates, axis=0)


def schedule(groups, sources, begin, wait, dispatch, expert, combine, finish):
    group = pl.program_id(0)

    @pl.when(group == 0)
    def _():
        begin()

        def first(src, carry):
            wait(src)
            dispatch(src)
            return carry

        lax.fori_loop(0, sources, first, 0)

    @pl.when((group > 0) & (group < groups))
    def _():
        def middle(src, carry):
            combine(src)
            dispatch(src)
            return carry

        lax.fori_loop(0, sources, middle, 0)

    @pl.when(group < groups)
    def _():
        def one(k, carry):
            expert(k)
            return carry

        lax.fori_loop(0, GROUP, one, 0, unroll=UNROLL)

    @pl.when(group == groups)
    def _():
        def last(src, carry):
            finish(src)
            return carry

        lax.fori_loop(0, sources, last, 0)


def start_all(copies):
    for copy in copies:
        copy.start()


def wait_all(copies):
    for copy in copies:
        copy.wait()


def fwd_kernel(layer, capacity, groups, base_ref, meta_ref, w1_ref, w3_ref, w2_ref, tokens_ref, out_ref, xs_ref, sum_ref, tok_ref, pick_ref, weigh_ref, x_ref, o_ref, sem, out_sem, save_sem):
    group = pl.program_id(0)
    sources = tok_ref.shape[0]
    width = w1_ref.shape[1]
    now = group % 2
    before = 1 - now

    def load(src):
        return pltpu.make_async_copy(tokens_ref.at[src], tok_ref.at[src, pl.ds(0, width)], sem.at[src])

    def begin():
        for src in range(sources):
            load(src).start()

    def dispatch(src):
        route(meta_ref, layer, src, base_ref[0] + group * GROUP, capacity, pick_ref, now, tok_ref, weigh_ref)
        found = dot_nt(pick_ref[now, src], tok_ref[src])
        x_ref[now, src] = found.astype(BF16)

    def expert(k):
        here = pl.ds(pl.multiple_of(k * capacity, capacity), capacity)
        x = x_ref[now, :, here, :width].reshape(sources * capacity, width)
        ff = w1_ref.shape[2]
        a = dot_nn(x, jnp.concatenate([w1_ref[k], w3_ref[k]], axis=1))
        hidden = (jax.nn.silu(a[:, :ff]) * a[:, ff:]).astype(BF16)
        o_ref[:, here, :] = dot_nt(hidden, w2_ref[k]).astype(BF16).reshape(sources, capacity, width)

    def added(src):
        rows = o_ref[src]
        return dot_tn(rows, weigh_ref[before, 0, src]) + dot_tn(rows, weigh_ref[before, 1, src]) + dot_tn(rows, weigh_ref[before, 2, src])

    def combine(src):
        @pl.when(group == 1)
        def _():
            sum_ref[src] = jnp.zeros(sum_ref.shape[1:], F32)

        sum_ref[src] += added(src)

    def store(src):
        return pltpu.make_async_copy(sum_ref.at[src], out_ref.at[src], out_sem.at[src])

    def finish(src):
        sum_ref[src] += added(src)
        store(src).start()

    def saves(step):
        slot = step % 2
        return [pltpu.make_async_copy(kept.at[slot], to.at[step], save_sem.at[slot, n]) for n, (kept, to) in enumerate(((x_ref, xs_ref),))]

    @pl.when(group >= 2)
    def _():
        wait_all(saves(group - 2))

    schedule(groups, sources, begin, lambda src: load(src).wait(), dispatch, expert, combine, finish)

    @pl.when(group < groups)
    def _():
        start_all(saves(group))

    @pl.when(group == groups)
    def _():
        wait_all(saves(group - 1))
        for src in range(sources):
            store(src).wait()


def bwd_kernel(layer, capacity, groups, held, pieces, keeps, base_ref, meta_ref, w1_ref, w3_ref, w2_ref, *refs):
    given_ref, piece_refs, other_refs, refs = refs[0], refs[1 : 1 + pieces], refs[1 + pieces : 1 + pieces + held], refs[1 + pieces + held :]
    out_ref, d1_ref, d3_ref, d2_ref, sum_ref, grad_ref, pick_ref, x_ref, g_ref, r_ref, d_ref, sem, grad_sem, out_sem, d_sem, from_ref = refs[:16]
    d_refs = (d1_ref, d3_ref, d2_ref)
    group = pl.program_id(0)
    sources = sum_ref.shape[0]
    width = w1_ref.shape[1]
    now = group % 2
    before = 1 - now
    x_slot = now if keeps else 0

    def load(src):
        return pltpu.make_async_copy(given_ref.at[src], from_ref.at[src, pl.ds(0, width)], sem.at[src])

    def loads_saved(step):
        return [pltpu.make_async_copy(given_ref.at[step], x_ref.at[step % 2], sem.at[step % 2])]

    def load_grad(src):
        piece = piece_refs[0].at[src] if pieces == 1 else piece_refs[src]
        return pltpu.make_async_copy(piece, grad_ref.at[src], grad_sem.at[src])

    def begin():
        if keeps:
            start_all(loads_saved(0))
        for src in range(sources):
            if not keeps:
                load(src).start()
            load_grad(src).start()
        if keeps:
            wait_all(loads_saved(0))

    def wait(src):
        if not keeps:
            load(src).wait()
        pltpu.make_async_copy(grad_ref.at[src], grad_ref.at[src], grad_sem.at[src]).wait()

    def dispatch(src):
        if keeps:
            route(meta_ref, layer, src, base_ref[0] + group * GROUP, capacity, pick_ref, now)
            gate = gate_column(x_ref[now, src].astype(F32), capacity)
        else:
            route(meta_ref, layer, src, base_ref[0] + group * GROUP, capacity, pick_ref, now, from_ref)
            found = dot_nt(pick_ref[now, src], from_ref[src])
            gate = gate_column(found, capacity)
            x_ref[0, src] = found.astype(BF16)
        g_ref[src] = (gate * dot_nt(pick_ref[now, src], grad_ref[src])).astype(BF16)

    def next_saved():
        @pl.when((group > 0) & (group < groups))
        def _():
            wait_all(loads_saved(group))

        @pl.when(group < groups - 1)
        def _():
            start_all(loads_saved(group + 1))

    def expert(k):
        here = pl.ds(pl.multiple_of(k * capacity, capacity), capacity)
        x = x_ref[x_slot, :, here, :width].reshape(sources * capacity, width)
        g = g_ref[:, here, :].reshape(sources * capacity, width)
        ff = w1_ref.shape[2]
        both = jnp.concatenate([w1_ref[k], w3_ref[k]], axis=1)
        a = dot_nn(x, both)
        a_three = a[:, ff:]
        act, slope = silu_parts(a[:, :ff])
        hidden = (act * a_three).astype(BF16)
        grad_hidden = dot_nn(g, w2_ref[k])
        grad_one = (grad_hidden * a_three * slope).astype(BF16)
        grad_three = (grad_hidden * act).astype(BF16)
        grads = jnp.concatenate([grad_one, grad_three], axis=1)
        r_ref[:, here, :] = dot_nt(grads, both).astype(BF16).reshape(sources, capacity, width)
        d13 = dot_tn(x, grads).astype(BF16)
        d2 = dot_tn(g, hidden).astype(BF16)
        for i, value in enumerate((d13[:, :ff], d13[:, ff:], d2)):
            d_ref[now, i, k] = value

    def added(src):
        return dot_tn(r_ref[src], pick_ref[before, src])

    def combine(src):
        @pl.when(group == 1)
        def _():
            sum_ref[src] = jnp.zeros(sum_ref.shape[1:], F32)

        sum_ref[src] += added(src)

    def store(src):
        return pltpu.make_async_copy(grad_ref.at[src], out_ref.at[src], out_sem.at[src])

    def finish(src):
        grad_ref[src] = (sum_ref[src] + added(src)).astype(BF16)
        store(src).start()

    def experts_at(start, step):
        return pl.ds(pl.multiple_of((start + step) * GROUP, GROUP), GROUP)

    def d_stores(step):
        slot = step % 2
        return [pltpu.make_async_copy(d_ref.at[slot, i], d_refs[i].at[layer, experts_at(base_ref[1], step)], d_sem.at[slot, i]) for i in range(3)]

    def other_load(step):
        return pltpu.make_async_copy(other_refs[0].at[:, experts_at(0, step)], refs[16].at[step % 2], refs[17].at[step % 2, 3])

    def other_stores(step):
        slot = step % 2
        return [pltpu.make_async_copy(refs[16].at[slot, i], d_refs[i].at[1 - layer, experts_at(base_ref[2], step)], refs[17].at[slot, i]) for i in range(3)]

    @pl.when(group >= 2)
    def _():
        wait_all(d_stores(group - 2))
        if held:
            wait_all(other_stores(group - 2))

    if held:
        @pl.when(group >= 1)
        def _():
            other_load(group - 1).wait()
            start_all(other_stores(group - 1))

        @pl.when(group < groups)
        def _():
            other_load(group).start()

    if keeps:
        next_saved()

    schedule(groups, sources, begin, wait, dispatch, expert, combine, finish)

    @pl.when(group < groups)
    def _():
        start_all(d_stores(group))

    @pl.when(group == groups)
    def _():
        wait_all(d_stores(group - 1))
        if held:
            wait_all(other_stores(group - 1))
        for src in range(sources):
            store(src).wait()


def weight_specs(layer, groups, width, ff):
    spec = pl.BlockSpec((None, GROUP, width, ff), lambda g, base: (layer, base[1] + jnp.minimum(g, groups - 1), 0, 0))
    return [spec, spec, spec]


def whole():
    return pl.BlockSpec(memory_space=pltpu.VMEM)


def anywhere():
    return pl.BlockSpec(memory_space=pl.ANY)


def expert_forward(layer, capacity, groups, base, tok, meta, w1, w3, w2):
    sources, width, tokens = tok.shape
    ff = w1.shape[3]
    rows = GROUP * capacity
    return pl.pallas_call(
        functools.partial(fwd_kernel, layer, capacity, groups),
        out_shape=(
            jax.ShapeDtypeStruct((sources, width, tokens), F32),
            jax.ShapeDtypeStruct((groups, sources, rows, width + 4 * GROUP), BF16),
        ),
        grid_spec=pltpu.PrefetchScalarGridSpec(
            num_scalar_prefetch=1,
            grid=(groups + 1,),
            in_specs=[whole()] + weight_specs(layer, groups, width, ff) + [anywhere()],
            out_specs=(anywhere(),) * 2,
            scratch_shapes=[
                pltpu.VMEM((sources, width, tokens), F32),
                pltpu.VMEM((sources, width + 4 * GROUP, tokens), BF16),
                pltpu.VMEM((2, sources, rows, tokens), BF16),
                pltpu.VMEM((2, 3, sources, rows, tokens), BF16),
                pltpu.VMEM((2, sources, rows, width + 4 * GROUP), BF16),
                pltpu.VMEM((sources, rows, width), BF16),
                pltpu.SemaphoreType.DMA((sources,)),
                pltpu.SemaphoreType.DMA((sources,)),
                pltpu.SemaphoreType.DMA((2, 1)),
            ],
        ),
        compiler_params=pltpu.CompilerParams(vmem_limit_bytes=VMEM_LIMIT),
        cost_estimate=COST,
    )(base, meta, w1, w3, w2, tok)


def expert_backward(layer, capacity, groups, base, given, keeps, grads, meta, w1, w3, w2, held):
    sources, tokens = meta.shape[0], meta.shape[2]
    width = w1.shape[2]
    ff = w1.shape[3]
    rows = GROUP * capacity
    pieces = len(grads)
    grad_shape = jax.ShapeDtypeStruct(w1.shape, BF16)
    block = pltpu.VMEM((2, 3, GROUP, width, ff), BF16)
    more = [block, pltpu.SemaphoreType.DMA((2, 4))] if held else []
    return pl.pallas_call(
        functools.partial(bwd_kernel, layer, capacity, groups, len(held), pieces, keeps),
        out_shape=(jax.ShapeDtypeStruct((sources, width, tokens), BF16), grad_shape, grad_shape, grad_shape),
        grid_spec=pltpu.PrefetchScalarGridSpec(
            num_scalar_prefetch=1,
            grid=(groups + 1,),
            in_specs=[whole()] + weight_specs(layer, groups, width, ff) + [anywhere()] * (1 + pieces + len(held)),
            out_specs=(anywhere(),) * 4,
            scratch_shapes=[
                pltpu.VMEM((sources, width, tokens), F32),
                pltpu.VMEM((sources, width, tokens), BF16),
                pltpu.VMEM((2, sources, rows, tokens), BF16),
                pltpu.VMEM((2 if keeps else 1, sources, rows, width + 4 * GROUP), BF16),
                pltpu.VMEM((sources, rows, width), BF16),
                pltpu.VMEM((sources, rows, width), BF16),
                block,
                pltpu.SemaphoreType.DMA((sources,)),
                pltpu.SemaphoreType.DMA((sources,)),
                pltpu.SemaphoreType.DMA((sources,)),
                pltpu.SemaphoreType.DMA((2, 4)),
                pltpu.VMEM((8, 128), BF16) if keeps else pltpu.VMEM((sources, width + 4 * GROUP, tokens), BF16),
            ]
            + more,
        ),
        input_output_aliases={7 + pieces + i: 1 + i for i in range(len(held) - 1)},
        compiler_params=pltpu.CompilerParams(vmem_limit_bytes=VMEM_LIMIT),
        cost_estimate=COST,
    )(base, meta, w1, w3, w2, given, *grads, *held)


def place_kernel(base_ref, recv_ref, *refs):
    for i in range(3):
        refs[3 + i][...] = recv_ref[i]


def place(layer, groups, base, recv, held):
    width, ff = recv.shape[2:]
    few = 8
    spec = pl.BlockSpec((None, few, width, ff), lambda g, base: (layer, base[2] * (GROUP // few) + g, 0, 0))
    shape = jax.ShapeDtypeStruct(held[0].shape, BF16)
    return pl.pallas_call(
        place_kernel,
        out_shape=(shape, shape, shape),
        grid_spec=pltpu.PrefetchScalarGridSpec(
            num_scalar_prefetch=1,
            grid=(groups * GROUP // few,),
            in_specs=[pl.BlockSpec((3, few, width, ff), lambda g, base: (0, g, 0, 0))] + [anywhere()] * 3,
            out_specs=(spec, spec, spec),
        ),
        input_output_aliases={2: 0, 3: 1, 4: 2},
        compiler_params=pltpu.CompilerParams(vmem_limit_bytes=VMEM_LIMIT),
        cost_estimate=COST,
    )(base, recv, *held)


def neighbours():
    ep = lax.axis_index("ep")
    dp = lax.axis_index("dp")
    return ({"ep": ep + 1 - 2 * (ep % 2), "dp": dp}, {"ep": (ep + 2) % 4, "dp": dp}, {"ep": ep, "dp": 1 - dp})


def greet(devices):
    barrier = pltpu.get_barrier_semaphore()
    for device in devices:
        pl.semaphore_signal(barrier, inc=1, device_id=device, device_id_type=pl.DeviceIdType.MESH)
    pl.semaphore_wait(barrier, len(devices))


def send_block(source, target, send, recv, device):
    made = pltpu.make_async_remote_copy(src_ref=source, dst_ref=target, send_sem=send, recv_sem=recv, device_id=device, device_id_type=pl.DeviceIdType.MESH)
    made.start()
    return made


def gather_phase(devices, own_refs, out_refs, land_refs, sems, shadows):
    by_x, by_y, partner = devices
    send_sem, recv_sem, store_sem = sems
    count = len(own_refs)
    stores = []

    made = [[] for _ in own_refs]

    def copy(which, source, target, half, device):
        rows = own_refs[which].shape[0]
        span = pl.ds(0, rows) if half is None else pl.ds(half * (rows // 2), rows // 2)
        block = land_refs[which].at[source, span] if source else own_refs[which].at[span]
        n = len(made[which])
        made[which].append(send_block(block, land_refs[which].at[target, span], send_sem.at[which, n], recv_sem.at[which, n], device))
        return made[which][n]

    def store(which, slot):
        block = land_refs[which].at[slot] if slot else own_refs[which]
        started = pltpu.make_async_copy(block, out_refs[which].at[slot], store_sem.at[which, slot])
        started.start()
        stores.append(started)

    near, far, pair = [], [], []
    for which in range(count):
        near.append([copy(which, OWN, X, LOW, by_x), copy(which, OWN, Y, HIGH, by_y), copy(which, OWN, X, HIGH, by_x), copy(which, OWN, Y, LOW, by_y)])
        pair.append(copy(which, OWN, 4, None, partner))
        store(which, OWN)
    shadows[0]()
    for which in range(count):
        x_low, y_high, x_high, y_low = near[which]
        x_low.wait_recv()
        relay_low = copy(which, X, FAR, LOW, by_y)
        y_high.wait_recv()
        relay_high = copy(which, Y, FAR, HIGH, by_x)
        if not far:
            shadows[1]()
        x_high.wait_recv()
        pair_x = copy(which, X, 4 + X, None, partner)
        store(which, X)
        y_low.wait_recv()
        pair_y = copy(which, Y, 4 + Y, None, partner)
        store(which, Y)
        pair[which].wait_recv()
        store(which, 4)
        far.append((relay_low, relay_high, pair_x, pair_y))
    for which in range(count):
        relay_low, relay_high, pair_x, pair_y = far[which]
        relay_low.wait_recv()
        pair_low = copy(which, FAR, 4 + FAR, LOW, partner)
        if which == 0:
            shadows[2]()
        relay_high.wait_recv()
        pair_high = copy(which, FAR, 4 + FAR, HIGH, partner)
        store(which, FAR)
        pair_x.wait_recv()
        store(which, 4 + X)
        pair_y.wait_recv()
        store(which, 4 + Y)
        pair_low.wait_recv()
        pair_high.wait_recv()
        store(which, 4 + FAR)
        for step in made[which]:
            step.wait_send()
    wait_all(stores)


def gather_scratch(*arrays):
    count = len(arrays)
    return [pltpu.VMEM((8,) + x.shape, x.dtype) for x in arrays] + [pltpu.SemaphoreType.DMA((count, n)) for n in (11, 11, 8)]


def reduce_phase(devices, part_ref, out_ref, scratch, extras, shadow):
    mine_ref, pair_ref, stage_ref, relay_ref, last_ref, send_sem, recv_sem, load_sem = scratch
    by_x, by_y, partner = devices
    rows = part_ref.shape[1]
    half = rows // 2
    low, high, full = pl.ds(0, half), pl.ds(half, half), pl.ds(0, rows)
    wire = part_ref.dtype

    made = []

    def copy(source, target, device):
        n = len(made)
        made.append(send_block(source, target, send_sem.at[n], recv_sem.at[n], device))
        return made[n]

    def chip_sum(i, span):
        return mine_ref[i, span, :].astype(F32) + pair_ref[i, span, :].astype(F32)

    loads, pair = {}, {}
    for i in (FAR, X, Y, OWN):
        loads[i] = pltpu.make_async_copy(part_ref.at[i], mine_ref.at[i], load_sem.at[i])
        loads[i].start()
        pair[i] = copy(part_ref.at[4 + i], pair_ref.at[i], partner)

    def ready(i):
        loads[i].wait()
        pair[i].wait_recv()

    ready(FAR)
    stage_ref[OWN, low, :] = chip_sum(FAR, low).astype(wire)
    relay_x = copy(stage_ref.at[OWN, low], relay_ref.at[LOW], by_x)
    stage_ref[OWN, high, :] = chip_sum(FAR, high).astype(wire)
    relay_y = copy(stage_ref.at[OWN, high], relay_ref.at[HIGH], by_y)
    ready(X)
    stage_ref[X, low, :] = chip_sum(X, low).astype(wire)
    arrive = [copy(stage_ref.at[X, low], last_ref.at[LOW, low], by_x)]
    ready(Y)
    stage_ref[Y, high, :] = chip_sum(Y, high).astype(wire)
    arrive.append(copy(stage_ref.at[Y, high], last_ref.at[HIGH, high], by_y))
    others = [copy(source, target, partner) for source, target in extras]
    relay_y.wait_recv()
    stage_ref[X, high, :] = (chip_sum(X, high) + relay_ref[HIGH].astype(F32)).astype(wire)
    arrive.append(copy(stage_ref.at[X, high], last_ref.at[LOW, high], by_x))
    relay_x.wait_recv()
    stage_ref[Y, low, :] = (chip_sum(Y, low) + relay_ref[LOW].astype(F32)).astype(wire)
    arrive.append(copy(stage_ref.at[Y, low], last_ref.at[HIGH, low], by_y))
    ready(OWN)
    out_ref[...] = chip_sum(OWN, full)
    shadow()
    for step in arrive:
        step.wait_recv()
    out_ref[...] += last_ref[LOW].astype(F32) + last_ref[HIGH].astype(F32)

    def drain():
        for step in others:
            step.wait_recv()
        for step in made:
            step.wait_send()

    return drain


def reduce_scratch(part):
    rows, tokens = part.shape[1:]
    return [
        pltpu.VMEM((4, rows, tokens), part.dtype),
        pltpu.VMEM((4, rows, tokens), part.dtype),
        pltpu.VMEM((3, rows, tokens), part.dtype),
        pltpu.VMEM((2, rows // 2, tokens), part.dtype),
        pltpu.VMEM((2, rows, tokens), part.dtype),
        pltpu.SemaphoreType.DMA((13,)),
        pltpu.SemaphoreType.DMA((13,)),
        pltpu.SemaphoreType.DMA((4,)),
    ]


def nothing():
    pass


def mix(x_ref, w_dense):
    x = x_ref[...]
    return (x.astype(F32) + dot_tn(w_dense, x)).astype(BF16)


def shared_forward(mixed, ws_gate, ws_up):
    s_one = dot_tn(ws_gate, mixed)
    s_three = dot_tn(ws_up, mixed)
    return s_one, s_three, (jax.nn.silu(s_one) * s_three).astype(BF16)


def shared_backward(grad_y, mixed, ws_gate, ws_up, ws_down, pack_ref, start):
    s_one, s_three, shared_hidden = shared_forward(mixed, ws_gate, ws_up)
    act_one, slope = silu_parts(s_one)
    grad_shared = dot_tn(ws_down, grad_y)
    grad_s_one = (grad_shared * s_three * slope).astype(BF16)
    grad_s_three = (grad_shared * act_one).astype(BF16)
    ff = ws_gate.shape[1]
    for i, value in enumerate((dot_nt(mixed, grad_s_one), dot_nt(mixed, grad_s_three), dot_nt(grad_y, shared_hidden))):
        pack_ref[:, start + i * ff : start + (i + 1) * ff] = value.astype(BF16)
    return dot_nn(ws_gate, grad_s_one) + dot_nn(ws_up, grad_s_three)


def comm_call(kernel, cid, out_shape, in_specs, out_specs, scratch, operands):
    return pl.pallas_call(
        kernel,
        out_shape=out_shape,
        in_specs=in_specs,
        out_specs=out_specs,
        scratch_shapes=scratch,
        compiler_params=pltpu.CompilerParams(collective_id=cid, has_side_effects=True, vmem_limit_bytes=VMEM_LIMIT),
        cost_estimate=COST,
    )(*operands)


def first_kernel(x_ref, w_dense_ref, meta_ref, tok_ref, metas_ref, own_ref, land_ref, land_meta_ref, *sems):
    devices = neighbours()
    own_ref[...] = mix(x_ref, w_dense_ref[0])
    greet(devices)
    gather_phase(devices, [own_ref, meta_ref], [tok_ref, metas_ref], [land_ref, land_meta_ref], sems, (nothing,) * 3)


def first_exchange(x, w_dense, meta):
    outs = (jax.ShapeDtypeStruct((8,) + x.shape, BF16), jax.ShapeDtypeStruct((8,) + meta.shape, F32), jax.ShapeDtypeStruct(x.shape, BF16))
    return comm_call(first_kernel, 0, outs, [whole()] * 3, (anywhere(), anywhere(), whole()), gather_scratch(x, meta), (x, w_dense, meta))


def forward_kernel(part_ref, u1_ref, ws_gate_ref, ws_up_ref, ws_down_ref, w_dense_ref, tok_ref, x2_ref, u2_ref, sum_ref, shared_ref, *scratch):
    devices = neighbours()
    greet(devices)

    def shadow():
        hidden = shared_forward(u1_ref[...], ws_gate_ref[0], ws_up_ref[0])[2]
        shared_ref[...] = dot_nn(ws_down_ref[0], hidden)

    drain = reduce_phase(devices, part_ref, sum_ref, scratch[:8], [], shadow)
    x2_ref[...] = (u1_ref[...].astype(F32) + sum_ref[...] + shared_ref[...]).astype(BF16)
    u2_ref[...] = mix(x2_ref, w_dense_ref[1])
    gather_phase(devices, [u2_ref], [tok_ref], [scratch[8]], scratch[9:], (nothing,) * 3)
    drain()


def forward_exchange(part, u1, ws_gate, ws_up, ws_down_t, w_dense):
    outs = (jax.ShapeDtypeStruct((8,) + u1.shape, BF16), jax.ShapeDtypeStruct(u1.shape, BF16), jax.ShapeDtypeStruct(u1.shape, BF16))
    scratch = [pltpu.VMEM(u1.shape, F32), pltpu.VMEM(u1.shape, F32)] + reduce_scratch(part) + gather_scratch(u1)
    specs = [anywhere()] + [whole()] * 5
    return comm_call(forward_kernel, 1, outs, specs, (anywhere(), whole(), whole()), scratch, (part, u1, ws_gate, ws_up, ws_down_t, w_dense))


def expert_half(refs, layer, target_ref):
    own = target_ref.shape[1]
    start = lax.axis_index("dp") * own
    return [(ref.at[layer, pl.ds(start, own)], target_ref.at[i]) for i, ref in enumerate(refs)]


def pair_half(partner, pack_ref, land_ref, sems):
    half = land_ref.shape[0]
    dp = lax.axis_index("dp")
    sent = []

    def start():
        theirs = pack_ref.at[pl.ds(pl.multiple_of((1 - dp) * half, 16), half)]
        sent.append(send_block(theirs, land_ref, sems.at[0], sems.at[1], partner))

    def finish():
        sent[0].wait()
        mine = pack_ref[pl.ds(pl.multiple_of(dp * half, 16), half), :]
        return (mine.astype(F32) + land_ref[...].astype(F32)).astype(BF16)

    return start, finish


def pair_scratch(shape):
    return [pltpu.VMEM(shape, BF16), pltpu.VMEM((shape[0] // 2, shape[1]), BF16), pltpu.SemaphoreType.DMA((2,))]


def backward_kernel(part_ref, d1_ref, d3_ref, d2_ref, grad_y_ref, x2_ref, u2_ref, u1_ref, w_dense_ref, ws_gate_ref, ws_up_ref, ws_down_ref, *refs):
    grad_all_ref, recv_ref, grad_x_ref, back_ref, chip_ref, sum_ref, mixed_ref, pack_ref, land_ref, pair_sem = refs[:10]
    scratch = refs[10:]
    devices = neighbours()
    greet(devices)
    ff = ws_gate_ref.shape[2]
    width = x2_ref.shape[0]
    start_pair, finish_pair = pair_half(devices[2], pack_ref, land_ref, pair_sem)

    def shadow():
        back_ref[...] = shared_backward(grad_y_ref[...], u2_ref[...], ws_gate_ref[1], ws_up_ref[1], ws_down_ref[1], pack_ref, 0)

    drain = reduce_phase(devices, part_ref, sum_ref, scratch[:8], expert_half((d1_ref, d3_ref, d2_ref), 1, recv_ref), shadow)
    mixed_ref[...] = (grad_y_ref[...].astype(F32) + sum_ref[...] + back_ref[...]).astype(BF16)
    grad_x_ref[...] = (mixed_ref[...].astype(F32) + dot_nn(w_dense_ref[1], mixed_ref[...])).astype(BF16)

    def dense_part():
        pack_ref[:, 6 * ff : 6 * ff + width] = dot_nt(x2_ref[...], mixed_ref[...]).astype(BF16)
        pack_ref[:, 6 * ff + width :] = jnp.zeros((width, pack_ref.shape[1] - 6 * ff - width), BF16)

    def shared_part():
        back_ref[...] = shared_backward(grad_x_ref[...], u1_ref[...], ws_gate_ref[0], ws_up_ref[0], ws_down_ref[0], pack_ref, 3 * ff)

    gather_phase(devices, [grad_x_ref], [grad_all_ref], [scratch[8]], scratch[9:], (dense_part, shared_part, start_pair))
    chip_ref[...] = finish_pair()
    drain()


def backward_exchange(part, held, grad_y, x2, u2, u1, w_dense, ws_gate, ws_up, ws_down_t):
    ff = ws_gate.shape[2]
    width = x2.shape[0]
    packed = 6 * ff + width + -(6 * ff + width) % 128
    own = held[0].shape[1] // 2
    outs = (
        jax.ShapeDtypeStruct((8,) + x2.shape, BF16),
        jax.ShapeDtypeStruct((3, own) + held[0].shape[2:], BF16),
        jax.ShapeDtypeStruct(x2.shape, BF16),
        jax.ShapeDtypeStruct(x2.shape, F32),
        jax.ShapeDtypeStruct((width // 2, packed), BF16),
    )
    scratch = [pltpu.VMEM(x2.shape, F32), pltpu.VMEM(x2.shape, BF16)] + pair_scratch((width, packed)) + reduce_scratch(part) + gather_scratch(x2)
    operands = (part, *held, grad_y, x2, u2, u1, w_dense, ws_gate, ws_up, ws_down_t)
    specs = [anywhere()] * 4 + [whole()] * 8
    return comm_call(backward_kernel, 2, outs, specs, (anywhere(), anywhere()) + (whole(),) * 3, scratch, operands)


def last_kernel(part_ref, d1_ref, d3_ref, d2_ref, grad_y_ref, back_ref, x_ref, w_dense_ref, grad_x_ref, recv_ref, chip_ref, sum_ref, mixed_ref, pack_ref, land_ref, pair_sem, *scratch):
    devices = neighbours()
    greet(devices)
    start_pair, finish_pair = pair_half(devices[2], pack_ref, land_ref, pair_sem)
    drain = reduce_phase(devices, part_ref, sum_ref, scratch, expert_half((d1_ref, d3_ref, d2_ref), 0, recv_ref), nothing)
    mixed_ref[...] = (grad_y_ref[...].astype(F32) + sum_ref[...] + back_ref[...]).astype(BF16)
    pack_ref[...] = dot_nt(x_ref[...], mixed_ref[...]).astype(BF16)
    grad_x_ref[...] = (mixed_ref[...].astype(F32) + dot_nn(w_dense_ref[0], mixed_ref[...])).astype(BF16)
    start_pair()
    drain()
    chip_ref[...] = finish_pair()


def last_exchange(part, held, grad_y, back, x, w_dense):
    own = held[0].shape[1] // 2
    width = x.shape[0]
    outs = (jax.ShapeDtypeStruct(x.shape, BF16), jax.ShapeDtypeStruct((3, own) + held[0].shape[2:], BF16), jax.ShapeDtypeStruct((width // 2, width), BF16))
    scratch = [pltpu.VMEM(x.shape, F32), pltpu.VMEM(x.shape, BF16)] + pair_scratch((width, width)) + reduce_scratch(part)
    specs = [anywhere()] * 4 + [whole()] * 4
    return comm_call(last_kernel, 3, outs, specs, (whole(), anywhere(), whole()), scratch, (part, *held, grad_y, back, x, w_dense))


def send_over(x, flip):
    return lax.ppermute(x, "ep", [(i, i ^ flip) for i in range(4)])


def swap_cores(x):
    return lax.ppermute(x, "dp", [(0, 1), (1, 0)])


def sum_start(chip):
    sent = [chip]
    for flip in (1, 2, 3):
        sent.append(send_over(chip, flip))
    return sent


def sum_finish(parts):
    total = sum(part.astype(F32) for part in parts).astype(BF16)
    other = swap_cores(total)
    first = lax.axis_index("dp") == 0
    return jnp.concatenate([jnp.where(first, total, other), jnp.where(first, other, total)], axis=0)


def solution(mesh):
    ep_size = mesh.shape["ep"]
    dp_size = mesh.shape["dp"]
    tok_spec = P(ALL_AXES)
    route_spec = P(None, ALL_AXES)
    exp_spec = P(None, "ep")
    repl_spec = P()

    def body(act_in, grad_out, slot_ids, gate_vals, w_dense, w_gate, w_up, w_down, ws_gate, ws_up, ws_down):
        layers, local_exp = w_gate.shape[:2]
        tokens = act_in.shape[0]
        top = slot_ids.shape[2]
        own = local_exp // dp_size
        groups = own // GROUP
        capacity = 2 * tokens * top // (local_exp * ep_size)
        dp = lax.axis_index("dp")
        base = jnp.stack([lax.axis_index("ep") * local_exp + dp * own, dp * groups, (dp_size - 1 - dp) * groups]).astype(jnp.int32)
        w_down_t = jnp.swapaxes(w_down, 2, 3)
        meta = jnp.concatenate([jnp.swapaxes(slot_ids, 1, 2).astype(F32), jnp.swapaxes(gate_vals, 1, 2)], axis=1)
        meta = meta.reshape(layers * 2 * top, tokens)

        x1 = act_in.T
        grad_y2 = grad_out.T
        shared_w = (ws_gate, ws_up, jnp.swapaxes(ws_down, 1, 2))
        tok1, metas, u1 = first_exchange(x1, w_dense, meta)
        tok1, grad_y2 = lax.optimization_barrier((tok1, grad_y2))
        grads2 = [grad_y2, send_over(grad_y2, 1), send_over(grad_y2, 2), send_over(grad_y2, 3)]
        grads2 = grads2 + [swap_cores(x) for x in grads2]
        part, rows1 = expert_forward(0, capacity, groups, base, tok1, metas, w_gate, w_up, w_down_t)
        tok2, x2, u2 = forward_exchange(part, u1, *shared_w, w_dense)
        back2, *held = expert_backward(1, capacity, groups, base, tok2, False, grads2, metas, w_gate, w_up, w_down_t, [])
        grad1_all, recv2, grad_y1, shared1, early = backward_exchange(back2, held, grad_y2, x2, u2, u1, w_dense, *shared_w)
        ff = ws_gate.shape[2]
        width = w_dense.shape[1]
        early = sum_start(early)
        grad1_all, early[0] = lax.optimization_barrier((grad1_all, early[0]))
        back1, *held = expert_backward(0, capacity, groups, base, rows1, True, [grad1_all], metas, w_gate, w_up, w_down_t, [recv2] + held)
        grad_x, recv1, late = last_exchange(back1, held, grad_y1, shared1, x1, w_dense)
        late = sum_start(late)
        g_gate, g_up, g_down = place(0, groups, base, recv1, held)
        g_gate, late = lax.optimization_barrier((g_gate, late))
        g_down = jnp.swapaxes(g_down, 2, 3)
        early = sum_finish(early)
        late = sum_finish(late)
        g_dense = jnp.stack([late, early[:, 6 * ff : 6 * ff + width]])
        shared = [jnp.stack([early[:, (3 + i) * ff : (4 + i) * ff], early[:, i * ff : (i + 1) * ff]]) for i in range(3)]
        return (grad_x.T, g_dense, g_gate, g_up, g_down, shared[0], shared[1], jnp.swapaxes(shared[2], 1, 2))

    return jax.shard_map(body, mesh=mesh, in_specs=(tok_spec, tok_spec, route_spec, route_spec, repl_spec, exp_spec, exp_spec, exp_spec, repl_spec, repl_spec, repl_spec), out_specs=(tok_spec, repl_spec, exp_spec, exp_spec, exp_spec, repl_spec, repl_spec, repl_spec), check_vma=False)
```

```python
import functools
import jax
import jax.numpy as jnp
from jax import lax
from jax.experimental import pallas as pl
from jax.experimental.pallas import tpu as pltpu
from jax.sharding import PartitionSpec as P

ALL_AXES = ("ep", "dp")
GROUP = 8
UNROLL = 8
VMEM_LIMIT = 62 << 20
LOW, HIGH = range(2)
OWN, X, Y, FAR = range(4)
COST = pl.CostEstimate(flops=20_000_000_000, bytes_accessed=20_000_000, transcendentals=0)
F32 = jnp.float32
BF16 = jnp.bfloat16


def dot(left, right, left_dim, right_dim):
    return lax.dot_general(left, right, (((left_dim,), (right_dim,)), ((), ())), preferred_element_type=F32)


def dot_nn(left, right):
    return dot(left, right, 1, 0)


def dot_nt(left, right):
    return dot(left, right, 1, 1)


def dot_tn(left, right):
    return dot(left, right, 0, 0)


def silu_parts(pre_act):
    sigma = jax.nn.sigmoid(pre_act)
    return pre_act * sigma, sigma * (1.0 + pre_act * (1.0 - sigma))


def route(meta_ref, layer, src, first_expert, capacity, pick_ref, slot, tok_ref=None, weigh_ref=None):
    top = meta_ref.shape[1] // 4
    tokens = meta_ref.shape[2]
    start = 2 * layer * top
    slots = meta_ref[src, start : start + top, :].astype(jnp.int32)
    gates = meta_ref[src, start + top : start + 2 * top, :]
    expert = slots // capacity - first_expert
    row = (slots % capacity).astype(F32)
    which = lax.broadcasted_iota(jnp.int32, (GROUP, tokens), 0)
    row_of = jnp.full((GROUP, tokens), -1.0, F32)
    gate_of = jnp.zeros((GROUP, tokens), F32)
    for j in range(top):
        hit = expert[j : j + 1, :] == which
        row_of = jnp.where(hit, row[j : j + 1, :], row_of)
        gate_of = jnp.where(hit, gates[j : j + 1, :], gate_of)
    if tok_ref is not None:
        width = tok_ref.shape[1] - 4 * GROUP
        high = gate_of.astype(BF16)
        rest = gate_of - high.astype(F32)
        middle = rest.astype(BF16)
        low = (rest - middle.astype(F32)).astype(BF16)
        tok_ref[src, width : width + 4 * GROUP, :] = jnp.concatenate([high, middle, low, jnp.zeros_like(low)], axis=0)
    step = 16
    rows = lax.broadcasted_iota(jnp.int32, (step, tokens), 0).astype(F32).astype(BF16)
    for k in range(GROUP):
        wanted = jnp.broadcast_to(row_of[k : k + 1, :], (step, tokens)).astype(BF16)
        if weigh_ref is not None:
            parts = [jnp.broadcast_to(part[k : k + 1, :].astype(F32), (step, tokens)).astype(BF16) for part in (high, middle, low)]
        for h in range(capacity // step):
            hit = wanted == rows + jnp.asarray(h * step, BF16)
            start = k * capacity + h * step
            pick_ref[slot, src, start : start + step, :] = jnp.where(hit, jnp.asarray(1, BF16), jnp.asarray(0, BF16))
            if weigh_ref is not None:
                for i, part in enumerate(parts):
                    weigh_ref[slot, i, src, start : start + step, :] = jnp.where(hit, part, jnp.asarray(0, BF16))


def gate_column(found, capacity):
    width = found.shape[1] - 4 * GROUP
    gates = []
    for k in range(GROUP):
        rows = found[k * capacity : (k + 1) * capacity, :]
        gates.append(rows[:, width + k : width + k + 1] + rows[:, width + GROUP + k : width + GROUP + k + 1] + rows[:, width + 2 * GROUP + k : width + 2 * GROUP + k + 1])
    return jnp.concatenate(gates, axis=0)


def schedule(groups, sources, begin, wait, dispatch, expert, combine, finish):
    group = pl.program_id(0)

    @pl.when(group == 0)
    def _():
        begin()

        def first(src, carry):
            wait(src)
            dispatch(src)
            return carry

        lax.fori_loop(0, sources, first, 0)

    @pl.when((group > 0) & (group < groups))
    def _():
        def middle(src, carry):
            combine(src)
            dispatch(src)
            return carry

        lax.fori_loop(0, sources, middle, 0)

    @pl.when(group < groups)
    def _():
        def one(k, carry):
            expert(k)
            return carry

        lax.fori_loop(0, GROUP, one, 0, unroll=UNROLL)

    @pl.when(group == groups)
    def _():
        def last(src, carry):
            finish(src)
            return carry

        lax.fori_loop(0, sources, last, 0)


def start_all(copies):
    for copy in copies:
        copy.start()


def wait_all(copies):
    for copy in copies:
        copy.wait()


def fwd_kernel(layer, capacity, groups, base_ref, meta_ref, w1_ref, w3_ref, w2_ref, tokens_ref, out_ref, xs_ref, sum_ref, tok_ref, pick_ref, weigh_ref, x_ref, o_ref, sem, out_sem, save_sem):
    group = pl.program_id(0)
    sources = tok_ref.shape[0]
    width = w1_ref.shape[1]
    now = group % 2
    before = 1 - now

    def load(src):
        return pltpu.make_async_copy(tokens_ref.at[src], tok_ref.at[src, pl.ds(0, width)], sem.at[src])

    def begin():
        for src in range(sources):
            load(src).start()

    def wait(src):
        load(src).wait()
        sum_ref[src] = jnp.zeros(sum_ref.shape[1:], F32)

    def dispatch(src):
        route(meta_ref, layer, src, base_ref[0] + group * GROUP, capacity, pick_ref, now, tok_ref, weigh_ref)
        found = dot_nt(pick_ref[now, src], tok_ref[src])
        x_ref[now, src] = found.astype(BF16)

    def expert(k):
        here = pl.ds(pl.multiple_of(k * capacity, capacity), capacity)
        x = x_ref[now, :, here, :width].reshape(sources * capacity, width)
        ff = w1_ref.shape[2]
        a = dot_nn(x, jnp.concatenate([w1_ref[k], w3_ref[k]], axis=1))
        hidden = (jax.nn.silu(a[:, :ff]) * a[:, ff:]).astype(BF16)
        o_ref[:, here, :] = dot_nt(hidden, w2_ref[k]).astype(BF16).reshape(sources, capacity, width)

    def added(src):
        rows = o_ref[src]
        return dot_tn(rows, weigh_ref[before, 0, src]) + dot_tn(rows, weigh_ref[before, 1, src]) + dot_tn(rows, weigh_ref[before, 2, src])

    def combine(src):
        sum_ref[src] += added(src)

    def store(src):
        return pltpu.make_async_copy(sum_ref.at[src], out_ref.at[src], out_sem.at[src])

    def finish(src):
        sum_ref[src] += added(src)
        store(src).start()

    def saves(step):
        slot = step % 2
        return [pltpu.make_async_copy(kept.at[slot], to.at[step], save_sem.at[slot, n]) for n, (kept, to) in enumerate(((x_ref, xs_ref),))]

    @pl.when(group >= 2)
    def _():
        wait_all(saves(group - 2))

    schedule(groups, sources, begin, wait, dispatch, expert, combine, finish)

    @pl.when(group < groups)
    def _():
        start_all(saves(group))

    @pl.when(group == groups)
    def _():
        wait_all(saves(group - 1))
        for src in range(sources):
            store(src).wait()


def bwd_kernel(layer, capacity, groups, held, pieces, keeps, base_ref, meta_ref, w1_ref, w3_ref, w2_ref, *refs):
    given_ref, piece_refs, other_refs, refs = refs[0], refs[1 : 1 + pieces], refs[1 + pieces : 1 + pieces + held], refs[1 + pieces + held :]
    out_ref, d1_ref, d3_ref, d2_ref, sum_ref, grad_ref, pick_ref, x_ref, g_ref, r_ref, d_ref, sem, grad_sem, out_sem, d_sem, from_ref = refs[:16]
    d_refs = (d1_ref, d3_ref, d2_ref)
    group = pl.program_id(0)
    sources = sum_ref.shape[0]
    width = w1_ref.shape[1]
    now = group % 2
    before = 1 - now
    x_slot = now if keeps else 0

    def load(src):
        return pltpu.make_async_copy(given_ref.at[src], from_ref.at[src, pl.ds(0, width)], sem.at[src])

    def loads_saved(step):
        return [pltpu.make_async_copy(given_ref.at[step], x_ref.at[step % 2], sem.at[step % 2])]

    def load_grad(src):
        piece = piece_refs[0].at[src] if pieces == 1 else piece_refs[src]
        return pltpu.make_async_copy(piece, grad_ref.at[src], grad_sem.at[src])

    def begin():
        if keeps:
            start_all(loads_saved(0))
        for src in range(sources):
            if not keeps:
                load(src).start()
            load_grad(src).start()
        if keeps:
            wait_all(loads_saved(0))

    def wait(src):
        if not keeps:
            load(src).wait()
        pltpu.make_async_copy(grad_ref.at[src], grad_ref.at[src], grad_sem.at[src]).wait()
        sum_ref[src] = jnp.zeros(sum_ref.shape[1:], F32)

    def dispatch(src):
        if keeps:
            route(meta_ref, layer, src, base_ref[0] + group * GROUP, capacity, pick_ref, now)
            gate = gate_column(x_ref[now, src].astype(F32), capacity)
        else:
            route(meta_ref, layer, src, base_ref[0] + group * GROUP, capacity, pick_ref, now, from_ref)
            found = dot_nt(pick_ref[now, src], from_ref[src])
            gate = gate_column(found, capacity)
            x_ref[0, src] = found.astype(BF16)
        g_ref[src] = (gate * dot_nt(pick_ref[now, src], grad_ref[src])).astype(BF16)

    def next_saved():
        @pl.when((group > 0) & (group < groups))
        def _():
            wait_all(loads_saved(group))

        @pl.when(group < groups - 1)
        def _():
            start_all(loads_saved(group + 1))

    def expert(k):
        here = pl.ds(pl.multiple_of(k * capacity, capacity), capacity)
        x = x_ref[x_slot, :, here, :width].reshape(sources * capacity, width)
        g = g_ref[:, here, :].reshape(sources * capacity, width)
        ff = w1_ref.shape[2]
        both = jnp.concatenate([w1_ref[k], w3_ref[k]], axis=1)
        a = dot_nn(x, both)
        a_three = a[:, ff:]
        act, slope = silu_parts(a[:, :ff])
        hidden = (act * a_three).astype(BF16)
        grad_hidden = dot_nn(g, w2_ref[k])
        grad_one = (grad_hidden * a_three * slope).astype(BF16)
        grad_three = (grad_hidden * act).astype(BF16)
        grads = jnp.concatenate([grad_one, grad_three], axis=1)
        r_ref[:, here, :] = dot_nt(grads, both).astype(BF16).reshape(sources, capacity, width)
        d13 = dot_tn(x, grads).astype(BF16)
        d2 = dot_tn(g, hidden).astype(BF16)
        for i, value in enumerate((d13[:, :ff], d13[:, ff:], d2)):
            d_ref[now, i, k] = value

    def added(src):
        return dot_tn(r_ref[src], pick_ref[before, src])

    def combine(src):
        sum_ref[src] += added(src)

    def store(src):
        return pltpu.make_async_copy(grad_ref.at[src], out_ref.at[src], out_sem.at[src])

    def finish(src):
        grad_ref[src] = (sum_ref[src] + added(src)).astype(BF16)
        store(src).start()

    def experts_at(start, step):
        return pl.ds(pl.multiple_of((start + step) * GROUP, GROUP), GROUP)

    def d_stores(step):
        slot = step % 2
        return [pltpu.make_async_copy(d_ref.at[slot, i], d_refs[i].at[layer, experts_at(base_ref[1], step)], d_sem.at[slot, i]) for i in range(3)]

    def other_load(step):
        return pltpu.make_async_copy(other_refs[0].at[:, experts_at(0, step)], refs[16].at[step % 2], refs[17].at[step % 2, 3])

    def other_stores(step):
        slot = step % 2
        return [pltpu.make_async_copy(refs[16].at[slot, i], d_refs[i].at[1 - layer, experts_at(base_ref[2], step)], refs[17].at[slot, i]) for i in range(3)]

    @pl.when(group >= 2)
    def _():
        wait_all(d_stores(group - 2))
        if held:
            wait_all(other_stores(group - 2))

    if held:
        @pl.when(group >= 1)
        def _():
            other_load(group - 1).wait()
            start_all(other_stores(group - 1))

        @pl.when(group < groups)
        def _():
            other_load(group).start()

    if keeps:
        next_saved()

    schedule(groups, sources, begin, wait, dispatch, expert, combine, finish)

    @pl.when(group < groups)
    def _():
        start_all(d_stores(group))

    @pl.when(group == groups)
    def _():
        wait_all(d_stores(group - 1))
        if held:
            wait_all(other_stores(group - 1))
        for src in range(sources):
            store(src).wait()


def weight_specs(layer, groups, width, ff):
    spec = pl.BlockSpec((None, GROUP, width, ff), lambda g, base: (layer, base[1] + jnp.minimum(g, groups - 1), 0, 0))
    return [spec, spec, spec]


def whole():
    return pl.BlockSpec(memory_space=pltpu.VMEM)


def anywhere():
    return pl.BlockSpec(memory_space=pl.ANY)


def expert_forward(layer, capacity, groups, base, tok, meta, w1, w3, w2):
    sources, width, tokens = tok.shape
    ff = w1.shape[3]
    rows = GROUP * capacity
    return pl.pallas_call(
        functools.partial(fwd_kernel, layer, capacity, groups),
        out_shape=(
            jax.ShapeDtypeStruct((sources, width, tokens), F32),
            jax.ShapeDtypeStruct((groups, sources, rows, width + 4 * GROUP), BF16),
        ),
        grid_spec=pltpu.PrefetchScalarGridSpec(
            num_scalar_prefetch=1,
            grid=(groups + 1,),
            in_specs=[whole()] + weight_specs(layer, groups, width, ff) + [anywhere()],
            out_specs=(anywhere(),) * 2,
            scratch_shapes=[
                pltpu.VMEM((sources, width, tokens), F32),
                pltpu.VMEM((sources, width + 4 * GROUP, tokens), BF16),
                pltpu.VMEM((2, sources, rows, tokens), BF16),
                pltpu.VMEM((2, 3, sources, rows, tokens), BF16),
                pltpu.VMEM((2, sources, rows, width + 4 * GROUP), BF16),
                pltpu.VMEM((sources, rows, width), BF16),
                pltpu.SemaphoreType.DMA((sources,)),
                pltpu.SemaphoreType.DMA((sources,)),
                pltpu.SemaphoreType.DMA((2, 1)),
            ],
        ),
        compiler_params=pltpu.CompilerParams(vmem_limit_bytes=VMEM_LIMIT),
        cost_estimate=COST,
    )(base, meta, w1, w3, w2, tok)


def expert_backward(layer, capacity, groups, base, given, keeps, grads, meta, w1, w3, w2, held):
    sources, tokens = meta.shape[0], meta.shape[2]
    width = w1.shape[2]
    ff = w1.shape[3]
    rows = GROUP * capacity
    pieces = len(grads)
    grad_shape = jax.ShapeDtypeStruct(w1.shape, BF16)
    block = pltpu.VMEM((2, 3, GROUP, width, ff), BF16)
    more = [block, pltpu.SemaphoreType.DMA((2, 4))] if held else []
    return pl.pallas_call(
        functools.partial(bwd_kernel, layer, capacity, groups, len(held), pieces, keeps),
        out_shape=(jax.ShapeDtypeStruct((sources, width, tokens), BF16), grad_shape, grad_shape, grad_shape),
        grid_spec=pltpu.PrefetchScalarGridSpec(
            num_scalar_prefetch=1,
            grid=(groups + 1,),
            in_specs=[whole()] + weight_specs(layer, groups, width, ff) + [anywhere()] * (1 + pieces + len(held)),
            out_specs=(anywhere(),) * 4,
            scratch_shapes=[
                pltpu.VMEM((sources, width, tokens), F32),
                pltpu.VMEM((sources, width, tokens), BF16),
                pltpu.VMEM((2, sources, rows, tokens), BF16),
                pltpu.VMEM((2 if keeps else 1, sources, rows, width + 4 * GROUP), BF16),
                pltpu.VMEM((sources, rows, width), BF16),
                pltpu.VMEM((sources, rows, width), BF16),
                block,
                pltpu.SemaphoreType.DMA((sources,)),
                pltpu.SemaphoreType.DMA((sources,)),
                pltpu.SemaphoreType.DMA((sources,)),
                pltpu.SemaphoreType.DMA((2, 4)),
                pltpu.VMEM((8, 128), BF16) if keeps else pltpu.VMEM((sources, width + 4 * GROUP, tokens), BF16),
            ]
            + more,
        ),
        input_output_aliases={7 + pieces + i: 1 + i for i in range(len(held) - 1)},
        compiler_params=pltpu.CompilerParams(vmem_limit_bytes=VMEM_LIMIT),
        cost_estimate=COST,
    )(base, meta, w1, w3, w2, given, *grads, *held)


def place_kernel(base_ref, recv_ref, *refs):
    for i in range(3):
        refs[3 + i][...] = recv_ref[i]


def place(layer, groups, base, recv, held):
    width, ff = recv.shape[2:]
    few = 8
    spec = pl.BlockSpec((None, few, width, ff), lambda g, base: (layer, base[2] * (GROUP // few) + g, 0, 0))
    shape = jax.ShapeDtypeStruct(held[0].shape, BF16)
    return pl.pallas_call(
        place_kernel,
        out_shape=(shape, shape, shape),
        grid_spec=pltpu.PrefetchScalarGridSpec(
            num_scalar_prefetch=1,
            grid=(groups * GROUP // few,),
            in_specs=[pl.BlockSpec((3, few, width, ff), lambda g, base: (0, g, 0, 0))] + [anywhere()] * 3,
            out_specs=(spec, spec, spec),
        ),
        input_output_aliases={2: 0, 3: 1, 4: 2},
        compiler_params=pltpu.CompilerParams(vmem_limit_bytes=VMEM_LIMIT),
        cost_estimate=COST,
    )(base, recv, *held)


def neighbours():
    ep = lax.axis_index("ep")
    dp = lax.axis_index("dp")
    return ({"ep": ep + 1 - 2 * (ep % 2), "dp": dp}, {"ep": (ep + 2) % 4, "dp": dp}, {"ep": ep, "dp": 1 - dp})


def greet(devices):
    barrier = pltpu.get_barrier_semaphore()
    for device in devices:
        pl.semaphore_signal(barrier, inc=1, device_id=device, device_id_type=pl.DeviceIdType.MESH)
    pl.semaphore_wait(barrier, len(devices))


def send_block(source, target, send, recv, device):
    made = pltpu.make_async_remote_copy(src_ref=source, dst_ref=target, send_sem=send, recv_sem=recv, device_id=device, device_id_type=pl.DeviceIdType.MESH)
    made.start()
    return made


def gather_phase(devices, own_refs, out_refs, land_refs, sems, shadows):
    by_x, by_y, partner = devices
    send_sem, recv_sem, store_sem = sems
    count = len(own_refs)
    stores = []

    made = [[] for _ in own_refs]

    def copy(which, source, target, half, device):
        rows = own_refs[which].shape[0]
        span = pl.ds(0, rows) if half is None else pl.ds(half * (rows // 2), rows // 2)
        block = land_refs[which].at[source, span] if source else own_refs[which].at[span]
        n = len(made[which])
        made[which].append(send_block(block, land_refs[which].at[target, span], send_sem.at[which, n], recv_sem.at[which, n], device))
        return made[which][n]

    def store(which, slot):
        block = land_refs[which].at[slot] if slot else own_refs[which]
        started = pltpu.make_async_copy(block, out_refs[which].at[slot], store_sem.at[which, slot])
        started.start()
        stores.append(started)

    near, far, pair = [], [], []
    for which in range(count):
        near.append([copy(which, OWN, X, LOW, by_x), copy(which, OWN, Y, HIGH, by_y), copy(which, OWN, X, HIGH, by_x), copy(which, OWN, Y, LOW, by_y)])
        pair.append(copy(which, OWN, 4, None, partner))
        store(which, OWN)
    shadows[0]()
    for which in range(count):
        x_low, y_high, x_high, y_low = near[which]
        x_low.wait_recv()
        relay_low = copy(which, X, FAR, LOW, by_y)
        y_high.wait_recv()
        relay_high = copy(which, Y, FAR, HIGH, by_x)
        if not far:
            shadows[1]()
        x_high.wait_recv()
        pair_x = copy(which, X, 4 + X, None, partner)
        store(which, X)
        y_low.wait_recv()
        pair_y = copy(which, Y, 4 + Y, None, partner)
        store(which, Y)
        pair[which].wait_recv()
        store(which, 4)
        far.append((relay_low, relay_high, pair_x, pair_y))
    for which in range(count):
        relay_low, relay_high, pair_x, pair_y = far[which]
        relay_low.wait_recv()
        pair_low = copy(which, FAR, 4 + FAR, LOW, partner)
        if which == 0:
            shadows[2]()
        relay_high.wait_recv()
        pair_high = copy(which, FAR, 4 + FAR, HIGH, partner)
        store(which, FAR)
        pair_x.wait_recv()
        store(which, 4 + X)
        pair_y.wait_recv()
        store(which, 4 + Y)
        pair_low.wait_recv()
        pair_high.wait_recv()
        store(which, 4 + FAR)
        for step in made[which]:
            step.wait_send()
    wait_all(stores)


def gather_scratch(*arrays):
    count = len(arrays)
    return [pltpu.VMEM((8,) + x.shape, x.dtype) for x in arrays] + [pltpu.SemaphoreType.DMA((count, n)) for n in (11, 11, 8)]


def reduce_phase(devices, part_ref, out_ref, scratch, extras, shadow):
    mine_ref, pair_ref, stage_ref, relay_ref, last_ref, send_sem, recv_sem, load_sem = scratch
    by_x, by_y, partner = devices
    rows = part_ref.shape[1]
    half = rows // 2
    low, high, full = pl.ds(0, half), pl.ds(half, half), pl.ds(0, rows)
    wire = part_ref.dtype

    made = []

    def copy(source, target, device):
        n = len(made)
        made.append(send_block(source, target, send_sem.at[n], recv_sem.at[n], device))
        return made[n]

    def chip_sum(i, span):
        return mine_ref[i, span, :].astype(F32) + pair_ref[i, span, :].astype(F32)

    loads, pair = {}, {}
    for i in (FAR, X, Y, OWN):
        loads[i] = pltpu.make_async_copy(part_ref.at[i], mine_ref.at[i], load_sem.at[i])
        loads[i].start()
        pair[i] = copy(part_ref.at[4 + i], pair_ref.at[i], partner)

    def ready(i):
        loads[i].wait()
        pair[i].wait_recv()

    ready(FAR)
    stage_ref[OWN, low, :] = chip_sum(FAR, low).astype(wire)
    relay_x = copy(stage_ref.at[OWN, low], relay_ref.at[LOW], by_x)
    stage_ref[OWN, high, :] = chip_sum(FAR, high).astype(wire)
    relay_y = copy(stage_ref.at[OWN, high], relay_ref.at[HIGH], by_y)
    ready(X)
    stage_ref[X, low, :] = chip_sum(X, low).astype(wire)
    arrive = [copy(stage_ref.at[X, low], last_ref.at[LOW, low], by_x)]
    ready(Y)
    stage_ref[Y, high, :] = chip_sum(Y, high).astype(wire)
    arrive.append(copy(stage_ref.at[Y, high], last_ref.at[HIGH, high], by_y))
    others = [copy(source, target, partner) for source, target in extras]
    relay_y.wait_recv()
    stage_ref[X, high, :] = (chip_sum(X, high) + relay_ref[HIGH].astype(F32)).astype(wire)
    arrive.append(copy(stage_ref.at[X, high], last_ref.at[LOW, high], by_x))
    relay_x.wait_recv()
    stage_ref[Y, low, :] = (chip_sum(Y, low) + relay_ref[LOW].astype(F32)).astype(wire)
    arrive.append(copy(stage_ref.at[Y, low], last_ref.at[HIGH, low], by_y))
    ready(OWN)
    out_ref[...] = chip_sum(OWN, full)
    shadow()
    for step in arrive:
        step.wait_recv()
    out_ref[...] += last_ref[LOW].astype(F32) + last_ref[HIGH].astype(F32)

    def drain():
        for step in others:
            step.wait_recv()
        for step in made:
            step.wait_send()

    return drain


def reduce_scratch(part):
    rows, tokens = part.shape[1:]
    return [
        pltpu.VMEM((4, rows, tokens), part.dtype),
        pltpu.VMEM((4, rows, tokens), part.dtype),
        pltpu.VMEM((3, rows, tokens), part.dtype),
        pltpu.VMEM((2, rows // 2, tokens), part.dtype),
        pltpu.VMEM((2, rows, tokens), part.dtype),
        pltpu.SemaphoreType.DMA((13,)),
        pltpu.SemaphoreType.DMA((13,)),
        pltpu.SemaphoreType.DMA((4,)),
    ]


def nothing():
    pass


def mix(x_ref, w_dense):
    x = x_ref[...]
    return (x.astype(F32) + dot_tn(w_dense, x)).astype(BF16)


def shared_forward(mixed, ws_gate, ws_up):
    s_one = dot_tn(ws_gate, mixed)
    s_three = dot_tn(ws_up, mixed)
    return s_one, s_three, (jax.nn.silu(s_one) * s_three).astype(BF16)


def shared_backward(grad_y, mixed, ws_gate, ws_up, ws_down, pack_ref, start):
    s_one, s_three, shared_hidden = shared_forward(mixed, ws_gate, ws_up)
    act_one, slope = silu_parts(s_one)
    grad_shared = dot_tn(ws_down, grad_y)
    grad_s_one = (grad_shared * s_three * slope).astype(BF16)
    grad_s_three = (grad_shared * act_one).astype(BF16)
    ff = ws_gate.shape[1]
    for i, value in enumerate((dot_nt(mixed, grad_s_one), dot_nt(mixed, grad_s_three), dot_nt(grad_y, shared_hidden))):
        pack_ref[:, start + i * ff : start + (i + 1) * ff] = value.astype(BF16)
    return dot_nn(ws_gate, grad_s_one) + dot_nn(ws_up, grad_s_three)


def comm_call(kernel, cid, out_shape, in_specs, out_specs, scratch, operands):
    return pl.pallas_call(
        kernel,
        out_shape=out_shape,
        in_specs=in_specs,
        out_specs=out_specs,
        scratch_shapes=scratch,
        compiler_params=pltpu.CompilerParams(collective_id=cid, has_side_effects=True, vmem_limit_bytes=VMEM_LIMIT),
        cost_estimate=COST,
    )(*operands)


def first_kernel(x_ref, w_dense_ref, meta_ref, tok_ref, metas_ref, own_ref, land_ref, land_meta_ref, *sems):
    devices = neighbours()
    own_ref[...] = mix(x_ref, w_dense_ref[0])
    greet(devices)
    gather_phase(devices, [own_ref, meta_ref], [tok_ref, metas_ref], [land_ref, land_meta_ref], sems, (nothing,) * 3)


def first_exchange(x, w_dense, meta):
    outs = (jax.ShapeDtypeStruct((8,) + x.shape, BF16), jax.ShapeDtypeStruct((8,) + meta.shape, F32), jax.ShapeDtypeStruct(x.shape, BF16))
    return comm_call(first_kernel, 0, outs, [whole()] * 3, (anywhere(), anywhere(), whole()), gather_scratch(x, meta), (x, w_dense, meta))


def forward_kernel(part_ref, u1_ref, ws_gate_ref, ws_up_ref, ws_down_ref, w_dense_ref, tok_ref, x2_ref, u2_ref, sum_ref, shared_ref, *scratch):
    devices = neighbours()
    greet(devices)

    def shadow():
        hidden = shared_forward(u1_ref[...], ws_gate_ref[0], ws_up_ref[0])[2]
        shared_ref[...] = dot_nn(ws_down_ref[0], hidden)

    drain = reduce_phase(devices, part_ref, sum_ref, scratch[:8], [], shadow)
    x2_ref[...] = (u1_ref[...].astype(F32) + sum_ref[...] + shared_ref[...]).astype(BF16)
    u2_ref[...] = mix(x2_ref, w_dense_ref[1])
    gather_phase(devices, [u2_ref], [tok_ref], [scratch[8]], scratch[9:], (nothing,) * 3)
    drain()


def forward_exchange(part, u1, ws_gate, ws_up, ws_down_t, w_dense):
    outs = (jax.ShapeDtypeStruct((8,) + u1.shape, BF16), jax.ShapeDtypeStruct(u1.shape, BF16), jax.ShapeDtypeStruct(u1.shape, BF16))
    scratch = [pltpu.VMEM(u1.shape, F32), pltpu.VMEM(u1.shape, F32)] + reduce_scratch(part) + gather_scratch(u1)
    specs = [anywhere()] + [whole()] * 5
    return comm_call(forward_kernel, 1, outs, specs, (anywhere(), whole(), whole()), scratch, (part, u1, ws_gate, ws_up, ws_down_t, w_dense))


def expert_half(refs, layer, target_ref):
    own = target_ref.shape[1]
    start = lax.axis_index("dp") * own
    return [(ref.at[layer, pl.ds(start, own)], target_ref.at[i]) for i, ref in enumerate(refs)]


def pair_half(partner, pack_ref, land_ref, sems):
    half = land_ref.shape[0]
    dp = lax.axis_index("dp")
    sent = []

    def start():
        theirs = pack_ref.at[pl.ds(pl.multiple_of((1 - dp) * half, 16), half)]
        sent.append(send_block(theirs, land_ref, sems.at[0], sems.at[1], partner))

    def finish():
        sent[0].wait()
        mine = pack_ref[pl.ds(pl.multiple_of(dp * half, 16), half), :]
        return (mine.astype(F32) + land_ref[...].astype(F32)).astype(BF16)

    return start, finish


def pair_scratch(shape):
    return [pltpu.VMEM(shape, BF16), pltpu.VMEM((shape[0] // 2, shape[1]), BF16), pltpu.SemaphoreType.DMA((2,))]


def backward_kernel(part_ref, d1_ref, d3_ref, d2_ref, grad_y_ref, x2_ref, u2_ref, u1_ref, w_dense_ref, ws_gate_ref, ws_up_ref, ws_down_ref, *refs):
    grad_all_ref, recv_ref, grad_x_ref, back_ref, chip_ref, sum_ref, mixed_ref, pack_ref, land_ref, pair_sem = refs[:10]
    scratch = refs[10:]
    devices = neighbours()
    greet(devices)
    ff = ws_gate_ref.shape[2]
    width = x2_ref.shape[0]
    start_pair, finish_pair = pair_half(devices[2], pack_ref, land_ref, pair_sem)

    def shadow():
        back_ref[...] = shared_backward(grad_y_ref[...], u2_ref[...], ws_gate_ref[1], ws_up_ref[1], ws_down_ref[1], pack_ref, 0)

    drain = reduce_phase(devices, part_ref, sum_ref, scratch[:8], expert_half((d1_ref, d3_ref, d2_ref), 1, recv_ref), shadow)
    mixed_ref[...] = (grad_y_ref[...].astype(F32) + sum_ref[...] + back_ref[...]).astype(BF16)
    grad_x_ref[...] = (mixed_ref[...].astype(F32) + dot_nn(w_dense_ref[1], mixed_ref[...])).astype(BF16)

    def dense_part():
        pack_ref[:, 6 * ff : 6 * ff + width] = dot_nt(x2_ref[...], mixed_ref[...]).astype(BF16)
        pack_ref[:, 6 * ff + width :] = jnp.zeros((width, pack_ref.shape[1] - 6 * ff - width), BF16)

    def shared_part():
        back_ref[...] = shared_backward(grad_x_ref[...], u1_ref[...], ws_gate_ref[0], ws_up_ref[0], ws_down_ref[0], pack_ref, 3 * ff)

    gather_phase(devices, [grad_x_ref], [grad_all_ref], [scratch[8]], scratch[9:], (dense_part, shared_part, start_pair))
    chip_ref[...] = finish_pair()
    drain()


def backward_exchange(part, held, grad_y, x2, u2, u1, w_dense, ws_gate, ws_up, ws_down_t):
    ff = ws_gate.shape[2]
    width = x2.shape[0]
    packed = 6 * ff + width + -(6 * ff + width) % 128
    own = held[0].shape[1] // 2
    outs = (
        jax.ShapeDtypeStruct((8,) + x2.shape, BF16),
        jax.ShapeDtypeStruct((3, own) + held[0].shape[2:], BF16),
        jax.ShapeDtypeStruct(x2.shape, BF16),
        jax.ShapeDtypeStruct(x2.shape, F32),
        jax.ShapeDtypeStruct((width // 2, packed), BF16),
    )
    scratch = [pltpu.VMEM(x2.shape, F32), pltpu.VMEM(x2.shape, BF16)] + pair_scratch((width, packed)) + reduce_scratch(part) + gather_scratch(x2)
    operands = (part, *held, grad_y, x2, u2, u1, w_dense, ws_gate, ws_up, ws_down_t)
    specs = [anywhere()] * 4 + [whole()] * 8
    return comm_call(backward_kernel, 2, outs, specs, (anywhere(), anywhere()) + (whole(),) * 3, scratch, operands)


def last_kernel(part_ref, d1_ref, d3_ref, d2_ref, grad_y_ref, back_ref, x_ref, w_dense_ref, grad_x_ref, recv_ref, chip_ref, sum_ref, mixed_ref, pack_ref, land_ref, pair_sem, *scratch):
    devices = neighbours()
    greet(devices)
    start_pair, finish_pair = pair_half(devices[2], pack_ref, land_ref, pair_sem)
    drain = reduce_phase(devices, part_ref, sum_ref, scratch, expert_half((d1_ref, d3_ref, d2_ref), 0, recv_ref), nothing)
    mixed_ref[...] = (grad_y_ref[...].astype(F32) + sum_ref[...] + back_ref[...]).astype(BF16)
    pack_ref[...] = dot_nt(x_ref[...], mixed_ref[...]).astype(BF16)
    grad_x_ref[...] = (mixed_ref[...].astype(F32) + dot_nn(w_dense_ref[0], mixed_ref[...])).astype(BF16)
    start_pair()
    drain()
    chip_ref[...] = finish_pair()


def last_exchange(part, held, grad_y, back, x, w_dense):
    own = held[0].shape[1] // 2
    width = x.shape[0]
    outs = (jax.ShapeDtypeStruct(x.shape, BF16), jax.ShapeDtypeStruct((3, own) + held[0].shape[2:], BF16), jax.ShapeDtypeStruct((width // 2, width), BF16))
    scratch = [pltpu.VMEM(x.shape, F32), pltpu.VMEM(x.shape, BF16)] + pair_scratch((width, width)) + reduce_scratch(part)
    specs = [anywhere()] * 4 + [whole()] * 4
    return comm_call(last_kernel, 3, outs, specs, (whole(), anywhere(), whole()), scratch, (part, *held, grad_y, back, x, w_dense))


def send_over(x, flip):
    return lax.ppermute(x, "ep", [(i, i ^ flip) for i in range(4)])


def swap_cores(x):
    return lax.ppermute(x, "dp", [(0, 1), (1, 0)])


def sum_start(chip):
    sent = [chip]
    for flip in (1, 2, 3):
        sent.append(send_over(chip, flip))
    return sent


def sum_finish(parts):
    total = sum(part.astype(F32) for part in parts).astype(BF16)
    other = swap_cores(total)
    first = lax.axis_index("dp") == 0
    return jnp.concatenate([jnp.where(first, total, other), jnp.where(first, other, total)], axis=0)


def solution(mesh):
    ep_size = mesh.shape["ep"]
    dp_size = mesh.shape["dp"]
    tok_spec = P(ALL_AXES)
    route_spec = P(None, ALL_AXES)
    exp_spec = P(None, "ep")
    repl_spec = P()

    def body(act_in, grad_out, slot_ids, gate_vals, w_dense, w_gate, w_up, w_down, ws_gate, ws_up, ws_down):
        layers, local_exp = w_gate.shape[:2]
        tokens = act_in.shape[0]
        top = slot_ids.shape[2]
        own = local_exp // dp_size
        groups = own // GROUP
        capacity = 2 * tokens * top // (local_exp * ep_size)
        dp = lax.axis_index("dp")
        base = jnp.stack([lax.axis_index("ep") * local_exp + dp * own, dp * groups, (dp_size - 1 - dp) * groups]).astype(jnp.int32)
        w_down_t = jnp.swapaxes(w_down, 2, 3)
        meta = jnp.concatenate([jnp.swapaxes(slot_ids, 1, 2).astype(F32), jnp.swapaxes(gate_vals, 1, 2)], axis=1)
        meta = meta.reshape(layers * 2 * top, tokens)

        x1 = act_in.T
        grad_y2 = grad_out.T
        shared_w = (ws_gate, ws_up, jnp.swapaxes(ws_down, 1, 2))
        tok1, metas, u1 = first_exchange(x1, w_dense, meta)
        tok1, grad_y2 = lax.optimization_barrier((tok1, grad_y2))
        grads2 = [grad_y2, send_over(grad_y2, 1), send_over(grad_y2, 2), send_over(grad_y2, 3)]
        grads2 = grads2 + [swap_cores(x) for x in grads2]
        part, rows1 = expert_forward(0, capacity, groups, base, tok1, metas, w_gate, w_up, w_down_t)
        tok2, x2, u2 = forward_exchange(part, u1, *shared_w, w_dense)
        back2, *held = expert_backward(1, capacity, groups, base, tok2, False, grads2, metas, w_gate, w_up, w_down_t, [])
        grad1_all, recv2, grad_y1, shared1, early = backward_exchange(back2, held, grad_y2, x2, u2, u1, w_dense, *shared_w)
        ff = ws_gate.shape[2]
        width = w_dense.shape[1]
        early = sum_start(early)
        grad1_all, early[0] = lax.optimization_barrier((grad1_all, early[0]))
        back1, *held = expert_backward(0, capacity, groups, base, rows1, True, [grad1_all], metas, w_gate, w_up, w_down_t, [recv2] + held)
        grad_x, recv1, late = last_exchange(back1, held, grad_y1, shared1, x1, w_dense)
        late = sum_start(late)
        g_gate, g_up, g_down = place(0, groups, base, recv1, held)
        g_gate, late = lax.optimization_barrier((g_gate, late))
        g_down = jnp.swapaxes(g_down, 2, 3)
        early = sum_finish(early)
        late = sum_finish(late)
        g_dense = jnp.stack([late, early[:, 6 * ff : 6 * ff + width]])
        shared = [jnp.stack([early[:, (3 + i) * ff : (4 + i) * ff], early[:, i * ff : (i + 1) * ff]]) for i in range(3)]
        return (grad_x.T, g_dense, g_gate, g_up, g_down, shared[0], shared[1], jnp.swapaxes(shared[2], 1, 2))

    return jax.shard_map(body, mesh=mesh, in_specs=(tok_spec, tok_spec, route_spec, route_spec, repl_spec, exp_spec, exp_spec, exp_spec, repl_spec, repl_spec, repl_spec), out_specs=(tok_spec, repl_spec, exp_spec, exp_spec, exp_spec, repl_spec, repl_spec, repl_spec), check_vma=False)
```
